8 devices in a mesh: tp: 2 (over z, y), ep: 4 (over x, core).
Axes of the slice: x: 2, y: 2, z: 1, core: 2. Of those that a mesh axis runs over, the one named last changes fastest.
Arguments:
- x: bfloat16 [4096, 2048], P(('ep', 'tp'))
- idx: int32 [4096, 4], P(('ep', 'tp'))
- g: float32 [4096, 4], P(('ep', 'tp'))
- slot: int32 [4096, 4], P(('ep', 'tp'))
- ws1: bfloat16 [2048, 5632], P(None, 'tp')
- ws3: bfloat16 [2048, 5632], P(None, 'tp')
- ws2: bfloat16 [5632, 2048], P('tp')
- w1: bfloat16 [60, 2048, 1408], P('ep')
- w3: bfloat16 [60, 2048, 1408], P('ep')
- w2: bfloat16 [60, 1408, 2048], P('ep')
Outputs:
- output: bfloat16 [4096, 2048], P(('ep', 'tp'))
All inputs are finite; a program needn't handle non-finite values.
Results may differ from the reference program's by a relative error of at most 0.001.
Values are sent between devices in bfloat16 or wider.
A program may use at most 1.25 GiB of HBM per device.

```python
import jax
import jax.numpy as jnp
from jax import lax

D = 2048
F = 1408
FS = 5632
E = 60
K = 4
TOK = 512
DEV = 8
C = 72

T = TOK * DEV
ROWS = DEV * C


def _weights(key, n, shape, fan_in):
    return lax.map(lambda kk: (jax.random.normal(kk, shape, jnp.float32) * fan_in ** -0.5).astype(jnp.bfloat16), jax.random.split(key, n))


def _positions(idx):
    oh = jax.nn.one_hot(idx.reshape(DEV, TOK * K), E, dtype=jnp.int32)
    return jnp.sum((jnp.cumsum(oh, axis=1) - 1) * oh, axis=-1).reshape(T, K)


def _route_ids(key):
    weight = jnp.uint32(96) + (jnp.uint32(256) * jnp.arange(E, dtype=jnp.uint32)) // jnp.uint32(E)
    wait = (jax.random.bits(key, (T, E), jnp.uint32) >> 10) * weight[None, :]
    return jnp.argsort(wait, axis=-1, stable=True)[:, :K].astype(jnp.int32)


def setup_inputs(seed: int = 0) -> dict:
    ks = jax.random.split(jax.random.PRNGKey(seed), 10)
    x = jax.random.normal(ks[0], (T, D), jnp.float32).astype(jnp.bfloat16)
    idx = _route_ids(jax.random.fold_in(ks[1], 7))
    g = jax.random.uniform(ks[2], (T, K), jnp.float32, 0.4, 1.0)
    pos = _positions(idx)
    slot = jnp.where(pos < C, C - 1 - pos, -1).astype(jnp.int32)
    return {
        "x": x, "idx": idx, "g": g, "slot": slot,
        "ws1": _weights(ks[3], 1, (D, FS), D)[0],
        "ws3": _weights(ks[4], 1, (D, FS), D)[0],
        "ws2": _weights(ks[5], 1, (FS, D), FS)[0],
        "w1": _weights(ks[6], E, (D, F), D),
        "w3": _weights(ks[7], E, (D, F), D),
        "w2": _weights(ks[8], E, (F, D), F),
    }


def _swiglu(x, w1, w3, w2):
    a = jnp.dot(x, w1, preferred_element_type=jnp.float32)
    b = jnp.dot(x, w3, preferred_element_type=jnp.float32)
    h = (jax.nn.silu(a) * b).astype(jnp.bfloat16)
    return jnp.dot(h, w2, preferred_element_type=jnp.float32)


def reference(x, idx, g, slot, ws1, ws3, ws2, w1, w3, w2):
    s = _swiglu(x, ws1, ws3, ws2)
    blk = (jnp.arange(T, dtype=jnp.int32) // TOK)[:, None]
    kept = slot >= 0
    dest = jnp.where(kept, idx * ROWS + blk * C + slot, E * ROWS)
    buf = jnp.zeros((E * ROWS, D), jnp.bfloat16)
    for j in range(K):
        buf = buf.at[dest[:, j]].set(x, mode="drop")
    out = lax.map(lambda a: _swiglu(*a).astype(jnp.bfloat16), (buf.reshape(E, ROWS, D), w1, w3, w2))
    out = out.reshape(E * ROWS, D)
    gate = jnp.where(kept, g, 0.0)
    src = jnp.where(kept, dest, 0)
    y = x.astype(jnp.float32) + s
    for j in range(K):
        y = y + gate[:, j:j + 1] * jnp.take(out, src[:, j], axis=0).astype(jnp.float32)
    return y.astype(jnp.bfloat16)
```

```python
import functools

import jax
import jax.numpy as jnp
from jax import lax
from jax.experimental import pallas as pl
from jax.experimental.pallas import tpu as pltpu
from jax.sharding import PartitionSpec as P

CAP = 72
MAIN = 64
TAIL = CAP - MAIN
NC = 4


def _swiglu2(x, w1, w3, w2):
    a = jnp.dot(x, w1, preferred_element_type=jnp.float32)
    b = jnp.dot(x, w3, preferred_element_type=jnp.float32)
    h = (jax.nn.silu(a) * b).astype(jnp.bfloat16)
    return jnp.dot(h, w2, preferred_element_type=jnp.float32)


def _up_kernel(*refs):
    m = refs[0:4]
    t = refs[4:8]
    w1, w3, h, xs = refs[8:]
    for s in range(4):
        xs[s * MAIN:(s + 1) * MAIN, :] = m[s][0]
    xs[4 * MAIN:4 * CAP, :] = jnp.concatenate([t[s][0] for s in range(4)], axis=0).astype(jnp.bfloat16)
    f = h.shape[-1]
    full = f // 256 * 256
    x = xs[...]
    for n in range(0, full, 256):
        a = jnp.dot(x, w1[0, :, n:n + 256], preferred_element_type=jnp.float32)
        b = jnp.dot(x, w3[0, :, n:n + 256], preferred_element_type=jnp.float32)
        h[0, :, n:n + 256] = (jax.nn.silu(a) * b).astype(jnp.bfloat16)
    if full < f:
        r = f - full
        w = jnp.concatenate([w1[0, :, full:], w3[0, :, full:]], axis=1)
        ab = jnp.dot(x, w, preferred_element_type=jnp.float32)
        h[0, :, full:] = (jax.nn.silu(ab[:, :r]) * ab[:, r:]).astype(jnp.bfloat16)


def _up(mains, tails, w1, w3):
    el, d, f = w1.shape
    spec = lambda a, b: pl.BlockSpec((1, a, b), lambda e: (e, 0, 0))
    return pl.pallas_call(
        _up_kernel,
        grid=(el,),
        out_shape=jax.ShapeDtypeStruct((el, 4 * CAP, f), jnp.bfloat16),
        in_specs=[spec(MAIN, d)] * 4 + [spec(TAIL, d)] * 4 + [spec(d, f)] * 2,
        out_specs=spec(4 * CAP, f),
        scratch_shapes=[pltpu.VMEM((4 * CAP, d), jnp.bfloat16)],
        compiler_params=pltpu.CompilerParams(vmem_limit_bytes=48 * 1024 * 1024),
        cost_estimate=pl.CostEstimate(flops=2 * 2 * el * 4 * CAP * d * f, bytes_accessed=4 * el * d * f, transcendentals=0),
        name="up",
    )(*mains, *tails, w1, w3)


def _down_kernel(el, tab, h, w2, o0, o1, o2, o3, gm, rm, rt):
    e = pl.program_id(0)
    outs = (o0, o1, o2, o3)
    kt = gm.shape[-1]
    tok = o0.shape[0]
    cols = o0.shape[1]
    blk = 128
    nblk = 4 * tok // blk

    @pl.when(e == 0)
    def _():
        rt[:, el * TAIL:, :] = jnp.zeros((4, rt.shape[1] - el * TAIL, cols), jnp.float32)

    def gates(b):
        row = pl.multiple_of(b * blk, blk)
        t = tab[pl.ds(row, blk), :]
        lane = lax.broadcasted_iota(jnp.int32, (blk, kt), 1).astype(jnp.float32)
        acc = [jnp.zeros((blk, kt), jnp.float32) for _ in range(3)]
        for j in range(4):
            hit = t[:, j:j + 1] == lane
            for i in range(3):
                acc[i] = jnp.where(hit, t[:, 4 + 4 * i + j:5 + 4 * i + j], acc[i])
        for i in range(3):
            gm[i, pl.ds(row, blk), :] = acc[i].astype(jnp.bfloat16)

    @pl.when(e < el)
    def _():
        for n in range(0, cols, 256):
            r = jnp.dot(h[0], w2[0, :, n:n + 256], preferred_element_type=jnp.float32).astype(jnp.bfloat16)
            for s in range(4):
                rm[s, pl.ds(pl.multiple_of(e * MAIN, MAIN), MAIN), n:n + 256] = r[s * MAIN:(s + 1) * MAIN]
            q = r[4 * MAIN:].astype(jnp.float32)
            for s in range(4):
                rt[s, pl.ds(pl.multiple_of(e * TAIL, TAIL), TAIL), n:n + 256] = q[s * TAIL:(s + 1) * TAIL]
        gates(e)

    @pl.when(e == el)
    def _():
        for b in range(el, nblk):
            gates(b)
        for s in range(4):
            for n in range(0, cols, 256):
                acc = jnp.zeros((tok, 256), jnp.float32)
                tail = rt[s, :, n:n + 256].astype(jnp.bfloat16)
                for i in range(3):
                    acc += jnp.dot(gm[i, s * tok:(s + 1) * tok, :rm.shape[1]], rm[s, :, n:n + 256],
                                   preferred_element_type=jnp.float32)
                    acc += jnp.dot(gm[i, s * tok:(s + 1) * tok, rm.shape[1]:], tail,
                                   preferred_element_type=jnp.float32)
                outs[s][:, n:n + 256] = acc


def _down(c, tab, h, w2, tok):
    el, f, d = w2.shape
    cols = d // NC
    kt = el * MAIN + 128
    last = el - 1
    return pl.pallas_call(
        functools.partial(_down_kernel, el),
        grid=(el + 1,),
        out_shape=[jax.ShapeDtypeStruct((tok, cols), jnp.float32)] * 4,
        in_specs=[
            pl.BlockSpec(tab.shape, lambda e: (0, 0)),
            pl.BlockSpec((1, 4 * CAP, f), lambda e: (jnp.minimum(e, last), 0, 0)),
            pl.BlockSpec((1, f, cols), lambda e: (jnp.minimum(e, last), 0, c)),
        ],
        out_specs=[pl.BlockSpec((tok, cols), lambda e: (0, 0))] * 4,
        scratch_shapes=[
            pltpu.VMEM((3, 4 * tok, kt), jnp.bfloat16),
            pltpu.VMEM((4, el * MAIN, cols), jnp.bfloat16),
            pltpu.VMEM((4, 128, cols), jnp.float32),
        ],
        compiler_params=pltpu.CompilerParams(vmem_limit_bytes=60 * 1024 * 1024),
        cost_estimate=pl.CostEstimate(flops=2 * el * 4 * CAP * f * cols + 6 * 4 * tok * kt * cols,
                                      bytes_accessed=2 * el * f * cols + 2 * el * 4 * CAP * f, transcendentals=0),
        name=f"down{c}",
    )(tab, h, w2)


def solution(mesh):
    ep = mesh.shape["ep"]
    rows = P(("ep", "tp"), None)
    pair = lambda k: [(i, i ^ k) for i in range(ep)]

    def body(x, idx, g, slot, ws1, ws3, ws2, w1, w3, w2):
        tok, d = x.shape
        el = w1.shape[0]
        me = lax.axis_index("ep")
        bf = lambda a: lax.reduce_precision(a, 8, 7)

        code = jnp.where(slot >= 0, idx * 128 + slot, -1).astype(jnp.float32)
        mine = jnp.concatenate([code, g], axis=1).T
        xx = lax.ppermute(x, "ep", pair(2))
        xy = lax.ppermute(x, "tp", [(0, 1), (1, 0)])
        xc = lax.ppermute(x, "ep", pair(1))
        xxc = lax.ppermute(xx, "ep", pair(1))
        xsrc = (x, xc, xx, xxc)
        tabs = (mine,) + tuple(lax.ppermute(mine, "ep", pair(k)) for k in (1, 2, 3))

        mains, tails, cols = [], [], []
        for s in range(4):
            code = tabs[s][:4].astype(jnp.int32)
            gs = tabs[s][4:]
            e, k = code >> 7, code & 127
            le = e - me * el
            ok = (code >= 0) & (le >= 0) & (le < el)
            c = jnp.where(ok, jnp.where(k < MAIN, le * MAIN + k, el * MAIN + le * TAIL + k - MAIN), -1)
            g0 = bf(gs)
            g1 = bf(gs - g0)
            g2 = gs - g0 - g1
            cols.append(jnp.concatenate([c.astype(jnp.float32), g0, g1, g2], axis=0))
            r = lax.broadcasted_iota(jnp.int32, (el * CAP, tok), 0)
            hot = (r == c[0]) | (r == c[1]) | (r == c[2]) | (r == c[3])
            hot = hot.astype(jnp.bfloat16)
            mains.append(jnp.dot(hot[:el * MAIN], xsrc[s], preferred_element_type=jnp.float32)
                         .astype(jnp.bfloat16).reshape(el, MAIN, d))
            tails.append(jnp.dot(hot[el * MAIN:], xsrc[s], preferred_element_type=jnp.float32).reshape(el, TAIL, d))
        tab = jnp.concatenate(cols, axis=1).T

        so = _swiglu2(x, ws1, ws3, ws2)
        sy = lax.ppermute(_swiglu2(xy, ws1, ws3, ws2), "tp", [(0, 1), (1, 0)])

        h = _up(mains, tails, w1, w3)
        parts = []
        for c in range(NC):
            p0, p1, p2, p3 = _down(c, tab, h, w2, tok)
            q0 = lax.ppermute(p1, "ep", pair(1))
            q2 = lax.ppermute(p3, "ep", pair(1))
            back = lax.ppermute(p2 + q2, "ep", pair(2))
            parts.append(p0 + q0 + back)
        r = jnp.concatenate(parts, axis=1)
        return (x.astype(jnp.float32) + (so + sy) + r).astype(jnp.bfloat16)

    return jax.shard_map(
        body, mesh=mesh,
        in_specs=(rows, rows, rows, rows, P(None, "tp"), P(None, "tp"), P("tp", None),
                  P("ep", None, None), P("ep", None, None), P("ep", None, None)),
        out_specs=rows, check_vma=False)
```

```python
import functools

import jax
import jax.numpy as jnp
from jax import lax
from jax.experimental import pallas as pl
from jax.experimental.pallas import tpu as pltpu
from jax.sharding import PartitionSpec as P

CAP = 72
MAIN = 64
TAIL = CAP - MAIN
NC = 4
MIB = 1024 * 1024
ANY = pl.BlockSpec(memory_space=pl.ANY)


def _params(mib):
    return pltpu.CompilerParams(vmem_limit_bytes=mib * MIB)


def _dot(a, b):
    return jnp.dot(a, b, preferred_element_type=jnp.float32)


def _shared_kernel(nf, x, w1, w3, w2, *rest):
    o, h = rest[-2:]
    i = pl.program_id(0)

    @pl.when(i < nf)
    def _():
        a = _dot(x[...], w1[...])
        b = _dot(x[...], w3[...])
        h[i] = (jax.nn.silu(a) * b).astype(jnp.bfloat16)

    @pl.when(i >= nf)
    def _():
        o[...] = _dot(jnp.concatenate([h[k] for k in range(nf)], axis=1), w2[...])


def _shared(x, w1, w3, w2, deps=()):
    m, d = x.shape
    f = w1.shape[1]
    tf, tn = 256, 256
    nf, nn = f // tf, d // tn
    up = pl.BlockSpec((d, tf), lambda i: (0, jnp.minimum(i, nf - 1)))
    down = lambda i: (0, jnp.maximum(i - nf, 0))
    return pl.pallas_call(
        functools.partial(_shared_kernel, nf),
        grid=(nf + nn,),
        out_shape=jax.ShapeDtypeStruct((m, d), jnp.float32),
        in_specs=[pl.BlockSpec((m, d), lambda i: (0, 0)), up, up, pl.BlockSpec((f, tn), down)] + [ANY] * len(deps),
        out_specs=pl.BlockSpec((m, tn), down),
        scratch_shapes=[pltpu.VMEM((nf, m, tf), jnp.bfloat16)],
        compiler_params=_params(60),
        cost_estimate=pl.CostEstimate(flops=6 * m * d * f, bytes_accessed=6 * d * f, transcendentals=0),
        name="shared",
    )(x, w1, w3, w2, *deps)


def _gather_kernel(el, c, x, *rest):
    main, tail = rest[-2:]
    i = pl.program_id(0)
    tok = x.shape[0]

    def hot(n, base):
        r = (lax.broadcasted_iota(jnp.int32, (n, tok), 0) + base).astype(jnp.float32)
        hit = r == c[0:1, :]
        for j in range(1, 4):
            hit = hit | (r == c[j:j + 1, :])
        return jnp.where(hit, 1.0, 0.0).astype(jnp.bfloat16)

    rows = main.shape[0]
    p = hot(rows, i * rows)
    for n in range(0, x.shape[1], 512):
        main[:, n:n + 512] = _dot(p, x[:, n:n + 512]).astype(jnp.bfloat16)

    @pl.when(i == 0)
    def _():
        p = hot(el * TAIL, el * MAIN)
        for n in range(0, x.shape[1], 512):
            tail[:, n:n + 512] = _dot(p, x[:, n:n + 512])


def _gather(c, x, el, deps=()):
    tok, d = x.shape
    rows = el * MAIN // 2
    main, tail = pl.pallas_call(
        functools.partial(_gather_kernel, el),
        grid=(2,),
        out_shape=[jax.ShapeDtypeStruct((el * MAIN, d), jnp.bfloat16), jax.ShapeDtypeStruct((el * TAIL, d), jnp.float32)],
        in_specs=[pl.BlockSpec(c.shape, lambda i: (0, 0)), pl.BlockSpec((tok, d), lambda i: (0, 0))] + [ANY] * len(deps),
        out_specs=[pl.BlockSpec((rows, d), lambda i: (i, 0)), pl.BlockSpec((el * TAIL, d), lambda i: (0, 0))],
        compiler_params=_params(60),
        cost_estimate=pl.CostEstimate(flops=2 * el * CAP * tok * d, bytes_accessed=2 * el * CAP * d, transcendentals=0),
        name="gather",
    )(c, x, *deps)
    return main.reshape(el, MAIN, d), tail.reshape(el, TAIL, d)


def _gates_kernel(tab, g):
    blk, k3 = g.shape
    kt = k3 // 3
    lane = lax.broadcasted_iota(jnp.int32, (blk, kt), 1).astype(jnp.float32)
    acc = [jnp.zeros((blk, kt), jnp.float32) for _ in range(3)]
    for j in range(4):
        hit = tab[:, j:j + 1] == lane
        for i in range(3):
            acc[i] = jnp.where(hit, tab[:, 4 + 4 * i + j:5 + 4 * i + j], acc[i])
    for i in range(3):
        g[:, i * kt:(i + 1) * kt] = acc[i].astype(jnp.bfloat16)


def _gates(tab, kt):
    n = tab.shape[0]
    blk = 128
    return pl.pallas_call(
        _gates_kernel,
        grid=(n // blk,),
        out_shape=jax.ShapeDtypeStruct((n, 3 * kt), jnp.bfloat16),
        in_specs=[pl.BlockSpec((blk, tab.shape[1]), lambda i: (i, 0))],
        out_specs=pl.BlockSpec((blk, 3 * kt), lambda i: (i, 0)),
        compiler_params=_params(60),
        cost_estimate=pl.CostEstimate(flops=100 * n * kt, bytes_accessed=6 * n * kt, transcendentals=0),
        name="gates",
    )(tab)


def _up_kernel(*refs):
    m = refs[0:4]
    t = refs[4:8]
    w1, w3 = refs[8:10]
    h, xs = refs[-2:]
    for s in range(4):
        xs[s * MAIN:(s + 1) * MAIN, :] = m[s][0]
    xs[4 * MAIN:4 * CAP, :] = jnp.concatenate([t[s][0] for s in range(4)], axis=0).astype(jnp.bfloat16)
    f = h.shape[-1]
    full = f // 256 * 256
    x = xs[...]
    for n in range(0, full, 256):
        a = _dot(x, w1[0, :, n:n + 256])
        b = _dot(x, w3[0, :, n:n + 256])
        h[0, :, n:n + 256] = (jax.nn.silu(a) * b).astype(jnp.bfloat16)
    if full < f:
        r = f - full
        ab = _dot(x, jnp.concatenate([w1[0, :, full:], w3[0, :, full:]], axis=1))
        h[0, :, full:] = (jax.nn.silu(ab[:, :r]) * ab[:, r:]).astype(jnp.bfloat16)


def _up(mains, tails, w1, w3, deps=()):
    el, d, f = w1.shape
    spec = lambda a, b: pl.BlockSpec((1, a, b), lambda e: (e, 0, 0))
    return pl.pallas_call(
        _up_kernel,
        grid=(el,),
        out_shape=jax.ShapeDtypeStruct((el, 4 * CAP, f), jnp.bfloat16),
        in_specs=[spec(MAIN, d)] * 4 + [spec(TAIL, d)] * 4 + [spec(d, f)] * 2 + [ANY] * len(deps),
        out_specs=spec(4 * CAP, f),
        scratch_shapes=[pltpu.VMEM((4 * CAP, d), jnp.bfloat16)],
        compiler_params=_params(60),
        cost_estimate=pl.CostEstimate(flops=2 * 2 * el * 4 * CAP * d * f, bytes_accessed=4 * el * d * f, transcendentals=0),
        name="up",
    )(*mains, *tails, w1, w3, *deps)


def _down_kernel(el, g, h, w2, own, far, sib, r3, rt):
    e = pl.program_id(0)
    outs = (own, sib.at[0], far, sib.at[1])
    kt = r3.shape[1] // 3
    cols = own.shape[1]
    nm = el * MAIN

    @pl.when(e < el)
    def _():
        row = pl.multiple_of(e * MAIN, MAIN)
        for n in range(0, cols, 256):
            r = _dot(h[0], w2[0, :, n:n + 256]).astype(jnp.bfloat16)
            for s in range(4):
                for i in range(3):
                    r3[s, pl.ds(row + i * kt, MAIN), n:n + 256] = r[s * MAIN:(s + 1) * MAIN]
            q = r[4 * MAIN:].astype(jnp.float32)
            for s in range(4):
                rt[s, pl.ds(pl.multiple_of(e * TAIL, TAIL), TAIL), n:n + 256] = q[s * TAIL:(s + 1) * TAIL]

    for s in range(4):
        @pl.when(e == el + s)
        def _(s=s):
            tail = jnp.concatenate([rt[s], jnp.zeros((kt - el * CAP, cols), jnp.float32)], axis=0).astype(jnp.bfloat16)
            for i in range(3):
                r3[s, i * kt + nm:(i + 1) * kt, :] = tail
            for n in range(0, cols, 256):
                outs[s][:, n:n + 256] = _dot(g[...], r3[s, :, n:n + 256])


def _down(c, g, h, w2, tok, kt, deps=()):
    el, f, d = w2.shape
    cols = d // NC
    last = el - 1
    kern = functools.partial(_down_kernel, el)
    return pl.pallas_call(
        lambda g, h, w2, *r: kern(g, h, w2, *r[len(deps):]),
        grid=(el + 4,),
        out_shape=[jax.ShapeDtypeStruct((tok, cols), jnp.float32)] * 2 + [jax.ShapeDtypeStruct((2, tok, cols), jnp.float32)],
        in_specs=[
            pl.BlockSpec((tok, 3 * kt), lambda e: (jnp.maximum(e - el, 0), 0)),
            pl.BlockSpec((1, 4 * CAP, f), lambda e: (jnp.minimum(e, last), 0, 0)),
            pl.BlockSpec((1, f, cols), lambda e: (jnp.minimum(e, last), 0, c)),
        ] + [ANY] * len(deps),
        out_specs=[pl.BlockSpec((tok, cols), lambda e: (0, 0))] * 2 + [pl.BlockSpec((2, tok, cols), lambda e: (0, 0, 0))],
        scratch_shapes=[
            pltpu.VMEM((4, 3 * kt, cols), jnp.bfloat16),
            pltpu.VMEM((4, el * TAIL, cols), jnp.float32),
        ],
        compiler_params=_params(60),
        cost_estimate=pl.CostEstimate(flops=2 * el * 4 * CAP * f * cols + 6 * 4 * tok * kt * cols,
                                      bytes_accessed=2 * el * f * cols + 2 * el * 4 * CAP * f, transcendentals=0),
    )(g, h, w2, *deps)


def solution(mesh):
    rows = P(("ep", "tp"), None)

    def perm(a, axis, k=1):
        return lax.ppermute(a, axis, [(i, i ^ k) for i in range(mesh.shape[axis])])

    def body(x, idx, g, slot, ws1, ws3, ws2, w1, w3, w2):
        tok, _ = x.shape
        el = w1.shape[0]
        kt = -(-el * CAP // 16) * 16
        me = lax.axis_index("ep")
        bf = lambda a: lax.reduce_precision(a, 8, 7)
        half = tok // 2

        code = jnp.where(slot >= 0, idx * 128 + slot, -1).astype(jnp.float32)
        mine = jnp.concatenate([code, g], axis=1).T
        tabs = (mine,) + tuple(perm(mine, "ep", k) for k in (1, 2, 3))
        xx = perm(x, "ep", 2)
        y0 = perm(x[:half], "tp")
        y1 = perm(x[half:], "tp")
        xc = perm(x, "ep", 1)
        xxc = perm(xx, "ep", 1)

        cs, cols = [], []
        for s in range(4):
            code = tabs[s][:4].astype(jnp.int32)
            gs = tabs[s][4:]
            e, k = code >> 7, code & 127
            le = e - me * el
            ok = (code >= 0) & (le >= 0) & (le < el)
            c = jnp.where(ok, jnp.where(k < MAIN, le * MAIN + k, el * MAIN + le * TAIL + k - MAIN), -1).astype(jnp.float32)
            g0 = bf(gs)
            g1 = bf(gs - g0)
            g2 = gs - g0 - g1
            cs.append(c)
            cols.append(jnp.concatenate([c, g0, g1, g2], axis=0))
        tab = jnp.concatenate(cols, axis=1).T

        m0, t0 = _gather(cs[0], x, el)
        so = _shared(x, ws1, ws3, ws2, (t0,))
        gm = _gates(tab, kt)
        m1, t1 = _gather(cs[1], xc, el, (so, gm))
        s0 = _shared(y0, ws1, ws3, ws2, (t1,))
        r0 = perm(s0, "tp")
        s1 = _shared(y1, ws1, ws3, ws2, (s0,))
        r1 = perm(s1, "tp")
        m2, t2 = _gather(cs[2], xx, el, (s1,))
        m3, t3 = _gather(cs[3], xxc, el, (t2,))
        h = _up((m0, m1, m2, m3), (t0, t1, t2, t3), w1, w3)
        parts = []
        dep = ()
        for c in range(NC):
            own, far, sib = _down(c, gm, h, w2, tok, kt, dep)
            dep = (own,)
            q = perm(sib, "ep", 1)
            back = perm(far + q[1], "ep", 2)
            parts.append(own + q[0] + back)
        r = jnp.concatenate(parts, axis=1)
        sy = jnp.concatenate([r0, r1], axis=0)
        return (x.astype(jnp.float32) + (so + sy) + r).astype(jnp.bfloat16)

    return jax.shard_map(
        body, mesh=mesh,
        in_specs=(rows, rows, rows, rows, P(None, "tp"), P(None, "tp"), P("tp", None),
                  P("ep", None, None), P("ep", None, None), P("ep", None, None)),
        out_specs=rows, check_vma=False)
```

```python
import functools

import jax
import jax.numpy as jnp
from jax import lax
from jax.experimental import pallas as pl
from jax.experimental.pallas import tpu as pltpu
from jax.sharding import PartitionSpec as P

CAP = 72
MAIN = 64
TAIL = CAP - MAIN
MIB = 1024 * 1024
ANY = pl.BlockSpec(memory_space=pl.ANY)


def _params(mib):
    return pltpu.CompilerParams(vmem_limit_bytes=mib * MIB)


def _dot(a, b):
    return jnp.dot(a, b, preferred_element_type=jnp.float32)


def _shared_kernel(nf, nn, x, w1, w3, w2, *rest):
    o, v1, v3, v2, h, s1, s3, s2 = rest[-8:]
    tf, tn = v1.shape[2], v2.shape[2]
    up = lambda w, v, s, i: pltpu.make_async_copy(w.at[:, pl.ds(pl.multiple_of(i * tf, tf), tf)], v.at[i], s.at[i])
    down = lambda i: pltpu.make_async_copy(w2.at[:, pl.ds(pl.multiple_of(i * tn, tn), tn)], v2.at[i], s2.at[i])
    for i in range(nf):
        up(w1, v1, s1, i).start()
        up(w3, v3, s3, i).start()
    for i in range(nn):
        down(i).start()

    def gate(i, _):
        up(w1, v1, s1, i).wait()
        up(w3, v3, s3, i).wait()
        a = _dot(x[...], v1[i])
        b = _dot(x[...], v3[i])
        h[:, pl.ds(pl.multiple_of(i * tf, tf), tf)] = (jax.nn.silu(a) * b).astype(jnp.bfloat16)
        return 0

    def out(i, _):
        down(i).wait()
        o[:, pl.ds(pl.multiple_of(i * tn, tn), tn)] = _dot(h[...], v2[i])
        return 0

    lax.fori_loop(0, nf, gate, 0)
    lax.fori_loop(0, nn, out, 0)


def _shared(x, w1, w3, w2, deps=()):
    m, d = x.shape
    f = w1.shape[1]
    tf, tn = 256, 512
    nf, nn = f // tf, d // tn
    vmem = pl.BlockSpec(memory_space=pltpu.VMEM)
    return pl.pallas_call(
        functools.partial(_shared_kernel, nf, nn),
        out_shape=jax.ShapeDtypeStruct((m, d), jnp.float32),
        in_specs=[vmem] + [ANY] * (3 + len(deps)),
        out_specs=vmem,
        scratch_shapes=[
            pltpu.VMEM((nf, d, tf), jnp.bfloat16),
            pltpu.VMEM((nf, d, tf), jnp.bfloat16),
            pltpu.VMEM((nn, f, tn), jnp.bfloat16),
            pltpu.VMEM((m, f), jnp.bfloat16),
            pltpu.SemaphoreType.DMA((nf,)),
            pltpu.SemaphoreType.DMA((nf,)),
            pltpu.SemaphoreType.DMA((nn,)),
        ],
        compiler_params=_params(60),
        cost_estimate=pl.CostEstimate(flops=6 * m * d * f, bytes_accessed=6 * d * f, transcendentals=0),
        name="shared",
    )(x, w1, w3, w2, *deps)


def _gather_kernel(el, c, x, *rest):
    main, tail = rest[-2:]
    i = pl.program_id(0)
    tok = x.shape[0]

    def hot(n, base):
        r = (lax.broadcasted_iota(jnp.int32, (n, tok), 0) + base).astype(jnp.float32)
        hit = r == c[0:1, :]
        for j in range(1, 4):
            hit = hit | (r == c[j:j + 1, :])
        return jnp.where(hit, 1.0, 0.0).astype(jnp.bfloat16)

    rows = main.shape[0]
    p = hot(rows, i * rows)
    for n in range(0, x.shape[1], 512):
        main[:, n:n + 512] = _dot(p, x[:, n:n + 512]).astype(jnp.bfloat16)

    @pl.when(i == 0)
    def _():
        p = hot(el * TAIL, el * MAIN)
        for n in range(0, x.shape[1], 512):
            tail[:, n:n + 512] = _dot(p, x[:, n:n + 512])


def _gather(c, x, el, deps=()):
    tok, d = x.shape
    rows = el * MAIN // 2
    main, tail = pl.pallas_call(
        functools.partial(_gather_kernel, el),
        grid=(2,),
        out_shape=[jax.ShapeDtypeStruct((el * MAIN, d), jnp.bfloat16), jax.ShapeDtypeStruct((el * TAIL, d), jnp.float32)],
        in_specs=[pl.BlockSpec(c.shape, lambda i: (0, 0)), pl.BlockSpec((tok, d), lambda i: (0, 0))] + [ANY] * len(deps),
        out_specs=[pl.BlockSpec((rows, d), lambda i: (i, 0)), pl.BlockSpec((el * TAIL, d), lambda i: (0, 0))],
        compiler_params=_params(60),
        cost_estimate=pl.CostEstimate(flops=2 * el * CAP * tok * d, bytes_accessed=2 * el * CAP * d, transcendentals=0),
        name="gather",
    )(c, x, *deps)
    return main.reshape(el, MAIN, d), tail.reshape(el, TAIL, d)


def _gates_kernel(tab, g):
    blk, k3 = g.shape
    kt = k3 // 3
    lane = lax.broadcasted_iota(jnp.int32, (blk, kt), 1).astype(jnp.float32)
    acc = [jnp.zeros((blk, kt), jnp.float32) for _ in range(3)]
    for j in range(4):
        hit = tab[:, j:j + 1] == lane
        for i in range(3):
            acc[i] = jnp.where(hit, tab[:, 4 + 4 * i + j:5 + 4 * i + j], acc[i])
    for i in range(3):
        g[:, i * kt:(i + 1) * kt] = acc[i].astype(jnp.bfloat16)


def _gates(tab, kt):
    n = tab.shape[0]
    blk = 128
    return pl.pallas_call(
        _gates_kernel,
        grid=(n // blk,),
        out_shape=jax.ShapeDtypeStruct((n, 3 * kt), jnp.bfloat16),
        in_specs=[pl.BlockSpec((blk, tab.shape[1]), lambda i: (i, 0))],
        out_specs=pl.BlockSpec((blk, 3 * kt), lambda i: (i, 0)),
        compiler_params=_params(60),
        cost_estimate=pl.CostEstimate(flops=100 * n * kt, bytes_accessed=6 * n * kt, transcendentals=0),
        name="gates",
    )(tab)


def _up_kernel(*refs):
    m = refs[0:4]
    t = refs[4:8]
    w1, w3 = refs[8:10]
    h, xs = refs[-2:]
    for s in range(4):
        xs[s * MAIN:(s + 1) * MAIN, :] = m[s][0]
    xs[4 * MAIN:4 * CAP, :] = jnp.concatenate([t[s][0] for s in range(4)], axis=0).astype(jnp.bfloat16)
    f = h.shape[-1]
    full = f // 256 * 256
    x = xs[...]
    for n in range(0, full, 256):
        a = _dot(x, w1[0, :, n:n + 256])
        b = _dot(x, w3[0, :, n:n + 256])
        h[0, :, n:n + 256] = (jax.nn.silu(a) * b).astype(jnp.bfloat16)
    if full < f:
        r = f - full
        ab = _dot(x, jnp.concatenate([w1[0, :, full:], w3[0, :, full:]], axis=1))
        h[0, :, full:] = (jax.nn.silu(ab[:, :r]) * ab[:, r:]).astype(jnp.bfloat16)


def _up(mains, tails, w1, w3, deps=()):
    el, d, f = w1.shape
    spec = lambda a, b: pl.BlockSpec((1, a, b), lambda e: (e, 0, 0))
    return pl.pallas_call(
        _up_kernel,
        grid=(el,),
        out_shape=jax.ShapeDtypeStruct((el, 4 * CAP, f), jnp.bfloat16),
        in_specs=[spec(MAIN, d)] * 4 + [spec(TAIL, d)] * 4 + [spec(d, f)] * 2 + [ANY] * len(deps),
        out_specs=spec(4 * CAP, f),
        scratch_shapes=[pltpu.VMEM((4 * CAP, d), jnp.bfloat16)],
        compiler_params=_params(60),
        cost_estimate=pl.CostEstimate(flops=2 * 2 * el * 4 * CAP * d * f, bytes_accessed=4 * el * d * f, transcendentals=0),
        name="up",
    )(*mains, *tails, w1, w3, *deps)


def _route_kernel(el, tok, cols, g, h, w2, out, gv, hv, wv, r3, rt, send, recv, far, own, back,
                  gsem, hsem, wsem, ssem, rsem, xssem, xrsem, osem):
    me = lax.axis_index("ep")
    sib = me + 1 - 2 * lax.rem(me, 2)
    peer = lax.rem(me + 2, 4)
    ring = wv.shape[0]
    chunks = back.shape[0]
    kt = gv.shape[1] // 3
    nm = el * MAIN
    total = chunks * el

    gcopy = lambda s: pltpu.make_async_copy(g.at[pl.ds(s * tok, tok)], gv.at[pl.ds(s * tok, tok)], gsem.at[s])
    hcopy = lambda e: pltpu.make_async_copy(h.at[e], hv.at[e], hsem.at[e])

    def wcopy(t):
        slot = lax.rem(t, ring)
        col = pl.multiple_of(t // el * cols, cols)
        return pltpu.make_async_copy(w2.at[lax.rem(t, el), :, pl.ds(col, cols)], wv.at[slot], wsem.at[slot])

    def pair(c, k):
        return pltpu.make_async_remote_copy(send.at[lax.rem(c, 2), k], recv.at[c, k], ssem.at[c, k], rsem.at[c, k],
                                            device_id={"ep": sib}, device_id_type=pl.DeviceIdType.MESH)

    def across(c):
        return pltpu.make_async_remote_copy(recv.at[c, 1], back.at[c], xssem.at[c], xrsem.at[c],
                                            device_id={"ep": peer}, device_id_type=pl.DeviceIdType.MESH)

    def ocopy(c):
        return pltpu.make_async_copy(recv.at[c, 0], out.at[:, pl.ds(pl.multiple_of(c * cols, cols), cols)], osem.at[c])

    for t in range(ring):
        wcopy(jnp.int32(t)).start()
    for e in range(el):
        hcopy(e).start()
    for s in range(4):
        gcopy(s).start()
    barrier = pltpu.get_barrier_semaphore()
    for dev in (sib, peer):
        pl.semaphore_signal(barrier, inc=1, device_id={"ep": dev}, device_id_type=pl.DeviceIdType.MESH)
    pl.semaphore_wait(barrier, 2)

    def expert(c, e):
        t = c * el + e
        slot = lax.rem(t, ring)
        wcopy(t).wait()

        @pl.when(c == 0)
        def _():
            hcopy(e).wait()

        r = _dot(hv[e], wv[slot]).astype(jnp.bfloat16)
        row = pl.multiple_of(e * MAIN, MAIN)
        for s in range(4):
            for i in range(3):
                r3[s, pl.ds(row + i * kt, MAIN), :] = r[s * MAIN:(s + 1) * MAIN]
        q = r[4 * MAIN:].astype(jnp.float32)
        for s in range(4):
            rt[s, pl.ds(pl.multiple_of(e * TAIL, TAIL), TAIL), :] = q[s * TAIL:(s + 1) * TAIL]

        @pl.when(t + ring < total)
        def _():
            wcopy(t + ring).start()

    def combine(s):
        tail = jnp.concatenate([rt[s], jnp.zeros((kt - el * CAP, cols), jnp.float32)], axis=0).astype(jnp.bfloat16)
        for i in range(3):
            r3[s, i * kt + nm:(i + 1) * kt, :] = tail
        return _dot(gv[s * tok:(s + 1) * tok, :], r3[s])

    def chunk(c, _):
        def step(e, _):
            expert(c, e)
            return 0

        lax.fori_loop(0, el, step, 0)

        @pl.when(c == 0)
        def _():
            for s in range(4):
                gcopy(s).wait()

        @pl.when(c >= 2)
        def _():
            pair(c - 2, 0).wait_send()
            pair(c - 2, 1).wait_send()

        slot = lax.rem(c, 2)
        send[slot, 1] = combine(3)
        send[slot, 0] = combine(1)
        pair(c, 1).start()
        far[...] = combine(2)
        pair(c, 0).start()
        own[...] = combine(0)
        pair(c, 1).wait_recv()
        recv[c, 1] = recv[c, 1] + far[...]
        pair(c, 0).wait_recv()
        recv[c, 0] = recv[c, 0] + own[...]
        across(c).start()
        return 0

    lax.fori_loop(0, chunks, chunk, 0)

    def finish(c, _):
        across(c).wait_recv()
        recv[c, 0] = recv[c, 0] + back[c]
        ocopy(c).start()
        return 0

    lax.fori_loop(0, chunks, finish, 0)
    for c in range(chunks - 2, chunks):
        pair(jnp.int32(c), 0).wait_send()
        pair(jnp.int32(c), 1).wait_send()
    for c in range(chunks):
        across(jnp.int32(c)).wait_send()
        ocopy(jnp.int32(c)).wait()


def _route(g, h, w2, tok):
    el, f, d = w2.shape
    cols = 256
    chunks = d // cols
    ring = 8
    k3 = g.shape[1]
    f32 = jnp.float32
    return pl.pallas_call(
        functools.partial(_route_kernel, el, tok, cols),
        out_shape=jax.ShapeDtypeStruct((tok, d), f32),
        in_specs=[ANY] * 3,
        out_specs=ANY,
        scratch_shapes=[
            pltpu.VMEM((4 * tok, k3), jnp.bfloat16),
            pltpu.VMEM((el, 4 * CAP, f), jnp.bfloat16),
            pltpu.VMEM((ring, f, cols), jnp.bfloat16),
            pltpu.VMEM((4, k3, cols), jnp.bfloat16),
            pltpu.VMEM((4, el * TAIL, cols), f32),
            pltpu.VMEM((2, 2, tok, cols), f32),
            pltpu.VMEM((chunks, 2, tok, cols), f32),
            pltpu.VMEM((tok, cols), f32),
            pltpu.VMEM((tok, cols), f32),
            pltpu.VMEM((chunks, tok, cols), f32),
            pltpu.SemaphoreType.DMA((4,)),
            pltpu.SemaphoreType.DMA((el,)),
            pltpu.SemaphoreType.DMA((ring,)),
            pltpu.SemaphoreType.DMA((chunks, 2)),
            pltpu.SemaphoreType.DMA((chunks, 2)),
            pltpu.SemaphoreType.DMA((chunks,)),
            pltpu.SemaphoreType.DMA((chunks,)),
            pltpu.SemaphoreType.DMA((chunks,)),
        ],
        compiler_params=pltpu.CompilerParams(vmem_limit_bytes=63 * MIB, collective_id=0, has_side_effects=True),
        cost_estimate=pl.CostEstimate(flops=2 * el * 4 * CAP * f * d + 8 * tok * k3 * d,
                                      bytes_accessed=2 * el * f * d + 2 * el * 4 * CAP * f, transcendentals=0),
        name="route",
    )(g, h, w2)


def solution(mesh):
    rows = P(("ep", "tp"), None)

    def perm(a, axis, k=1):
        return lax.ppermute(a, axis, [(i, i ^ k) for i in range(mesh.shape[axis])])

    def body(x, idx, g, slot, ws1, ws3, ws2, w1, w3, w2):
        tok, _ = x.shape
        el = w1.shape[0]
        kt = -(-el * CAP // 16) * 16
        me = lax.axis_index("ep")
        bf = lambda a: lax.reduce_precision(a, 8, 7)

        code = jnp.where(slot >= 0, idx * 128 + slot, -1).astype(jnp.float32)
        mine = jnp.concatenate([code, g], axis=1).T
        tabs = (mine,) + tuple(perm(mine, "ep", k) for k in (1, 2, 3))
        xx = perm(x, "ep", 2)
        xy = perm(x, "tp")
        xc = perm(x, "ep", 1)
        xxc = perm(xx, "ep", 1)

        cs, cols = [], []
        for s in range(4):
            code = tabs[s][:4].astype(jnp.int32)
            gs = tabs[s][4:]
            e, k = code >> 7, code & 127
            le = e - me * el
            ok = (code >= 0) & (le >= 0) & (le < el)
            c = jnp.where(ok, jnp.where(k < MAIN, le * MAIN + k, el * MAIN + le * TAIL + k - MAIN), -1).astype(jnp.float32)
            g0 = bf(gs)
            g1 = bf(gs - g0)
            g2 = gs - g0 - g1
            cs.append(c)
            cols.append(jnp.concatenate([c, g0, g1, g2], axis=0))
        tab = jnp.concatenate(cols, axis=1).T

        m0, t0 = _gather(cs[0], x, el)
        so = _shared(x, ws1, ws3, ws2, (t0,))
        gm = _gates(tab, kt)
        m1, t1 = _gather(cs[1], xc, el, (so, gm))
        m2, t2 = _gather(cs[2], xx, el, (t1,))
        sy = _shared(xy, ws1, ws3, ws2, (t2,))
        sy = perm(sy, "tp")
        m3, t3 = _gather(cs[3], xxc, el, (t2,))
        h = _up((m0, m1, m2, m3), (t0, t1, t2, t3), w1, w3)
        r = _route(gm, h, w2, tok)
        return (x.astype(jnp.float32) + (so + sy) + r).astype(jnp.bfloat16)

    return jax.shard_map(
        body, mesh=mesh,
        in_specs=(rows, rows, rows, rows, P(None, "tp"), P(None, "tp"), P("tp", None),
                  P("ep", None, None), P("ep", None, None), P("ep", None, None)),
        out_specs=rows, check_vma=False)
```

```python
import functools

import jax
import jax.numpy as jnp
from jax import lax
from jax.experimental import pallas as pl
from jax.experimental.pallas import tpu as pltpu
from jax.sharding import PartitionSpec as P

CAP = 72
MAIN = 64
TAIL = CAP - MAIN
MIB = 1024 * 1024
ANY = pl.BlockSpec(memory_space=pl.ANY)


def _params(mib):
    return pltpu.CompilerParams(vmem_limit_bytes=mib * MIB)


def _dot(a, b):
    return jnp.dot(a, b, preferred_element_type=jnp.float32)


def _shared_kernel(nf, nn, x, w1, w3, w2, *rest):
    o, v1, v3, v2, h, s1, s3, s2 = rest[-8:]
    tf, tn = v1.shape[2], v2.shape[2]
    up = lambda w, v, s, i: pltpu.make_async_copy(w.at[:, pl.ds(pl.multiple_of(i * tf, tf), tf)], v.at[i], s.at[i])
    down = lambda i: pltpu.make_async_copy(w2.at[:, pl.ds(pl.multiple_of(i * tn, tn), tn)], v2.at[i], s2.at[i])
    for i in range(nf):
        up(w1, v1, s1, i).start()
        up(w3, v3, s3, i).start()
    for i in range(nn):
        down(i).start()

    def gate(i, _):
        up(w1, v1, s1, i).wait()
        up(w3, v3, s3, i).wait()
        a = _dot(x[...], v1[i])
        b = _dot(x[...], v3[i])
        h[:, pl.ds(pl.multiple_of(i * tf, tf), tf)] = (jax.nn.silu(a) * b).astype(jnp.bfloat16)
        return 0

    def out(i, _):
        down(i).wait()
        o[:, pl.ds(pl.multiple_of(i * tn, tn), tn)] = _dot(h[...], v2[i])
        return 0

    lax.fori_loop(0, nf, gate, 0)
    lax.fori_loop(0, nn, out, 0)


def _shared(x, w1, w3, w2, deps=()):
    m, d = x.shape
    f = w1.shape[1]
    tf, tn = 256, 512
    nf, nn = f // tf, d // tn
    vmem = pl.BlockSpec(memory_space=pltpu.VMEM)
    return pl.pallas_call(
        functools.partial(_shared_kernel, nf, nn),
        out_shape=jax.ShapeDtypeStruct((m, d), jnp.float32),
        in_specs=[vmem] + [ANY] * (3 + len(deps)),
        out_specs=vmem,
        scratch_shapes=[
            pltpu.VMEM((nf, d, tf), jnp.bfloat16),
            pltpu.VMEM((nf, d, tf), jnp.bfloat16),
            pltpu.VMEM((nn, f, tn), jnp.bfloat16),
            pltpu.VMEM((m, f), jnp.bfloat16),
            pltpu.SemaphoreType.DMA((nf,)),
            pltpu.SemaphoreType.DMA((nf,)),
            pltpu.SemaphoreType.DMA((nn,)),
        ],
        compiler_params=_params(60),
        cost_estimate=pl.CostEstimate(flops=6 * m * d * f, bytes_accessed=6 * d * f, transcendentals=0),
        name="shared",
    )(x, w1, w3, w2, *deps)


def _hot(c, n, base, tok):
    r = (lax.broadcasted_iota(jnp.int32, (n, tok), 0) + base).astype(jnp.float32)
    hit = r == c[0:1, :]
    for j in range(1, 4):
        hit = hit | (r == c[j:j + 1, :])
    return jnp.where(hit, 1.0, 0.0).astype(jnp.bfloat16)


def _gather_kernel(el, c, x, *rest):
    main, tail = rest[-2:]
    i = pl.program_id(0)
    tok = x.shape[0]
    rows = main.shape[0]
    p = _hot(c, rows, i * rows, tok)
    for n in range(0, x.shape[1], 512):
        main[:, n:n + 512] = _dot(p, x[:, n:n + 512]).astype(jnp.bfloat16)

    @pl.when(i == 0)
    def _():
        p = _hot(c, el * TAIL, el * MAIN, tok)
        for n in range(0, x.shape[1], 512):
            tail[:, n:n + 512] = _dot(p, x[:, n:n + 512])


def _gather(c, x, el, deps=()):
    tok, d = x.shape
    rows = el * MAIN // 2
    main, tail = pl.pallas_call(
        functools.partial(_gather_kernel, el),
        grid=(2,),
        out_shape=[jax.ShapeDtypeStruct((el * MAIN, d), jnp.bfloat16), jax.ShapeDtypeStruct((el * TAIL, d), jnp.float32)],
        in_specs=[pl.BlockSpec(c.shape, lambda i: (0, 0)), pl.BlockSpec((tok, d), lambda i: (0, 0))] + [ANY] * len(deps),
        out_specs=[pl.BlockSpec((rows, d), lambda i: (i, 0)), pl.BlockSpec((el * TAIL, d), lambda i: (0, 0))],
        compiler_params=_params(60),
        cost_estimate=pl.CostEstimate(flops=2 * el * CAP * tok * d, bytes_accessed=2 * el * CAP * d, transcendentals=0),
        name="gather",
    )(c, x, *deps)
    return main.reshape(el, MAIN, d), tail.reshape(el, TAIL, d)


def _gates_kernel(tab, g):
    blk, k3 = g.shape
    kt = k3 // 3
    lane = lax.broadcasted_iota(jnp.int32, (blk, kt), 1).astype(jnp.float32)
    acc = [jnp.zeros((blk, kt), jnp.float32) for _ in range(3)]
    for j in range(4):
        hit = tab[:, j:j + 1] == lane
        for i in range(3):
            acc[i] = jnp.where(hit, tab[:, 4 + 4 * i + j:5 + 4 * i + j], acc[i])
    for i in range(3):
        g[:, i * kt:(i + 1) * kt] = acc[i].astype(jnp.bfloat16)


def _gates(tab, kt):
    n = tab.shape[0]
    blk = 128
    return pl.pallas_call(
        _gates_kernel,
        grid=(n // blk,),
        out_shape=jax.ShapeDtypeStruct((n, 3 * kt), jnp.bfloat16),
        in_specs=[pl.BlockSpec((blk, tab.shape[1]), lambda i: (i, 0))],
        out_specs=pl.BlockSpec((blk, 3 * kt), lambda i: (i, 0)),
        compiler_params=_params(60),
        cost_estimate=pl.CostEstimate(flops=100 * n * kt, bytes_accessed=6 * n * kt, transcendentals=0),
        name="gates",
    )(tab)


def _up_kernel(el, m0, m1, t0, t1, c2, c3, x2, x3, w1h, w3h, h, xs, mg, tg, v1, v3, sem):
    e = pl.program_id(0)
    tok, d = x2.shape
    ring = v1.shape[0]

    def weights(i):
        k = lax.rem(i, ring)
        return (pltpu.make_async_copy(w1h.at[i], v1.at[k], sem.at[0, k]), pltpu.make_async_copy(w3h.at[i], v3.at[k], sem.at[1, k]))

    @pl.when(e == 0)
    def _():
        for i in range(ring):
            for c in weights(jnp.int32(i)):
                c.start()

    @pl.when(e == 0)
    def _():
        for k, (c, x) in enumerate(((c2, x2), (c3, x3))):
            rows = el * MAIN // 2
            for b in range(2):
                p = _hot(c, rows, b * rows, tok)
                for n in range(0, d, 512):
                    mg[k, b * rows:(b + 1) * rows, n:n + 512] = _dot(p, x[:, n:n + 512]).astype(jnp.bfloat16)
            p = _hot(c, el * TAIL, el * MAIN, tok)
            for n in range(0, d, 512):
                tg[k, :, n:n + 512] = _dot(p, x[:, n:n + 512])

    row = pl.ds(pl.multiple_of(e * MAIN, MAIN), MAIN)
    tail = pl.ds(pl.multiple_of(e * TAIL, TAIL), TAIL)
    xs[0:MAIN, :] = m0[0]
    xs[MAIN:2 * MAIN, :] = m1[0]
    xs[2 * MAIN:3 * MAIN, :] = mg[0, row, :]
    xs[3 * MAIN:4 * MAIN, :] = mg[1, row, :]
    xs[4 * MAIN:4 * CAP, :] = jnp.concatenate([t0[0], t1[0], tg[0, tail, :], tg[1, tail, :]], axis=0).astype(jnp.bfloat16)
    f = h.shape[-1]
    full = f // 256 * 256
    for c in weights(e):
        c.wait()
    x = xs[...]
    w1, w3 = v1.at[lax.rem(e, ring)], v3.at[lax.rem(e, ring)]
    for n in range(0, full, 256):
        a = _dot(x, w1[:, n:n + 256])
        b = _dot(x, w3[:, n:n + 256])
        h[0, :, n:n + 256] = (jax.nn.silu(a) * b).astype(jnp.bfloat16)
    if full < f:
        r = f - full
        ab = _dot(x, jnp.concatenate([w1[:, full:], w3[:, full:]], axis=1))
        h[0, :, full:] = (jax.nn.silu(ab[:, :r]) * ab[:, r:]).astype(jnp.bfloat16)

    @pl.when(e + ring < el)
    def _():
        for c in weights(e + ring):
            c.start()


def _up(mains, tails, cs, xs, w1, w3):
    el, d, f = w1.shape
    spec = lambda a, b, **k: pl.BlockSpec((1, a, b), lambda e: (e, 0, 0), **k)
    once = lambda a: pl.BlockSpec(a.shape, lambda e: (0, 0), pipeline_mode=pl.Buffered(1))
    return pl.pallas_call(
        functools.partial(_up_kernel, el),
        grid=(el,),
        out_shape=jax.ShapeDtypeStruct((el, 4 * CAP, f), jnp.bfloat16),
        in_specs=[spec(MAIN, d)] * 2 + [spec(TAIL, d)] * 2 + [once(cs[0])] * 2 + [once(xs[0])] * 2
        + [ANY] * 2,
        out_specs=spec(4 * CAP, f),
        scratch_shapes=[
            pltpu.VMEM((4 * CAP, d), jnp.bfloat16),
            pltpu.VMEM((2, el * MAIN, d), jnp.bfloat16),
            pltpu.VMEM((2, el * TAIL, d), jnp.float32),
            pltpu.VMEM((3, d, f), jnp.bfloat16),
            pltpu.VMEM((3, d, f), jnp.bfloat16),
            pltpu.SemaphoreType.DMA((2, 3)),
        ],
        compiler_params=_params(63),
        cost_estimate=pl.CostEstimate(flops=2 * 2 * el * 4 * CAP * d * f, bytes_accessed=4 * el * d * f, transcendentals=0),
        name="up",
    )(*mains, *tails, *cs, *xs, w1, w3)


def _route_kernel(el, tok, cols, g, h, w2, x, ws1, ws3, ws2, out, send, recv, far, own, back,
                  gsem, hsem, wsem, ssem, rsem, xssem, xrsem, osem, usem):
    bf16 = jnp.bfloat16
    d = x.shape[1]
    fs = ws1.shape[1]
    k3 = g.shape[1]
    pl.run_scoped(
        functools.partial(_route_chunks, el, tok, cols, g, h, w2, send, recv, far, own, back,
                          gsem, hsem, wsem, ssem, rsem, xssem, xrsem),
        pltpu.VMEM((4 * tok, k3), bf16),
        pltpu.VMEM(h.shape, bf16),
        pltpu.VMEM((wsem.shape[0], h.shape[2], cols), bf16),
        pltpu.VMEM((4, k3, cols), bf16),
        pltpu.VMEM((4, el * TAIL, cols), jnp.float32),
    )
    pl.run_scoped(
        functools.partial(_route_shared, cols, x, ws1, ws3, ws2, recv, usem),
        pltpu.VMEM(x.shape, bf16),
        pltpu.VMEM((fs // 256, d, 256), bf16),
        pltpu.VMEM((fs // 256, d, 256), bf16),
        pltpu.VMEM((d // cols, fs, cols), bf16),
        pltpu.VMEM((tok, fs), bf16),
    )
    peer = lax.rem(lax.axis_index("ep") + 2, 4)
    chunks = back.shape[0]

    def across(c):
        return pltpu.make_async_remote_copy(recv.at[c, 1], back.at[c], xssem.at[c], xrsem.at[c],
                                            device_id={"ep": peer}, device_id_type=pl.DeviceIdType.MESH)

    def ocopy(c):
        return pltpu.make_async_copy(recv.at[c, 0], out.at[:, pl.ds(pl.multiple_of(c * cols, cols), cols)], osem.at[c])

    def finish(c, _):
        across(c).wait_recv()
        recv[c, 0] = recv[c, 0] + back[c]
        ocopy(c).start()
        return 0

    lax.fori_loop(0, chunks, finish, 0)
    for c in range(chunks):
        across(jnp.int32(c)).wait_send()
        ocopy(jnp.int32(c)).wait()


def _route_shared(cols, x, w1, w3, w2, recv, usem, xv, v1, v3, v2, h):
    nf, nn = v1.shape[0], v2.shape[0]
    tf = v1.shape[2]
    xcopy = pltpu.make_async_copy(x, xv, usem.at[2 * nf + nn])

    def up(i):
        col = pl.ds(pl.multiple_of(i * tf, tf), tf)
        return (pltpu.make_async_copy(w1.at[:, col], v1.at[i], usem.at[i]),
                pltpu.make_async_copy(w3.at[:, col], v3.at[i], usem.at[nf + i]))

    def down(i):
        return pltpu.make_async_copy(w2.at[:, pl.ds(pl.multiple_of(i * cols, cols), cols)], v2.at[i], usem.at[2 * nf + i])

    xcopy.start()
    for i in range(nf):
        for c in up(i):
            c.start()
    for i in range(nn):
        down(i).start()
    xcopy.wait()

    def gate(i, _):
        for c in up(i):
            c.wait()
        a = _dot(xv[...], v1[i])
        b = _dot(xv[...], v3[i])
        h[:, pl.ds(pl.multiple_of(i * tf, tf), tf)] = (jax.nn.silu(a) * b).astype(jnp.bfloat16)
        return 0

    def add(i, _):
        down(i).wait()
        s = _dot(h[...], v2[i])
        recv[i, 0] = recv[i, 0] + (xv[:, pl.ds(pl.multiple_of(i * cols, cols), cols)].astype(jnp.float32) + s)
        return 0

    lax.fori_loop(0, nf, gate, 0)
    lax.fori_loop(0, nn, add, 0)


def _route_chunks(el, tok, cols, g, h, w2, send, recv, far, own, back,
                  gsem, hsem, wsem, ssem, rsem, xssem, xrsem, gv, hv, wv, r3, rt):
    me = lax.axis_index("ep")
    sib = me + 1 - 2 * lax.rem(me, 2)
    peer = lax.rem(me + 2, 4)
    ring = wv.shape[0]
    chunks = back.shape[0]
    kt = gv.shape[1] // 3
    nm = el * MAIN
    total = chunks * el

    gcopy = lambda s: pltpu.make_async_copy(g.at[pl.ds(s * tok, tok)], gv.at[pl.ds(s * tok, tok)], gsem.at[s])
    hcopy = lambda e: pltpu.make_async_copy(h.at[e], hv.at[e], hsem.at[e])

    def wcopy(t):
        slot = lax.rem(t, ring)
        col = pl.multiple_of(t // el * cols, cols)
        return pltpu.make_async_copy(w2.at[lax.rem(t, el), :, pl.ds(col, cols)], wv.at[slot], wsem.at[slot])

    def pair(c, k):
        return pltpu.make_async_remote_copy(send.at[lax.rem(c, 2), k], recv.at[c, k], ssem.at[c, k], rsem.at[c, k],
                                            device_id={"ep": sib}, device_id_type=pl.DeviceIdType.MESH)

    def across(c):
        return pltpu.make_async_remote_copy(recv.at[c, 1], back.at[c], xssem.at[c], xrsem.at[c],
                                            device_id={"ep": peer}, device_id_type=pl.DeviceIdType.MESH)

    for t in range(ring):
        wcopy(jnp.int32(t)).start()
    for e in range(el):
        hcopy(e).start()
    for s in range(4):
        gcopy(s).start()
    barrier = pltpu.get_barrier_semaphore()
    for dev in (sib, peer):
        pl.semaphore_signal(barrier, inc=1, device_id={"ep": dev}, device_id_type=pl.DeviceIdType.MESH)
    pl.semaphore_wait(barrier, 2)

    def expert(c, e):
        t = c * el + e
        slot = lax.rem(t, ring)
        wcopy(t).wait()

        @pl.when(c == 0)
        def _():
            hcopy(e).wait()

        r = _dot(hv[e], wv[slot]).astype(jnp.bfloat16)
        row = pl.multiple_of(e * MAIN, MAIN)
        for s in range(4):
            for i in range(3):
                r3[s, pl.ds(row + i * kt, MAIN), :] = r[s * MAIN:(s + 1) * MAIN]
        q = r[4 * MAIN:].astype(jnp.float32)
        for s in range(4):
            rt[s, pl.ds(pl.multiple_of(e * TAIL, TAIL), TAIL), :] = q[s * TAIL:(s + 1) * TAIL]

        @pl.when(t + ring < total)
        def _():
            wcopy(t + ring).start()

    def combine(s):
        tail = jnp.concatenate([rt[s], jnp.zeros((kt - el * CAP, cols), jnp.float32)], axis=0).astype(jnp.bfloat16)
        for i in range(3):
            r3[s, i * kt + nm:(i + 1) * kt, :] = tail
        return _dot(gv[s * tok:(s + 1) * tok, :], r3[s])

    def chunk(c, _):
        def step(e, _):
            expert(c, e)
            return 0

        lax.fori_loop(0, el, step, 0)

        @pl.when(c == 0)
        def _():
            for s in range(4):
                gcopy(s).wait()

        @pl.when(c >= 2)
        def _():
            pair(c - 2, 0).wait_send()
            pair(c - 2, 1).wait_send()

        slot = lax.rem(c, 2)
        send[slot, 1] = combine(3)
        send[slot, 0] = combine(1)
        pair(c, 1).start()
        far[...] = combine(2)
        pair(c, 0).start()
        own[...] = combine(0)
        pair(c, 1).wait_recv()
        recv[c, 1] = recv[c, 1] + far[...]
        pair(c, 0).wait_recv()
        recv[c, 0] = recv[c, 0] + own[...]
        across(c).start()
        return 0

    lax.fori_loop(0, chunks, chunk, 0)

    for c in range(chunks - 2, chunks):
        pair(jnp.int32(c), 0).wait_send()
        pair(jnp.int32(c), 1).wait_send()


def _route(g, h, w2, x, ws1, ws3, ws2):
    el, f, d = w2.shape
    tok = x.shape[0]
    fs = ws1.shape[1]
    cols = 256
    chunks = d // cols
    ring = 8
    k3 = g.shape[1]
    f32 = jnp.float32
    return pl.pallas_call(
        functools.partial(_route_kernel, el, tok, cols),
        out_shape=jax.ShapeDtypeStruct((tok, d), f32),
        in_specs=[ANY] * 7,
        out_specs=ANY,
        scratch_shapes=[
            pltpu.VMEM((2, 2, tok, cols), f32),
            pltpu.VMEM((chunks, 2, tok, cols), f32),
            pltpu.VMEM((tok, cols), f32),
            pltpu.VMEM((tok, cols), f32),
            pltpu.VMEM((chunks, tok, cols), f32),
            pltpu.SemaphoreType.DMA((4,)),
            pltpu.SemaphoreType.DMA((el,)),
            pltpu.SemaphoreType.DMA((ring,)),
            pltpu.SemaphoreType.DMA((chunks, 2)),
            pltpu.SemaphoreType.DMA((chunks, 2)),
            pltpu.SemaphoreType.DMA((chunks,)),
            pltpu.SemaphoreType.DMA((chunks,)),
            pltpu.SemaphoreType.DMA((chunks,)),
            pltpu.SemaphoreType.DMA((fs // 256 * 2 + chunks + 1,)),
        ],
        compiler_params=pltpu.CompilerParams(vmem_limit_bytes=63 * MIB, collective_id=0, has_side_effects=True),
        cost_estimate=pl.CostEstimate(flops=2 * el * 4 * CAP * f * d + 8 * tok * k3 * d + 6 * tok * d * fs,
                                      bytes_accessed=2 * el * f * d + 2 * el * 4 * CAP * f, transcendentals=0),
        name="route",
    )(g, h, w2, x, ws1, ws3, ws2)


def solution(mesh):
    rows = P(("ep", "tp"), None)

    def perm(a, axis, k=1):
        return lax.ppermute(a, axis, [(i, i ^ k) for i in range(mesh.shape[axis])])

    def body(x, idx, g, slot, ws1, ws3, ws2, w1, w3, w2):
        tok, _ = x.shape
        el = w1.shape[0]
        kt = -(-el * CAP // 16) * 16
        me = lax.axis_index("ep")
        bf = lambda a: lax.reduce_precision(a, 8, 7)

        code = jnp.where(slot >= 0, idx * 128 + slot, -1).astype(jnp.float32)
        mine = jnp.concatenate([code, g], axis=1).T
        tabs = (mine,) + tuple(perm(mine, "ep", k) for k in (1, 2, 3))
        xx = perm(x, "ep", 2)
        half = tok // 2
        y0 = perm(x[:half], "tp")
        y1 = perm(x[half:], "tp")
        xc = perm(x, "ep", 1)
        xxc = perm(xx, "ep", 1)

        cs, cols = [], []
        for s in range(4):
            code = tabs[s][:4].astype(jnp.int32)
            gs = tabs[s][4:]
            e, k = code >> 7, code & 127
            le = e - me * el
            ok = (code >= 0) & (le >= 0) & (le < el)
            c = jnp.where(ok, jnp.where(k < MAIN, le * MAIN + k, el * MAIN + le * TAIL + k - MAIN), -1).astype(jnp.float32)
            g0 = bf(gs)
            g1 = bf(gs - g0)
            g2 = gs - g0 - g1
            cs.append(c)
            cols.append(jnp.concatenate([c, g0, g1, g2], axis=0))
        tab = jnp.concatenate(cols, axis=1).T

        m0, t0 = _gather(cs[0], x, el)
        gm = _gates(tab, kt)
        m1, t1 = _gather(cs[1], xc, el, (t0, gm))
        s0 = _shared(y0, ws1, ws3, ws2, (t1,))
        r0 = perm(s0, "tp")
        s1 = _shared(y1, ws1, ws3, ws2, (s0,))
        r1 = perm(s1, "tp")
        h = _up((m0, m1), (t0, t1), cs[2:], (xx, xxc), w1, w3)
        r = _route(gm, h, w2, x, ws1, ws3, ws2)
        return (jnp.concatenate([r0, r1], axis=0) + r).astype(jnp.bfloat16)

    return jax.shard_map(
        body, mesh=mesh,
        in_specs=(rows, rows, rows, rows, P(None, "tp"), P(None, "tp"), P("tp", None),
                  P("ep", None, None), P("ep", None, None), P("ep", None, None)),
        out_specs=rows, check_vma=False)
```

```python
import functools

import jax
import jax.numpy as jnp
from jax import lax
from jax.experimental import pallas as pl
from jax.experimental.pallas import tpu as pltpu
from jax.sharding import PartitionSpec as P

CAP = 72
MAIN = 64
TAIL = CAP - MAIN
MIB = 1024 * 1024
ANY = pl.BlockSpec(memory_space=pl.ANY)


def _params(mib):
    return pltpu.CompilerParams(vmem_limit_bytes=mib * MIB)


def _dot(a, b):
    return jnp.dot(a, b, preferred_element_type=jnp.float32)


def _hot(c, n, base, tok):
    r = (lax.broadcasted_iota(jnp.int32, (n, tok), 0) + base).astype(jnp.float32)
    hit = r == c[0:1, :]
    for j in range(1, 4):
        hit = hit | (r == c[j:j + 1, :])
    return jnp.where(hit, 1.0, 0.0).astype(jnp.bfloat16)


def _codes(t, me, el):
    code = t[0:4, :].astype(jnp.int32)
    e, k = code >> 7, code & 127
    le = e - me * el
    ok = (code >= 0) & (le >= 0) & (le < el)
    c = jnp.where(ok, jnp.where(k < MAIN, le * MAIN + k, el * MAIN + le * TAIL + k - MAIN), -1).astype(jnp.float32)
    g = t[4:8, :]
    g0 = g.astype(jnp.bfloat16).astype(jnp.float32)
    g1 = (g - g0).astype(jnp.bfloat16).astype(jnp.float32)
    return c, jnp.concatenate([c, g0, g1, g - g0 - g1], axis=0)


def _front_kernel(el, kt, x, mine, w1, w3, w2, cx, gm, base, sy, xc, xx, xxc,
                  y, tabs, tabt, v1, v3, v2, hs, sst, gst, wsem, xsend, xrecv, tsend, trecv, ssem, gsem):
    me = lax.axis_index("ep")
    tp = lax.axis_index("tp")
    sib = me + 1 - 2 * lax.rem(me, 2)
    peer = lax.rem(me + 2, 4)
    diag = lax.rem(sib + 2, 4)
    tok, d = x.shape
    half = tok // 2
    nf, nn = v1.shape[0], v2.shape[0]
    tf, tn = v1.shape[2], v2.shape[2]
    mesh_id = pl.DeviceIdType.MESH

    def remote(src, dst, ss, rs, dev):
        return pltpu.make_async_remote_copy(src, dst, ss, rs, device_id=dev, device_id_type=mesh_id)

    def up(i):
        col = pl.ds(pl.multiple_of(i * tf, tf), tf)
        return (pltpu.make_async_copy(w1.at[:, col], v1.at[i], wsem.at[i]),
                pltpu.make_async_copy(w3.at[:, col], v3.at[i], wsem.at[nf + i]))

    def down(i):
        return pltpu.make_async_copy(w2.at[:, pl.ds(pl.multiple_of(i * tn, tn), tn)], v2.at[i], wsem.at[2 * nf + i])

    barrier = pltpu.get_barrier_semaphore()
    for dev in (sib, peer, diag):
        pl.semaphore_signal(barrier, inc=1, device_id={"ep": dev}, device_id_type=mesh_id)
    pl.semaphore_signal(barrier, inc=1, device_id={"tp": 1 - tp}, device_id_type=mesh_id)
    pl.semaphore_wait(barrier, 4)
    tcopy = [remote(mine, tabs.at[k], tsend.at[k], trecv.at[k], {"ep": dev}) for k, dev in enumerate((sib, peer, diag))]
    xcopy = remote(x, xx, xsend.at[0], xrecv.at[0], {"ep": peer})
    ccopy = remote(x, xc, xsend.at[1], xrecv.at[1], {"ep": sib})
    ycopy = [remote(x.at[pl.ds(k * half, half)], y.at[pl.ds(k * half, half)], xsend.at[2 + k], xrecv.at[2 + k], {"tp": 1 - tp})
             for k in range(2)]
    relay = remote(xx, xxc, xsend.at[4], xrecv.at[4], {"ep": sib})
    for c in (*tcopy, xcopy, *ycopy, ccopy):
        c.start()
    for i in range(nf):
        for c in up(i):
            c.start()
    for i in range(nn):
        down(i).start()

    def store_tab(s, tab):
        wide = jnp.concatenate([tab, jnp.zeros((128 - tab.shape[0], tok), jnp.float32)], axis=0)
        for b in range(0, tok, 128):
            tabt[s * tok + b:s * tok + b + 128, :] = jnp.transpose(wide[:, b:b + 128])

    def shared(src, lo, n, out, add, first):
        scopy = lambda i: pltpu.make_async_copy(
            sst.at[lax.rem(i, 2), pl.ds(0, n)], out.at[pl.ds(lo, n), pl.ds(pl.multiple_of(i * tn, tn), tn)], ssem.at[lax.rem(i, 2)])

        def gate(i, _):
            if first:
                for c in up(i):
                    c.wait()
            r = src[lo:lo + n, :]
            a = _dot(r, v1[i])
            b = _dot(r, v3[i])
            hs[lo:lo + n, pl.ds(pl.multiple_of(i * tf, tf), tf)] = (jax.nn.silu(a) * b).astype(jnp.bfloat16)
            return 0

        def tile(i, _):
            if first:
                down(i).wait()

            @pl.when(i >= 2)
            def _():
                scopy(i - 2).wait()

            r = _dot(hs[lo:lo + n, :], v2[i])
            if add:
                r = r + src[lo:lo + n, pl.ds(pl.multiple_of(i * tn, tn), tn)].astype(jnp.float32)
            sst[lax.rem(i, 2), 0:n, :] = r
            scopy(i).start()
            return 0

        lax.fori_loop(0, nf, gate, 0)
        lax.fori_loop(0, nn, tile, 0)
        for i in (nn - 2, nn - 1):
            scopy(jnp.int32(i)).wait()

    shared(x, 0, tok, base, True, True)
    for k in range(4):
        if k:
            tcopy[k - 1].wait()
        c, tab = _codes(mine[...] if k == 0 else tabs[k - 1], me, el)
        cx[k] = jnp.concatenate([c, c], axis=0)
        store_tab(k, tab)

    blk = gst.shape[1]
    gcopy = lambda i: pltpu.make_async_copy(gst.at[lax.rem(i, 2)], gm.at[pl.ds(pl.multiple_of(i * blk, blk), blk)], gsem.at[lax.rem(i, 2)])

    def gates(i, _):
        @pl.when(i >= 2)
        def _():
            gcopy(i - 2).wait()

        t = tabt[pl.ds(pl.multiple_of(i * blk, blk), blk), :]
        lane = lax.broadcasted_iota(jnp.int32, (blk, kt), 1).astype(jnp.float32)
        acc = [jnp.zeros((blk, kt), jnp.float32) for _ in range(3)]
        for j in range(4):
            hit = t[:, j:j + 1] == lane
            for q in range(3):
                acc[q] = jnp.where(hit, t[:, 4 + 4 * q + j:5 + 4 * q + j], acc[q])
        for q in range(3):
            gst[lax.rem(i, 2), :, q * kt:(q + 1) * kt] = acc[q].astype(jnp.bfloat16)
        gcopy(i).start()
        return 0

    ng = 4 * tok // blk
    lax.fori_loop(0, ng, gates, 0)
    for i in (ng - 2, ng - 1):
        gcopy(jnp.int32(i)).wait()
    ycopy[0].wait()
    shared(y, 0, half, sy, False, False)
    xcopy.wait()
    relay.start()
    ycopy[1].wait()
    shared(y, half, half, sy, False, False)
    ccopy.wait()
    relay.wait()


def _front(x, mine, w1, w3, w2, el, kt):
    tok, d = x.shape
    f = w1.shape[1]
    tf, tn = 256, 256
    nf, nn = f // tf, d // tn
    bf16, f32 = jnp.bfloat16, jnp.float32
    vmem = pl.BlockSpec(memory_space=pltpu.VMEM)
    dma = pltpu.SemaphoreType.DMA
    return pl.pallas_call(
        functools.partial(_front_kernel, el, kt),
        out_shape=[jax.ShapeDtypeStruct(sh, dt) for sh, dt in (
            ((4, 8, tok), f32), ((4 * tok, 3 * kt), bf16), ((tok, d), f32), ((tok, d), f32),
            ((tok, d), bf16), ((tok, d), bf16), ((tok, d), bf16))],
        in_specs=[vmem, vmem] + [ANY] * 3,
        out_specs=[vmem] + [ANY] * 6,
        scratch_shapes=[
            pltpu.VMEM((tok, d), bf16),
            pltpu.VMEM((3, 8, tok), f32),
            pltpu.VMEM((4 * tok, 128), f32),
            pltpu.VMEM((nf, d, tf), bf16),
            pltpu.VMEM((nf, d, tf), bf16),
            pltpu.VMEM((nn, f, tn), bf16),
            pltpu.VMEM((tok, f), bf16),
            pltpu.VMEM((2, tok, tn), f32),
            pltpu.VMEM((2, 128, 3 * kt), bf16),
            dma((2 * nf + nn,)), dma((5,)), dma((5,)), dma((3,)), dma((3,)), dma((2,)), dma((2,)),
        ],
        compiler_params=pltpu.CompilerParams(vmem_limit_bytes=62 * MIB, collective_id=1, has_side_effects=True),
        cost_estimate=pl.CostEstimate(flops=12 * tok * d * f, bytes_accessed=6 * d * f, transcendentals=0),
        name="front",
    )(x, mine, w1, w3, w2)


def _up_kernel(el, x0, x1, x2, x3, cx, w1, w3, h, xs, tg, xb, wv, xsem, wsem):
    e = pl.program_id(0)
    tok, d = x0.shape
    ring = wv.shape[0]
    srcs = (x0, x1, x2, x3)
    some = 5

    def wcopy(w, i, k):
        slot = lax.rem(2 * i + k, ring)
        return pltpu.make_async_copy(w.at[i], wv.at[slot], wsem.at[slot])

    xcopy = lambda s, k: pltpu.make_async_copy(srcs[s], xb.at[k], xsem.at[k])

    @pl.when(e == 0)
    def _():
        xcopy(0, 0).start()
        xcopy(1, 1).start()
        for i in range(ring):
            wcopy(w3 if i % 2 else w1, jnp.int32(i // 2), i % 2).start()

        def select(s, _):
            k = lax.rem(s, 2)
            xcopy(0, k).wait()
            c = cx[s]
            for b in range(0, el, some):
                p = _hot(c, some * MAIN, b * MAIN, tok)
                for n in range(0, d, 512):
                    r = _dot(p, xb[k, :, n:n + 512]).astype(jnp.bfloat16)
                    for i in range(some):
                        xs[b + i, pl.ds(pl.multiple_of(s * MAIN, MAIN), MAIN), n:n + 512] = r[i * MAIN:(i + 1) * MAIN]
            p = _hot(c, el * TAIL, el * MAIN, tok)
            for n in range(0, d, 512):
                tg[s, :, n:n + 512] = _dot(p, xb[k, :, n:n + 512])
            for j in range(2):
                @pl.when(s == j)
                def _(j=j):
                    xcopy(2 + j, j).start()
            return 0

        lax.fori_loop(0, 4, select, 0)

    tail = pl.ds(pl.multiple_of(e * TAIL, TAIL), TAIL)
    xs[e, 4 * MAIN:4 * CAP, :] = jnp.concatenate([tg[s, tail, :] for s in range(4)], axis=0).astype(jnp.bfloat16)
    f = h.shape[-1]
    full = f // 256 * 256
    wcopy(w1, e, 0).wait()
    wcopy(w3, e, 1).wait()
    x = xs[e]
    v1, v3 = wv.at[lax.rem(2 * e, ring)], wv.at[lax.rem(2 * e + 1, ring)]
    for n in range(0, full, 256):
        a = _dot(x, v1[:, n:n + 256])
        b = _dot(x, v3[:, n:n + 256])
        h[0, :, n:n + 256] = (jax.nn.silu(a) * b).astype(jnp.bfloat16)
    if full < f:
        r = f - full
        ab = _dot(x, jnp.concatenate([v1[:, full:], v3[:, full:]], axis=1))
        h[0, :, full:] = (jax.nn.silu(ab[:, :r]) * ab[:, r:]).astype(jnp.bfloat16)

    @pl.when(e + 2 < el)
    def _():
        wcopy(w3, e + 2, 1).start()

    @pl.when(e + 3 < el)
    def _():
        wcopy(w1, e + 3, 0).start()


def _up(xs, cx, w1, w3):
    el, d, f = w1.shape
    tok = xs[0].shape[0]
    ring = 5
    return pl.pallas_call(
        functools.partial(_up_kernel, el),
        grid=(el,),
        out_shape=jax.ShapeDtypeStruct((el, 4 * CAP, f), jnp.bfloat16),
        in_specs=[ANY] * 4 + [pl.BlockSpec(cx.shape, lambda e: (0, 0, 0))] + [ANY] * 2,
        out_specs=pl.BlockSpec((1, 4 * CAP, f), lambda e: (e, 0, 0)),
        scratch_shapes=[
            pltpu.VMEM((el, 4 * CAP, d), jnp.bfloat16),
            pltpu.VMEM((4, el * TAIL, d), jnp.float32),
            pltpu.VMEM((2, tok, d), jnp.bfloat16),
            pltpu.VMEM((ring, d, f), jnp.bfloat16),
            pltpu.SemaphoreType.DMA((2,)),
            pltpu.SemaphoreType.DMA((ring,)),
        ],
        compiler_params=_params(63),
        cost_estimate=pl.CostEstimate(flops=2 * 2 * el * 4 * CAP * d * f, bytes_accessed=4 * el * d * f, transcendentals=0),
        name="up",
    )(*xs, cx, w1, w3)


def _route_kernel(el, tok, cols, g, h, w2, base, sy, out, gv, hv, wv, r3, rt, send, recv, far, own, back, yb, bv, ost,
                  gsem, hsem, wsem, ssem, rsem, xssem, xrsem, osem, yssem, yrsem, bsem):
    me = lax.axis_index("ep")
    tp = lax.axis_index("tp")
    sib = me + 1 - 2 * lax.rem(me, 2)
    peer = lax.rem(me + 2, 4)
    ring = wv.shape[0]
    chunks = back.shape[0]
    kt = gv.shape[1] // 3
    nm = el * MAIN
    total = chunks * el
    unroll = 5

    gcopy = lambda s: pltpu.make_async_copy(g.at[pl.ds(s * tok, tok)], gv.at[pl.ds(s * tok, tok)], gsem.at[s])
    hcopy = lambda e: pltpu.make_async_copy(h.at[e], hv.at[e], hsem.at[e])

    def wcopy(t):
        slot = lax.rem(t, ring)
        col = pl.multiple_of(t // el * cols, cols)
        return pltpu.make_async_copy(w2.at[lax.rem(t, el), :, pl.ds(col, cols)], wv.at[slot], wsem.at[slot])

    def pair(c, k):
        return pltpu.make_async_remote_copy(send.at[lax.rem(c, 2), k], recv.at[c, k], ssem.at[c, k], rsem.at[c, k],
                                            device_id={"ep": sib}, device_id_type=pl.DeviceIdType.MESH)

    def across(c):
        return pltpu.make_async_remote_copy(recv.at[c, 1], back.at[c], xssem.at[c], xrsem.at[c],
                                            device_id={"ep": peer}, device_id_type=pl.DeviceIdType.MESH)

    part = lambda ref, c: ref.at[:, pl.ds(pl.multiple_of(c * cols, cols), cols)]

    def ycopy(c):
        return pltpu.make_async_remote_copy(part(sy, c), yb.at[c], yssem.at[c], yrsem.at[c],
                                            device_id={"tp": 1 - tp}, device_id_type=pl.DeviceIdType.MESH)

    bcopy = lambda c: pltpu.make_async_copy(part(base, c), bv.at[lax.rem(c, 2)], bsem.at[lax.rem(c, 2)])
    ocopy = lambda c: pltpu.make_async_copy(ost.at[lax.rem(c, 2)], part(out, c), osem.at[lax.rem(c, 2)])

    for e in range(el):
        hcopy(e).start()
        if e < ring:
            wcopy(jnp.int32(e)).start()
    for s in (3, 1, 2, 0):
        gcopy(s).start()
    barrier = pltpu.get_barrier_semaphore()
    for dev in (sib, peer):
        pl.semaphore_signal(barrier, inc=1, device_id={"ep": dev}, device_id_type=pl.DeviceIdType.MESH)
    pl.semaphore_signal(barrier, inc=1, device_id={"tp": 1 - tp}, device_id_type=pl.DeviceIdType.MESH)
    pl.semaphore_wait(barrier, 3)
    for c in range(chunks):
        ycopy(jnp.int32(c)).start()
    for c in range(2):
        bcopy(jnp.int32(c)).start()

    def group(c, k):
        for u in range(unroll):
            t = c * el + k * unroll + u
            wcopy(t).wait()

            @pl.when(c == 0)
            def _():
                hcopy(k * unroll + u).wait()

        for u in range(unroll):
            e = k * unroll + u
            r = _dot(hv[e], wv[lax.rem(c * el + e, ring)]).astype(jnp.bfloat16)
            row = pl.multiple_of(e * MAIN, MAIN)
            for s in range(4):
                for i in range(3):
                    r3[s, pl.ds(row + i * kt, MAIN), :] = r[s * MAIN:(s + 1) * MAIN]
            q = r[4 * MAIN:].astype(jnp.float32)
            for s in range(4):
                rt[s, pl.ds(pl.multiple_of(e * TAIL, TAIL), TAIL), :] = q[s * TAIL:(s + 1) * TAIL]
        for u in range(unroll):
            t = c * el + k * unroll + u

            @pl.when(t + ring < total)
            def _():
                wcopy(t + ring).start()

    def combine(s):
        tail = jnp.concatenate([rt[s], jnp.zeros((kt - el * CAP, cols), jnp.float32)], axis=0).astype(jnp.bfloat16)
        for i in range(3):
            r3[s, i * kt + nm:(i + 1) * kt, :] = tail
        return _dot(gv[s * tok:(s + 1) * tok, :], r3[s])

    def merge(c):
        pair(c, 1).wait_recv()
        recv[c, 1] = recv[c, 1] + far[...]
        pair(c, 0).wait_recv()
        recv[c, 0] = recv[c, 0] + own[...]
        across(c).start()

    def chunk(c, _):
        def step(k, _):
            group(c, k)

            @pl.when((k == 0) & (c > 0))
            def _():
                merge(c - 1)

            return 0

        lax.fori_loop(0, el // unroll, step, 0)

        @pl.when(c == 0)
        def _():
            for s in range(4):
                gcopy(s).wait()

        @pl.when(c >= 2)
        def _():
            pair(c - 2, 0).wait_send()
            pair(c - 2, 1).wait_send()

        slot = lax.rem(c, 2)
        send[slot, 1] = combine(3)
        send[slot, 0] = combine(1)
        pair(c, 1).start()
        far[...] = combine(2)
        pair(c, 0).start()
        own[...] = combine(0)
        return 0

    lax.fori_loop(0, chunks, chunk, 0)
    merge(jnp.int32(chunks - 1))

    def finish(c, _):
        k = lax.rem(c, 2)
        bcopy(c).wait()
        ycopy(c).wait_recv()

        @pl.when(c >= 2)
        def _():
            ocopy(c - 2).wait()

        across(c).wait_recv()
        ost[k] = (bv[k] + yb[c] + (recv[c, 0] + back[c])).astype(jnp.bfloat16)
        ocopy(c).start()

        @pl.when(c + 2 < chunks)
        def _():
            bcopy(c + 2).start()

        return 0

    lax.fori_loop(0, chunks, finish, 0)
    for c in range(chunks - 2, chunks):
        pair(jnp.int32(c), 0).wait_send()
        pair(jnp.int32(c), 1).wait_send()
        ocopy(jnp.int32(c)).wait()
    for c in range(chunks):
        across(jnp.int32(c)).wait_send()
        ycopy(jnp.int32(c)).wait_send()


def _route(g, h, w2, base, sy):
    el, f, d = w2.shape
    tok = base.shape[0]
    cols = 256
    chunks = d // cols
    ring = 8
    k3 = g.shape[1]
    f32 = jnp.float32
    return pl.pallas_call(
        functools.partial(_route_kernel, el, tok, cols),
        out_shape=jax.ShapeDtypeStruct((tok, d), jnp.bfloat16),
        in_specs=[ANY] * 5,
        out_specs=ANY,
        scratch_shapes=[
            pltpu.VMEM((4 * tok, k3), jnp.bfloat16),
            pltpu.VMEM((el, 4 * CAP, f), jnp.bfloat16),
            pltpu.VMEM((ring, f, cols), jnp.bfloat16),
            pltpu.VMEM((4, k3, cols), jnp.bfloat16),
            pltpu.VMEM((4, el * TAIL, cols), f32),
            pltpu.VMEM((2, 2, tok, cols), f32),
            pltpu.VMEM((chunks, 2, tok, cols), f32),
            pltpu.VMEM((tok, cols), f32),
            pltpu.VMEM((tok, cols), f32),
            pltpu.VMEM((chunks, tok, cols), f32),
            pltpu.VMEM((chunks, tok, cols), f32),
            pltpu.VMEM((2, tok, cols), f32),
            pltpu.VMEM((2, tok, cols), jnp.bfloat16),
            pltpu.SemaphoreType.DMA((4,)),
            pltpu.SemaphoreType.DMA((el,)),
            pltpu.SemaphoreType.DMA((ring,)),
            pltpu.SemaphoreType.DMA((chunks, 2)),
            pltpu.SemaphoreType.DMA((chunks, 2)),
            pltpu.SemaphoreType.DMA((chunks,)),
            pltpu.SemaphoreType.DMA((chunks,)),
            pltpu.SemaphoreType.DMA((2,)),
            pltpu.SemaphoreType.DMA((chunks,)),
            pltpu.SemaphoreType.DMA((chunks,)),
            pltpu.SemaphoreType.DMA((2,)),
        ],
        compiler_params=pltpu.CompilerParams(vmem_limit_bytes=63 * MIB, collective_id=0, has_side_effects=True),
        cost_estimate=pl.CostEstimate(flops=2 * el * 4 * CAP * f * d + 8 * tok * k3 * d,
                                      bytes_accessed=2 * el * f * d + 2 * el * 4 * CAP * f, transcendentals=0),
        name="route",
    )(g, h, w2, base, sy)


def solution(mesh):
    rows = P(("ep", "tp"), None)
    def body(x, idx, g, slot, ws1, ws3, ws2, w1, w3, w2):
        tok, d = x.shape
        el = w1.shape[0]
        kt = -(-el * CAP // 16) * 16
        code = jnp.where(slot >= 0, idx * 128 + slot, -1).astype(jnp.float32)
        mine = jnp.concatenate([code, g], axis=1).T
        cx, gm, base, sy, xc, xx, xxc = _front(x, mine, ws1, ws3, ws2, el, kt)
        h = _up((x, xc, xx, xxc), cx, w1, w3)
        return _route(gm, h, w2, base, sy)

    return jax.shard_map(
        body, mesh=mesh,
        in_specs=(rows, rows, rows, rows, P(None, "tp"), P(None, "tp"), P("tp", None),
                  P("ep", None, None), P("ep", None, None), P("ep", None, None)),
        out_specs=rows, check_vma=False)
```

```python
import functools

import jax
import jax.numpy as jnp
from jax import lax
from jax.experimental import pallas as pl
from jax.experimental.pallas import tpu as pltpu
from jax.sharding import PartitionSpec as P

CAP = 72
MAIN = 64
TAIL = CAP - MAIN
MIB = 1024 * 1024
ANY = pl.BlockSpec(memory_space=pl.ANY)


def _params(mib):
    return pltpu.CompilerParams(vmem_limit_bytes=mib * MIB)


def _dot(a, b):
    return jnp.dot(a, b, preferred_element_type=jnp.float32)


def _hot(c, n, base, tok):
    r = (lax.broadcasted_iota(jnp.int32, (n, tok), 0) + base).astype(jnp.float32)
    hit = r == c[0:1, :]
    for j in range(1, 4):
        hit = hit | (r == c[j:j + 1, :])
    return jnp.where(hit, 1.0, 0.0).astype(jnp.bfloat16)


def _codes(t, me, el):
    code = t[0:4, :].astype(jnp.int32)
    e, k = code >> 7, code & 127
    le = e - me * el
    ok = (code >= 0) & (le >= 0) & (le < el)
    c = jnp.where(ok, jnp.where(k < MAIN, le * MAIN + k, el * MAIN + le * TAIL + k - MAIN), -1).astype(jnp.float32)
    g = t[4:8, :]
    g0 = g.astype(jnp.bfloat16).astype(jnp.float32)
    g1 = (g - g0).astype(jnp.bfloat16).astype(jnp.float32)
    return c, jnp.concatenate([c, g0, g1, g - g0 - g1], axis=0)


def _front_kernel(el, kt, x, mine, w1, w3, w2, cx, gm, base, sy, xc, xx, xxc,
                  y, tabs, tabt, v1, v3, v2, hs, sst, gst, wsem, xsend, xrecv, tsend, trecv, ssem, gsem):
    me = lax.axis_index("ep")
    tp = lax.axis_index("tp")
    sib = me + 1 - 2 * lax.rem(me, 2)
    peer = lax.rem(me + 2, 4)
    diag = lax.rem(sib + 2, 4)
    tok, d = x.shape
    half = tok // 2
    nf, nn = v1.shape[0], v2.shape[0]
    tf, tn = v1.shape[2], v2.shape[2]
    mesh_id = pl.DeviceIdType.MESH

    def remote(src, dst, ss, rs, dev):
        return pltpu.make_async_remote_copy(src, dst, ss, rs, device_id=dev, device_id_type=mesh_id)

    def up(i):
        col = pl.ds(pl.multiple_of(i * tf, tf), tf)
        return (pltpu.make_async_copy(w1.at[:, col], v1.at[i], wsem.at[i]),
                pltpu.make_async_copy(w3.at[:, col], v3.at[i], wsem.at[nf + i]))

    def down(i):
        return pltpu.make_async_copy(w2.at[:, pl.ds(pl.multiple_of(i * tn, tn), tn)], v2.at[i], wsem.at[2 * nf + i])

    barrier = pltpu.get_barrier_semaphore()
    for dev in (sib, peer, diag):
        pl.semaphore_signal(barrier, inc=1, device_id={"ep": dev}, device_id_type=mesh_id)
    pl.semaphore_signal(barrier, inc=1, device_id={"tp": 1 - tp}, device_id_type=mesh_id)
    pl.semaphore_wait(barrier, 4)
    tcopy = [remote(mine, tabs.at[k], tsend.at[k], trecv.at[k], {"ep": dev}) for k, dev in enumerate((sib, peer, diag))]
    xcopy = remote(x, xx, xsend.at[0], xrecv.at[0], {"ep": peer})
    ccopy = remote(x, xc, xsend.at[1], xrecv.at[1], {"ep": sib})
    ycopy = [remote(x.at[pl.ds(k * half, half)], y.at[pl.ds(k * half, half)], xsend.at[2 + k], xrecv.at[2 + k], {"tp": 1 - tp})
             for k in range(2)]
    relay = remote(xx, xxc, xsend.at[4], xrecv.at[4], {"ep": sib})
    for c in (*tcopy, xcopy, *ycopy, ccopy):
        c.start()
    for i in range(nf):
        for c in up(i):
            c.start()
    for i in range(nn):
        down(i).start()

    def store_tab(s, tab):
        wide = jnp.concatenate([tab, jnp.zeros((128 - tab.shape[0], tok), jnp.float32)], axis=0)
        for b in range(0, tok, 128):
            tabt[s * tok + b:s * tok + b + 128, :] = jnp.transpose(wide[:, b:b + 128])

    def shared(src, lo, n, out, add, first):
        scopy = lambda i: pltpu.make_async_copy(
            sst.at[lax.rem(i, 2), pl.ds(0, n)], out.at[pl.ds(lo, n), pl.ds(pl.multiple_of(i * tn, tn), tn)], ssem.at[lax.rem(i, 2)])

        def gate(i, _):
            if first:
                for c in up(i):
                    c.wait()
            r = src[lo:lo + n, :]
            a = _dot(r, v1[i])
            b = _dot(r, v3[i])
            hs[lo:lo + n, pl.ds(pl.multiple_of(i * tf, tf), tf)] = (jax.nn.silu(a) * b).astype(jnp.bfloat16)
            return 0

        def tile(i, _):
            if first:
                down(i).wait()

            @pl.when(i >= 2)
            def _():
                scopy(i - 2).wait()

            r = _dot(hs[lo:lo + n, :], v2[i])
            if add:
                r = r + src[lo:lo + n, pl.ds(pl.multiple_of(i * tn, tn), tn)].astype(jnp.float32)
            sst[lax.rem(i, 2), 0:n, :] = r
            scopy(i).start()
            return 0

        lax.fori_loop(0, nf, gate, 0)
        lax.fori_loop(0, nn, tile, 0)
        for i in (nn - 2, nn - 1):
            scopy(jnp.int32(i)).wait()

    shared(x, 0, tok, base, True, True)
    for k in range(4):
        if k:
            tcopy[k - 1].wait()
        c, tab = _codes(mine[...] if k == 0 else tabs[k - 1], me, el)
        cx[k] = jnp.concatenate([c, c], axis=0)
        store_tab(k, tab)

    blk = gst.shape[1]
    gcopy = lambda i: pltpu.make_async_copy(gst.at[lax.rem(i, 2)], gm.at[pl.ds(pl.multiple_of(i * blk, blk), blk)], gsem.at[lax.rem(i, 2)])

    def gates(i, _):
        @pl.when(i >= 2)
        def _():
            gcopy(i - 2).wait()

        t = tabt[pl.ds(pl.multiple_of(i * blk, blk), blk), :]
        lane = lax.broadcasted_iota(jnp.int32, (blk, kt), 1).astype(jnp.float32)
        acc = [jnp.zeros((blk, kt), jnp.float32) for _ in range(3)]
        for j in range(4):
            hit = t[:, j:j + 1] == lane
            for q in range(3):
                acc[q] = jnp.where(hit, t[:, 4 + 4 * q + j:5 + 4 * q + j], acc[q])
        for q in range(3):
            gst[lax.rem(i, 2), :, q * kt:(q + 1) * kt] = acc[q].astype(jnp.bfloat16)
        gcopy(i).start()
        return 0

    ng = 4 * tok // blk
    lax.fori_loop(0, ng, gates, 0)
    for i in (ng - 2, ng - 1):
        gcopy(jnp.int32(i)).wait()
    ycopy[0].wait()
    shared(y, 0, half, sy, False, False)
    xcopy.wait()
    relay.start()
    ycopy[1].wait()
    shared(y, half, half, sy, False, False)
    ccopy.wait()
    relay.wait()


def _front(x, mine, w1, w3, w2, el, kt):
    tok, d = x.shape
    f = w1.shape[1]
    tf, tn = 256, 512
    nf, nn = f // tf, d // tn
    bf16, f32 = jnp.bfloat16, jnp.float32
    vmem = pl.BlockSpec(memory_space=pltpu.VMEM)
    dma = pltpu.SemaphoreType.DMA
    return pl.pallas_call(
        functools.partial(_front_kernel, el, kt),
        out_shape=[jax.ShapeDtypeStruct(sh, dt) for sh, dt in (
            ((4, 8, tok), f32), ((4 * tok, 3 * kt), bf16), ((tok, d), f32), ((tok, d), f32),
            ((tok, d), bf16), ((tok, d), bf16), ((tok, d), bf16))],
        in_specs=[vmem, vmem] + [ANY] * 3,
        out_specs=[vmem] + [ANY] * 6,
        scratch_shapes=[
            pltpu.VMEM((tok, d), bf16),
            pltpu.VMEM((3, 8, tok), f32),
            pltpu.VMEM((4 * tok, 128), f32),
            pltpu.VMEM((nf, d, tf), bf16),
            pltpu.VMEM((nf, d, tf), bf16),
            pltpu.VMEM((nn, f, tn), bf16),
            pltpu.VMEM((tok, f), bf16),
            pltpu.VMEM((2, tok, tn), f32),
            pltpu.VMEM((2, 128, 3 * kt), bf16),
            dma((2 * nf + nn,)), dma((5,)), dma((5,)), dma((3,)), dma((3,)), dma((2,)), dma((2,)),
        ],
        compiler_params=pltpu.CompilerParams(vmem_limit_bytes=62 * MIB, collective_id=1, has_side_effects=True),
        cost_estimate=pl.CostEstimate(flops=12 * tok * d * f, bytes_accessed=6 * d * f, transcendentals=0),
        name="front",
    )(x, mine, w1, w3, w2)


def _up_kernel(el, x0, x1, x2, x3, cx, w1, w3, h, xs, tg, xb, wv, xsem, wsem):
    e = pl.program_id(0)
    tok, d = x0.shape
    ring = wv.shape[0]
    srcs = (x0, x1, x2, x3)
    some = 5

    def wcopy(w, i, k):
        slot = lax.rem(2 * i + k, ring)
        return pltpu.make_async_copy(w.at[i], wv.at[slot], wsem.at[slot])

    xcopy = lambda s, k: pltpu.make_async_copy(srcs[s], xb.at[k], xsem.at[k])

    @pl.when(e == 0)
    def _():
        xcopy(0, 0).start()
        xcopy(1, 1).start()
        for i in range(ring):
            wcopy(w3 if i % 2 else w1, jnp.int32(i // 2), i % 2).start()

        def select(s, _):
            k = lax.rem(s, 2)
            xcopy(0, k).wait()
            c = cx[s]
            for b in range(0, el, some):
                p = _hot(c, some * MAIN, b * MAIN, tok)
                for n in range(0, d, 512):
                    r = _dot(p, xb[k, :, n:n + 512]).astype(jnp.bfloat16)
                    for i in range(some):
                        xs[b + i, pl.ds(pl.multiple_of(s * MAIN, MAIN), MAIN), n:n + 512] = r[i * MAIN:(i + 1) * MAIN]
            p = _hot(c, el * TAIL, el * MAIN, tok)
            for n in range(0, d, 512):
                tg[s, :, n:n + 512] = _dot(p, xb[k, :, n:n + 512])
            for j in range(2):
                @pl.when(s == j)
                def _(j=j):
                    xcopy(2 + j, j).start()
            return 0

        lax.fori_loop(0, 4, select, 0)

    tail = pl.ds(pl.multiple_of(e * TAIL, TAIL), TAIL)
    xs[e, 4 * MAIN:4 * CAP, :] = jnp.concatenate([tg[s, tail, :] for s in range(4)], axis=0).astype(jnp.bfloat16)
    f = h.shape[-1]
    full = f // 256 * 256
    wcopy(w1, e, 0).wait()
    wcopy(w3, e, 1).wait()
    x = xs[e]
    v1, v3 = wv.at[lax.rem(2 * e, ring)], wv.at[lax.rem(2 * e + 1, ring)]
    for n in range(0, full, 256):
        a = _dot(x, v1[:, n:n + 256])
        b = _dot(x, v3[:, n:n + 256])
        h[0, :, n:n + 256] = (jax.nn.silu(a) * b).astype(jnp.bfloat16)
    if full < f:
        r = f - full
        ab = _dot(x, jnp.concatenate([v1[:, full:], v3[:, full:]], axis=1))
        h[0, :, full:] = (jax.nn.silu(ab[:, :r]) * ab[:, r:]).astype(jnp.bfloat16)

    @pl.when(e + 2 < el)
    def _():
        wcopy(w3, e + 2, 1).start()

    @pl.when(e + 3 < el)
    def _():
        wcopy(w1, e + 3, 0).start()


def _up(xs, cx, w1, w3):
    el, d, f = w1.shape
    tok = xs[0].shape[0]
    ring = 5
    return pl.pallas_call(
        functools.partial(_up_kernel, el),
        grid=(el,),
        out_shape=jax.ShapeDtypeStruct((el, 4 * CAP, f), jnp.bfloat16),
        in_specs=[ANY] * 4 + [pl.BlockSpec(cx.shape, lambda e: (0, 0, 0))] + [ANY] * 2,
        out_specs=pl.BlockSpec((1, 4 * CAP, f), lambda e: (e, 0, 0)),
        scratch_shapes=[
            pltpu.VMEM((el, 4 * CAP, d), jnp.bfloat16),
            pltpu.VMEM((4, el * TAIL, d), jnp.float32),
            pltpu.VMEM((2, tok, d), jnp.bfloat16),
            pltpu.VMEM((ring, d, f), jnp.bfloat16),
            pltpu.SemaphoreType.DMA((2,)),
            pltpu.SemaphoreType.DMA((ring,)),
        ],
        compiler_params=_params(63),
        cost_estimate=pl.CostEstimate(flops=2 * 2 * el * 4 * CAP * d * f, bytes_accessed=4 * el * d * f, transcendentals=0),
        name="up",
    )(*xs, cx, w1, w3)


def _route_kernel(el, tok, cols, g, h, w2, base, sy, out, gv, hv, wv, r3, rt, send, recv, far, own, back, yb, bv, ost,
                  gsem, hsem, wsem, ssem, rsem, xssem, xrsem, osem, yssem, yrsem, bsem):
    me = lax.axis_index("ep")
    tp = lax.axis_index("tp")
    sib = me + 1 - 2 * lax.rem(me, 2)
    peer = lax.rem(me + 2, 4)
    ring = wv.shape[0]
    chunks = back.shape[0]
    kt = gv.shape[1] // 3
    nm = el * MAIN
    total = chunks * el

    gcopy = lambda s: pltpu.make_async_copy(g.at[pl.ds(s * tok, tok)], gv.at[pl.ds(s * tok, tok)], gsem.at[s])
    hcopy = lambda e: pltpu.make_async_copy(h.at[e], hv.at[e], hsem.at[e])

    def wcopy(t):
        slot = lax.rem(t, ring)
        col = pl.multiple_of(t // el * cols, cols)
        return pltpu.make_async_copy(w2.at[lax.rem(t, el), :, pl.ds(col, cols)], wv.at[slot], wsem.at[slot])

    def pair(c, k):
        return pltpu.make_async_remote_copy(send.at[lax.rem(c, 2), k], recv.at[c, k], ssem.at[c, k], rsem.at[c, k],
                                            device_id={"ep": sib}, device_id_type=pl.DeviceIdType.MESH)

    def across(c):
        return pltpu.make_async_remote_copy(recv.at[c, 1], back.at[c], xssem.at[c], xrsem.at[c],
                                            device_id={"ep": peer}, device_id_type=pl.DeviceIdType.MESH)

    part = lambda ref, c: ref.at[:, pl.ds(pl.multiple_of(c * cols, cols), cols)]

    def ycopy(c):
        return pltpu.make_async_remote_copy(part(sy, c), yb.at[c], yssem.at[c], yrsem.at[c],
                                            device_id={"tp": 1 - tp}, device_id_type=pl.DeviceIdType.MESH)

    bcopy = lambda c: pltpu.make_async_copy(part(base, c), bv.at[lax.rem(c, 2)], bsem.at[lax.rem(c, 2)])
    ocopy = lambda c: pltpu.make_async_copy(ost.at[lax.rem(c, 2)], part(out, c), osem.at[lax.rem(c, 2)])

    for e in range(el):
        hcopy(e).start()
        if e < ring:
            wcopy(jnp.int32(e)).start()
    for s in (3, 1, 2, 0):
        gcopy(s).start()
    barrier = pltpu.get_barrier_semaphore()
    for dev in (sib, peer):
        pl.semaphore_signal(barrier, inc=1, device_id={"ep": dev}, device_id_type=pl.DeviceIdType.MESH)
    pl.semaphore_signal(barrier, inc=1, device_id={"tp": 1 - tp}, device_id_type=pl.DeviceIdType.MESH)
    pl.semaphore_wait(barrier, 3)
    for c in range(chunks):
        ycopy(jnp.int32(c)).start()
    for c in range(2):
        bcopy(jnp.int32(c)).start()

    def group(c, lo, hi):
        for e in range(lo, hi):
            wcopy(c * el + e).wait()

        @pl.when(c == 0)
        def _():
            for e in range(lo, hi):
                hcopy(e).wait()

        for e in range(lo, hi):
            r = _dot(hv[e], wv[lax.rem(c * el + e, ring)]).astype(jnp.bfloat16)
            for s in range(4):
                for i in range(3):
                    r3[s, e * MAIN + i * kt:(e + 1) * MAIN + i * kt, :] = r[s * MAIN:(s + 1) * MAIN]
            q = r[4 * MAIN:].astype(jnp.float32)
            for s in range(4):
                rt[s, e * TAIL:(e + 1) * TAIL, :] = q[s * TAIL:(s + 1) * TAIL]
        for e in range(lo, hi):
            t = c * el + e

            @pl.when(t + ring < total)
            def _(t=t):
                wcopy(t + ring).start()

    def combine(s):
        tail = jnp.concatenate([rt[s], jnp.zeros((kt - el * CAP, cols), jnp.float32)], axis=0).astype(jnp.bfloat16)
        for i in range(3):
            r3[s, i * kt + nm:(i + 1) * kt, :] = tail
        return _dot(gv[s * tok:(s + 1) * tok, :], r3[s])

    def merge(c):
        pair(c, 1).wait_recv()
        recv[c, 1] = recv[c, 1] + far[...]
        pair(c, 0).wait_recv()
        recv[c, 0] = recv[c, 0] + own[...]
        across(c).start()

    def chunk(c, _):
        group(c, 0, ring)

        @pl.when(c > 0)
        def _():
            merge(c - 1)

        group(c, ring, el)

        @pl.when(c == 0)
        def _():
            for s in range(4):
                gcopy(s).wait()

        @pl.when(c >= 2)
        def _():
            pair(c - 2, 0).wait_send()
            pair(c - 2, 1).wait_send()

        slot = lax.rem(c, 2)
        send[slot, 1] = combine(3)
        send[slot, 0] = combine(1)
        pair(c, 1).start()
        pair(c, 0).start()
        far[...] = combine(2)
        own[...] = combine(0)
        return 0

    lax.fori_loop(0, chunks, chunk, 0)
    merge(jnp.int32(chunks - 1))

    def finish(c, _):
        k = lax.rem(c, 2)
        bcopy(c).wait()
        ycopy(c).wait_recv()

        @pl.when(c >= 2)
        def _():
            ocopy(c - 2).wait()

        across(c).wait_recv()
        ost[k] = (bv[k] + yb[c] + (recv[c, 0] + back[c])).astype(jnp.bfloat16)
        ocopy(c).start()

        @pl.when(c + 2 < chunks)
        def _():
            bcopy(c + 2).start()

        return 0

    lax.fori_loop(0, chunks, finish, 0)
    for c in range(chunks - 2, chunks):
        pair(jnp.int32(c), 0).wait_send()
        pair(jnp.int32(c), 1).wait_send()
        ocopy(jnp.int32(c)).wait()
    for c in range(chunks):
        across(jnp.int32(c)).wait_send()
        ycopy(jnp.int32(c)).wait_send()


def _route(g, h, w2, base, sy):
    el, f, d = w2.shape
    tok = base.shape[0]
    cols = 256
    chunks = d // cols
    ring = 8
    k3 = g.shape[1]
    f32 = jnp.float32
    return pl.pallas_call(
        functools.partial(_route_kernel, el, tok, cols),
        out_shape=jax.ShapeDtypeStruct((tok, d), jnp.bfloat16),
        in_specs=[ANY] * 5,
        out_specs=ANY,
        scratch_shapes=[
            pltpu.VMEM((4 * tok, k3), jnp.bfloat16),
            pltpu.VMEM((el, 4 * CAP, f), jnp.bfloat16),
            pltpu.VMEM((ring, f, cols), jnp.bfloat16),
            pltpu.VMEM((4, k3, cols), jnp.bfloat16),
            pltpu.VMEM((4, el * TAIL, cols), f32),
            pltpu.VMEM((2, 2, tok, cols), f32),
            pltpu.VMEM((chunks, 2, tok, cols), f32),
            pltpu.VMEM((tok, cols), f32),
            pltpu.VMEM((tok, cols), f32),
            pltpu.VMEM((chunks, tok, cols), f32),
            pltpu.VMEM((chunks, tok, cols), f32),
            pltpu.VMEM((2, tok, cols), f32),
            pltpu.VMEM((2, tok, cols), jnp.bfloat16),
            pltpu.SemaphoreType.DMA((4,)),
            pltpu.SemaphoreType.DMA((el,)),
            pltpu.SemaphoreType.DMA((ring,)),
            pltpu.SemaphoreType.DMA((chunks, 2)),
            pltpu.SemaphoreType.DMA((chunks, 2)),
            pltpu.SemaphoreType.DMA((chunks,)),
            pltpu.SemaphoreType.DMA((chunks,)),
            pltpu.SemaphoreType.DMA((2,)),
            pltpu.SemaphoreType.DMA((chunks,)),
            pltpu.SemaphoreType.DMA((chunks,)),
            pltpu.SemaphoreType.DMA((2,)),
        ],
        compiler_params=pltpu.CompilerParams(vmem_limit_bytes=63 * MIB, collective_id=0, has_side_effects=True),
        cost_estimate=pl.CostEstimate(flops=2 * el * 4 * CAP * f * d + 8 * tok * k3 * d,
                                      bytes_accessed=2 * el * f * d + 2 * el * 4 * CAP * f, transcendentals=0),
        name="route",
    )(g, h, w2, base, sy)


def solution(mesh):
    rows = P(("ep", "tp"), None)
    def body(x, idx, g, slot, ws1, ws3, ws2, w1, w3, w2):
        tok, d = x.shape
        el = w1.shape[0]
        kt = -(-el * CAP // 16) * 16
        code = jnp.where(slot >= 0, idx * 128 + slot, -1).astype(jnp.float32)
        mine = jnp.concatenate([code, g], axis=1).T
        cx, gm, base, sy, xc, xx, xxc = _front(x, mine, ws1, ws3, ws2, el, kt)
        h = _up((x, xc, xx, xxc), cx, w1, w3)
        return _route(gm, h, w2, base, sy)

    return jax.shard_map(
        body, mesh=mesh,
        in_specs=(rows, rows, rows, rows, P(None, "tp"), P(None, "tp"), P("tp", None),
                  P("ep", None, None), P("ep", None, None), P("ep", None, None)),
        out_specs=rows, check_vma=False)
```

```python
import functools

import jax
import jax.numpy as jnp
from jax import lax
from jax.experimental import pallas as pl
from jax.experimental.pallas import tpu as pltpu
from jax.sharding import PartitionSpec as P

CAP = 72
MAIN = 64
TAIL = CAP - MAIN
MIB = 1024 * 1024
ANY = pl.BlockSpec(memory_space=pl.ANY)


def _params(mib):
    return pltpu.CompilerParams(vmem_limit_bytes=mib * MIB)


def _dot(a, b):
    return jnp.dot(a, b, preferred_element_type=jnp.float32)


def _hot(c, n, base, tok):
    r = (lax.broadcasted_iota(jnp.int32, (n, tok), 0) + base).astype(jnp.float32)
    g = jnp.zeros((n, tok), jnp.float32)
    hit = None
    for j in range(4):
        same = r == c[j:j + 1, :]
        hit = same if hit is None else hit | same
        g = jnp.where(same, c[4 + j:5 + j, :], g)
    g = jnp.broadcast_to(jnp.sum(g, axis=1, keepdims=True), (n, 128))
    return jnp.where(hit, 1.0, 0.0).astype(jnp.bfloat16), g


def _codes(t, me, el):
    code = t[0:4, :].astype(jnp.int32)
    e, k = code >> 7, code & 127
    le = e - me * el
    ok = (code >= 0) & (le >= 0) & (le < el)
    c = jnp.where(ok, jnp.where(k < MAIN, le * MAIN + k, el * MAIN + le * TAIL + k - MAIN), -1).astype(jnp.float32)
    return c


def _front_kernel(el, kt, x, mine, w1, w3, w2, cx, gm, base, sy, xc, xx, xxc,
                  y, tabs, tabt, v1, v3, v2, hs, sst, gst, wsem, xsend, xrecv, tsend, trecv, ssem, gsem):
    me = lax.axis_index("ep")
    tp = lax.axis_index("tp")
    sib = me + 1 - 2 * lax.rem(me, 2)
    peer = lax.rem(me + 2, 4)
    diag = lax.rem(sib + 2, 4)
    tok, d = x.shape
    half = tok // 2
    nf, nn = v1.shape[0], v2.shape[0]
    tf, tn = v1.shape[2], v2.shape[2]
    mesh_id = pl.DeviceIdType.MESH

    def remote(src, dst, ss, rs, dev):
        return pltpu.make_async_remote_copy(src, dst, ss, rs, device_id=dev, device_id_type=mesh_id)

    def up(i):
        col = pl.ds(pl.multiple_of(i * tf, tf), tf)
        return (pltpu.make_async_copy(w1.at[:, col], v1.at[i], wsem.at[i]),
                pltpu.make_async_copy(w3.at[:, col], v3.at[i], wsem.at[nf + i]))

    def down(i):
        return pltpu.make_async_copy(w2.at[:, pl.ds(pl.multiple_of(i * tn, tn), tn)], v2.at[i], wsem.at[2 * nf + i])

    barrier = pltpu.get_barrier_semaphore()
    for dev in (sib, peer, diag):
        pl.semaphore_signal(barrier, inc=1, device_id={"ep": dev}, device_id_type=mesh_id)
    pl.semaphore_signal(barrier, inc=1, device_id={"tp": 1 - tp}, device_id_type=mesh_id)
    pl.semaphore_wait(barrier, 4)
    tcopy = [remote(mine, tabs.at[k], tsend.at[k], trecv.at[k], {"ep": dev}) for k, dev in enumerate((sib, peer, diag))]
    xcopy = remote(x, xx, xsend.at[0], xrecv.at[0], {"ep": peer})
    ccopy = remote(x, xc, xsend.at[1], xrecv.at[1], {"ep": sib})
    ycopy = [remote(x.at[pl.ds(k * half, half)], y.at[pl.ds(k * half, half)], xsend.at[2 + k], xrecv.at[2 + k], {"tp": 1 - tp})
             for k in range(2)]
    relay = remote(xx, xxc, xsend.at[4], xrecv.at[4], {"ep": sib})
    for c in (*tcopy, xcopy, *ycopy, ccopy):
        c.start()
    for i in range(nf):
        for c in up(i):
            c.start()
    for i in range(nn):
        down(i).start()

    def table(k):
        t = mine[...] if k == 0 else tabs[k - 1]
        c = _codes(t, me, el)
        cx[k] = jnp.concatenate([c, t[4:8, :]], axis=0)
        wide = jnp.concatenate([c, jnp.zeros((124, tok), jnp.float32)], axis=0)
        for b in range(0, tok, 128):
            tabt[k * tok + b:k * tok + b + 128, :] = jnp.transpose(wide[:, b:b + 128])

    def shared(src, lo, n, out, add, first):
        scopy = lambda i: pltpu.make_async_copy(
            sst.at[lax.rem(i, 2), pl.ds(0, n)], out.at[pl.ds(lo, n), pl.ds(pl.multiple_of(i * tn, tn), tn)], ssem.at[lax.rem(i, 2)])

        def gate(i, _):
            if first:
                for c in up(i):
                    c.wait()
            r = src[lo:lo + n, :]
            a = _dot(r, v1[i])
            b = _dot(r, v3[i])
            hs[lo:lo + n, pl.ds(pl.multiple_of(i * tf, tf), tf)] = (jax.nn.silu(a) * b).astype(jnp.bfloat16)
            return 0

        def tile(i, _):
            if first:
                down(i).wait()

            @pl.when(i >= 2)
            def _():
                scopy(i - 2).wait()

            r = _dot(hs[lo:lo + n, :], v2[i])
            if add:
                r = r + src[lo:lo + n, pl.ds(pl.multiple_of(i * tn, tn), tn)].astype(jnp.float32)
            sst[lax.rem(i, 2), 0:n, :] = r
            scopy(i).start()
            return 0

        lax.fori_loop(0, nf, gate, 0)
        lax.fori_loop(0, nn, tile, 0)
        for i in (nn - 2, nn - 1):
            scopy(jnp.int32(i)).wait()

    blk = gst.shape[1]
    gcopy = lambda i: pltpu.make_async_copy(gst.at[lax.rem(i, 2)], gm.at[pl.ds(pl.multiple_of(i * blk, blk), blk)], gsem.at[lax.rem(i, 2)])

    def picks(i, _):
        @pl.when(i >= 2)
        def _():
            gcopy(i - 2).wait()

        t = tabt[pl.ds(pl.multiple_of(i * blk, blk), blk), :]
        lane = lax.broadcasted_iota(jnp.int32, (blk, kt), 1).astype(jnp.float32)
        hit = t[:, 0:1] == lane
        for j in range(1, 4):
            hit = hit | (t[:, j:j + 1] == lane)
        gst[lax.rem(i, 2)] = jnp.where(hit, 1.0, 0.0).astype(jnp.bfloat16)
        gcopy(i).start()
        return 0

    ng = tok // blk
    table(0)
    lax.fori_loop(0, ng, picks, 0)
    for k in range(1, 4):
        tcopy[k - 1].wait()
        table(k)
    lax.fori_loop(ng, 4 * ng, picks, 0)
    for i in (4 * ng - 2, 4 * ng - 1):
        gcopy(jnp.int32(i)).wait()
    shared(x, 0, tok, base, True, True)
    ycopy[0].wait()
    shared(y, 0, half, sy, False, False)
    xcopy.wait()
    relay.start()
    ycopy[1].wait()
    shared(y, half, half, sy, False, False)
    ccopy.wait()
    relay.wait()


def _front(x, mine, w1, w3, w2, el, kt):
    tok, d = x.shape
    f = w1.shape[1]
    tf, tn = 256, 512
    nf, nn = f // tf, d // tn
    bf16, f32 = jnp.bfloat16, jnp.float32
    vmem = pl.BlockSpec(memory_space=pltpu.VMEM)
    dma = pltpu.SemaphoreType.DMA
    return pl.pallas_call(
        functools.partial(_front_kernel, el, kt),
        out_shape=[jax.ShapeDtypeStruct(sh, dt) for sh, dt in (
            ((4, 8, tok), f32), ((4 * tok, kt), bf16), ((tok, d), f32), ((tok, d), f32),
            ((tok, d), bf16), ((tok, d), bf16), ((tok, d), bf16))],
        in_specs=[vmem, vmem] + [ANY] * 3,
        out_specs=[vmem] + [ANY] * 6,
        scratch_shapes=[
            pltpu.VMEM((tok, d), bf16),
            pltpu.VMEM((3, 8, tok), f32),
            pltpu.VMEM((4 * tok, 128), f32),
            pltpu.VMEM((nf, d, tf), bf16),
            pltpu.VMEM((nf, d, tf), bf16),
            pltpu.VMEM((nn, f, tn), bf16),
            pltpu.VMEM((tok, f), bf16),
            pltpu.VMEM((2, tok, tn), f32),
            pltpu.VMEM((2, 128, kt), bf16),
            dma((2 * nf + nn,)), dma((5,)), dma((5,)), dma((3,)), dma((3,)), dma((2,)), dma((2,)),
        ],
        compiler_params=pltpu.CompilerParams(vmem_limit_bytes=62 * MIB, collective_id=1, has_side_effects=True),
        cost_estimate=pl.CostEstimate(flops=12 * tok * d * f, bytes_accessed=6 * d * f, transcendentals=0),
        name="front",
    )(x, mine, w1, w3, w2)


def _up_kernel(el, x0, x1, x2, x3, cx, w1, w3, h, gs, xs, tg, xb, wv, xsem, wsem):
    e = pl.program_id(0)
    tok, d = x0.shape
    ring = wv.shape[0]
    srcs = (x0, x1, x2, x3)
    some = 5

    def wcopy(w, i, k):
        slot = lax.rem(2 * i + k, ring)
        return pltpu.make_async_copy(w.at[i], wv.at[slot], wsem.at[slot])

    xcopy = lambda s, k: pltpu.make_async_copy(srcs[s], xb.at[k], xsem.at[k])

    @pl.when(e == 0)
    def _():
        xcopy(0, 0).start()
        xcopy(1, 1).start()
        for i in range(ring):
            wcopy(w3 if i % 2 else w1, jnp.int32(i // 2), i % 2).start()

        def select(s, _):
            k = lax.rem(s, 2)
            xcopy(0, k).wait()
            c = cx[s]
            for b in range(0, el, some):
                p, g = _hot(c, some * MAIN, b * MAIN, tok)
                for i in range(some):
                    gs[b + i, pl.ds(pl.multiple_of(s * MAIN, MAIN), MAIN), :] = g[i * MAIN:(i + 1) * MAIN]
                for n in range(0, d, 512):
                    r = _dot(p, xb[k, :, n:n + 512]).astype(jnp.bfloat16)
                    for i in range(some):
                        xs[b + i, pl.ds(pl.multiple_of(s * MAIN, MAIN), MAIN), n:n + 512] = r[i * MAIN:(i + 1) * MAIN]
            p, g = _hot(c, el * TAIL, el * MAIN, tok)
            for i in range(el):
                gs[i, pl.ds(pl.multiple_of(4 * MAIN + s * TAIL, TAIL), TAIL), :] = g[i * TAIL:(i + 1) * TAIL]
            for n in range(0, d, 512):
                tg[s, :, n:n + 512] = _dot(p, xb[k, :, n:n + 512])
            for j in range(2):
                @pl.when(s == j)
                def _(j=j):
                    xcopy(2 + j, j).start()
            return 0

        lax.fori_loop(0, 4, select, 0)

    tail = pl.ds(pl.multiple_of(e * TAIL, TAIL), TAIL)
    xs[e, 4 * MAIN:4 * CAP, :] = jnp.concatenate([tg[s, tail, :] for s in range(4)], axis=0).astype(jnp.bfloat16)
    f = h.shape[-1]
    full = f // 256 * 256
    wcopy(w1, e, 0).wait()
    wcopy(w3, e, 1).wait()
    x = xs[e]
    v1, v3 = wv.at[lax.rem(2 * e, ring)], wv.at[lax.rem(2 * e + 1, ring)]
    for n in range(0, full, 256):
        a = _dot(x, v1[:, n:n + 256])
        b = _dot(x, v3[:, n:n + 256])
        h[0, :, n:n + 256] = (jax.nn.silu(a) * b).astype(jnp.bfloat16)
    if full < f:
        r = f - full
        ab = _dot(x, jnp.concatenate([v1[:, full:], v3[:, full:]], axis=1))
        h[0, :, full:] = (jax.nn.silu(ab[:, :r]) * ab[:, r:]).astype(jnp.bfloat16)

    @pl.when(e + 2 < el)
    def _():
        wcopy(w3, e + 2, 1).start()

    @pl.when(e + 3 < el)
    def _():
        wcopy(w1, e + 3, 0).start()


def _up(xs, cx, w1, w3):
    el, d, f = w1.shape
    tok = xs[0].shape[0]
    ring = 5
    return pl.pallas_call(
        functools.partial(_up_kernel, el),
        grid=(el,),
        out_shape=[jax.ShapeDtypeStruct((el, 4 * CAP, f), jnp.bfloat16), jax.ShapeDtypeStruct((el, 4 * CAP, 128), jnp.float32)],
        in_specs=[ANY] * 4 + [pl.BlockSpec(cx.shape, lambda e: (0, 0, 0))] + [ANY] * 2,
        out_specs=[pl.BlockSpec((1, 4 * CAP, f), lambda e: (e, 0, 0)), pl.BlockSpec((el, 4 * CAP, 128), lambda e: (0, 0, 0))],
        scratch_shapes=[
            pltpu.VMEM((el, 4 * CAP, d), jnp.bfloat16),
            pltpu.VMEM((4, el * TAIL, d), jnp.float32),
            pltpu.VMEM((2, tok, d), jnp.bfloat16),
            pltpu.VMEM((ring, d, f), jnp.bfloat16),
            pltpu.SemaphoreType.DMA((2,)),
            pltpu.SemaphoreType.DMA((ring,)),
        ],
        compiler_params=_params(63),
        cost_estimate=pl.CostEstimate(flops=2 * 2 * el * 4 * CAP * d * f, bytes_accessed=4 * el * d * f, transcendentals=0),
        name="up",
    )(*xs, cx, w1, w3)


def _route_kernel(el, tok, cols, g, gs, h, w2, base, sy, out, gv, gsv, hv, wv, r3, rt, send, recv, far, own, back, yb, bv, ost,
                  gsem, hsem, wsem, ssem, rsem, xssem, xrsem, osem, yssem, yrsem, bsem):
    me = lax.axis_index("ep")
    tp = lax.axis_index("tp")
    sib = me + 1 - 2 * lax.rem(me, 2)
    peer = lax.rem(me + 2, 4)
    ring = wv.shape[0]
    chunks = back.shape[0]
    kt = gv.shape[1]
    nm = el * MAIN
    total = chunks * el

    gcopy = lambda s: pltpu.make_async_copy(g.at[pl.ds(s * tok, tok)], gv.at[pl.ds(s * tok, tok)], gsem.at[s])
    hcopy = lambda e: pltpu.make_async_copy(h.at[e], hv.at[e], hsem.at[e])
    gscopy = pltpu.make_async_copy(gs, gsv, gsem.at[4])

    def split(v):
        hi = v.astype(jnp.bfloat16)
        v = v - hi.astype(jnp.float32)
        mid = v.astype(jnp.bfloat16)
        return hi, mid, (v - mid.astype(jnp.float32)).astype(jnp.bfloat16)

    def wcopy(t):
        slot = lax.rem(t, ring)
        col = pl.multiple_of(t // el * cols, cols)
        return pltpu.make_async_copy(w2.at[lax.rem(t, el), :, pl.ds(col, cols)], wv.at[slot], wsem.at[slot])

    def pair(c, k):
        return pltpu.make_async_remote_copy(send.at[lax.rem(c, 2), k], recv.at[c, k], ssem.at[c, k], rsem.at[c, k],
                                            device_id={"ep": sib}, device_id_type=pl.DeviceIdType.MESH)

    def across(c):
        return pltpu.make_async_remote_copy(recv.at[c, 1], back.at[c], xssem.at[c], xrsem.at[c],
                                            device_id={"ep": peer}, device_id_type=pl.DeviceIdType.MESH)

    part = lambda ref, c: ref.at[:, pl.ds(pl.multiple_of(c * cols, cols), cols)]

    def ycopy(c):
        return pltpu.make_async_remote_copy(part(sy, c), yb.at[c], yssem.at[c], yrsem.at[c],
                                            device_id={"tp": 1 - tp}, device_id_type=pl.DeviceIdType.MESH)

    bcopy = lambda c: pltpu.make_async_copy(part(base, c), bv.at[lax.rem(c, 2)], bsem.at[lax.rem(c, 2)])
    ocopy = lambda c: pltpu.make_async_copy(ost.at[lax.rem(c, 2)], part(out, c), osem.at[lax.rem(c, 2)])

    gscopy.start()
    for e in range(el):
        hcopy(e).start()
        if e < ring:
            wcopy(jnp.int32(e)).start()
    for s in (3, 1, 2, 0):
        gcopy(s).start()
    barrier = pltpu.get_barrier_semaphore()
    for dev in (sib, peer):
        pl.semaphore_signal(barrier, inc=1, device_id={"ep": dev}, device_id_type=pl.DeviceIdType.MESH)
    pl.semaphore_signal(barrier, inc=1, device_id={"tp": 1 - tp}, device_id_type=pl.DeviceIdType.MESH)
    pl.semaphore_wait(barrier, 3)
    for c in range(chunks):
        ycopy(jnp.int32(c)).start()
    for c in range(2):
        bcopy(jnp.int32(c)).start()

    def group(c, lo, hi):
        for e in range(lo, hi):
            wcopy(c * el + e).wait()

        @pl.when(c == 0)
        def _():
            if lo == 0:
                gscopy.wait()
            for e in range(lo, hi):
                hcopy(e).wait()

        for e in range(lo, hi):
            r = _dot(hv[e], wv[lax.rem(c * el + e, ring)]).astype(jnp.bfloat16).astype(jnp.float32)
            r = r * jnp.concatenate([gsv[e]] * (cols // 128), axis=1)
            for s in range(4):
                for i, v in enumerate(split(r[s * MAIN:(s + 1) * MAIN])):
                    r3[s, e * MAIN + i * kt:(e + 1) * MAIN + i * kt, :] = v
                rt[s, e * TAIL:(e + 1) * TAIL, :] = r[4 * MAIN + s * TAIL:4 * MAIN + (s + 1) * TAIL]
        for e in range(lo, hi):
            t = c * el + e

            @pl.when(t + ring < total)
            def _(t=t):
                wcopy(t + ring).start()

    def combine(s):
        tail = jnp.concatenate([rt[s], jnp.zeros((kt - el * CAP, cols), jnp.float32)], axis=0)
        for i, v in enumerate(split(tail)):
            r3[s, i * kt + nm:(i + 1) * kt, :] = v
        p = gv[s * tok:(s + 1) * tok, :]
        return sum(_dot(p, r3[s, i * kt:(i + 1) * kt, :]) for i in range(1, 3)) + _dot(p, r3[s, 0:kt, :])

    def merge(c):
        pair(c, 1).wait_recv()
        recv[c, 1] = recv[c, 1] + far[...]
        pair(c, 0).wait_recv()
        recv[c, 0] = recv[c, 0] + own[...]
        across(c).start()

    def chunk(c, _):
        group(c, 0, ring)

        @pl.when(c > 1)
        def _():
            merge(c - 1)

        group(c, ring, el)

        @pl.when(c == 0)
        def _():
            for s in range(4):
                gcopy(s).wait()

        @pl.when(c >= 2)
        def _():
            pair(c - 2, 0).wait_send()
            pair(c - 2, 1).wait_send()

        slot = lax.rem(c, 2)
        send[slot, 1] = combine(3)
        send[slot, 0] = combine(1)
        pair(c, 1).start()
        pair(c, 0).start()
        far[...] = combine(2)
        own[...] = combine(0)

        @pl.when(c == 0)
        def _():
            merge(c)

        return 0

    lax.fori_loop(0, chunks, chunk, 0)
    merge(jnp.int32(chunks - 1))

    def finish(c, _):
        k = lax.rem(c, 2)
        bcopy(c).wait()
        ycopy(c).wait_recv()

        @pl.when(c >= 2)
        def _():
            ocopy(c - 2).wait()

        across(c).wait_recv()
        ost[k] = (bv[k] + yb[c] + (recv[c, 0] + back[c])).astype(jnp.bfloat16)
        ocopy(c).start()

        @pl.when(c + 2 < chunks)
        def _():
            bcopy(c + 2).start()

        return 0

    lax.fori_loop(0, chunks, finish, 0)
    for c in range(chunks - 2, chunks):
        pair(jnp.int32(c), 0).wait_send()
        pair(jnp.int32(c), 1).wait_send()
        ocopy(jnp.int32(c)).wait()
    for c in range(chunks):
        across(jnp.int32(c)).wait_send()
        ycopy(jnp.int32(c)).wait_send()


def _route(g, gs, h, w2, base, sy):
    el, f, d = w2.shape
    tok = base.shape[0]
    cols = 256
    chunks = d // cols
    ring = 8
    kt = g.shape[1]
    f32 = jnp.float32
    return pl.pallas_call(
        functools.partial(_route_kernel, el, tok, cols),
        out_shape=jax.ShapeDtypeStruct((tok, d), jnp.bfloat16),
        in_specs=[ANY] * 6,
        out_specs=ANY,
        scratch_shapes=[
            pltpu.VMEM((4 * tok, kt), jnp.bfloat16),
            pltpu.VMEM(gs.shape, f32),
            pltpu.VMEM((el, 4 * CAP, f), jnp.bfloat16),
            pltpu.VMEM((ring, f, cols), jnp.bfloat16),
            pltpu.VMEM((4, 3 * kt, cols), jnp.bfloat16),
            pltpu.VMEM((4, el * TAIL, cols), f32),
            pltpu.VMEM((2, 2, tok, cols), f32),
            pltpu.VMEM((chunks, 2, tok, cols), f32),
            pltpu.VMEM((tok, cols), f32),
            pltpu.VMEM((tok, cols), f32),
            pltpu.VMEM((chunks, tok, cols), f32),
            pltpu.VMEM((chunks, tok, cols), f32),
            pltpu.VMEM((2, tok, cols), f32),
            pltpu.VMEM((2, tok, cols), jnp.bfloat16),
            pltpu.SemaphoreType.DMA((5,)),
            pltpu.SemaphoreType.DMA((el,)),
            pltpu.SemaphoreType.DMA((ring,)),
            pltpu.SemaphoreType.DMA((chunks, 2)),
            pltpu.SemaphoreType.DMA((chunks, 2)),
            pltpu.SemaphoreType.DMA((chunks,)),
            pltpu.SemaphoreType.DMA((chunks,)),
            pltpu.SemaphoreType.DMA((2,)),
            pltpu.SemaphoreType.DMA((chunks,)),
            pltpu.SemaphoreType.DMA((chunks,)),
            pltpu.SemaphoreType.DMA((2,)),
        ],
        compiler_params=pltpu.CompilerParams(vmem_limit_bytes=63 * MIB, collective_id=0, has_side_effects=True),
        cost_estimate=pl.CostEstimate(flops=2 * el * 4 * CAP * f * d + 24 * tok * kt * d,
                                      bytes_accessed=2 * el * f * d + 2 * el * 4 * CAP * f, transcendentals=0),
        name="route",
    )(g, gs, h, w2, base, sy)


def solution(mesh):
    rows = P(("ep", "tp"), None)
    def body(x, idx, g, slot, ws1, ws3, ws2, w1, w3, w2):
        tok, d = x.shape
        el = w1.shape[0]
        kt = -(-el * CAP // 16) * 16
        code = jnp.where(slot >= 0, idx * 128 + slot, -1).astype(jnp.float32)
        mine = jnp.concatenate([code, g], axis=1).T
        cx, gm, base, sy, xc, xx, xxc = _front(x, mine, ws1, ws3, ws2, el, kt)
        h, gs = _up((x, xc, xx, xxc), cx, w1, w3)
        return _route(gm, gs, h, w2, base, sy)

    return jax.shard_map(
        body, mesh=mesh,
        in_specs=(rows, rows, rows, rows, P(None, "tp"), P(None, "tp"), P("tp", None),
                  P("ep", None, None), P("ep", None, None), P("ep", None, None)),
        out_specs=rows, check_vma=False)
```

```python
import functools

import jax
import jax.numpy as jnp
from jax import lax
from jax.experimental import pallas as pl
from jax.experimental.pallas import tpu as pltpu
from jax.sharding import PartitionSpec as P

CAP = 72
MAIN = 64
TAIL = CAP - MAIN
MIB = 1024 * 1024
ANY = pl.BlockSpec(memory_space=pl.ANY)


def _params(mib):
    return pltpu.CompilerParams(vmem_limit_bytes=mib * MIB)


def _dot(a, b):
    return jnp.dot(a, b, preferred_element_type=jnp.float32)


def _hot(c, n, base, tok):
    r = (lax.broadcasted_iota(jnp.int32, (n, tok), 0) + base).astype(jnp.float32)
    g = jnp.zeros((n, tok), jnp.float32)
    for j in range(4):
        g = jnp.where(r == c[j:j + 1, :], c[4 + j:5 + j, :], g)
    pick = jnp.where(g > 0, 1.0, 0.0).astype(jnp.bfloat16)
    return pick, jnp.broadcast_to(jnp.sum(g, axis=1, keepdims=True), (n, 128))


def _codes(t, me, el):
    code = t[0:4, :].astype(jnp.int32)
    e, k = code >> 7, code & 127
    le = e - me * el
    ok = (code >= 0) & (le >= 0) & (le < el)
    c = jnp.where(ok, jnp.where(k < MAIN, le * MAIN + k, el * MAIN + le * TAIL + k - MAIN), -1).astype(jnp.float32)
    return c


def _front_kernel(el, kt, x, mine, w1, w3, w2, cx, gm, base, sy, xc, xx, xxc,
                  y, tabs, tabt, v1, v3, v2, hs, sst, gst, wsem, xsend, xrecv, tsend, trecv, ssem, gsem):
    me = lax.axis_index("ep")
    tp = lax.axis_index("tp")
    sib = me + 1 - 2 * lax.rem(me, 2)
    peer = lax.rem(me + 2, 4)
    diag = lax.rem(sib + 2, 4)
    tok, d = x.shape
    half = tok // 2
    nf, nn = v1.shape[0], v2.shape[0]
    tf, tn = v1.shape[2], v2.shape[2]
    mesh_id = pl.DeviceIdType.MESH

    def remote(src, dst, ss, rs, dev):
        return pltpu.make_async_remote_copy(src, dst, ss, rs, device_id=dev, device_id_type=mesh_id)

    def up(i):
        col = pl.ds(pl.multiple_of(i * tf, tf), tf)
        return (pltpu.make_async_copy(w1.at[:, col], v1.at[i], wsem.at[i]),
                pltpu.make_async_copy(w3.at[:, col], v3.at[i], wsem.at[nf + i]))

    def down(i):
        return pltpu.make_async_copy(w2.at[:, pl.ds(pl.multiple_of(i * tn, tn), tn)], v2.at[i], wsem.at[2 * nf + i])

    barrier = pltpu.get_barrier_semaphore()
    for dev in (sib, peer, diag):
        pl.semaphore_signal(barrier, inc=1, device_id={"ep": dev}, device_id_type=mesh_id)
    pl.semaphore_signal(barrier, inc=1, device_id={"tp": 1 - tp}, device_id_type=mesh_id)
    pl.semaphore_wait(barrier, 4)
    tcopy = [remote(mine, tabs.at[k], tsend.at[k], trecv.at[k], {"ep": dev}) for k, dev in enumerate((sib, peer, diag))]
    xcopy = remote(x, xx, xsend.at[0], xrecv.at[0], {"ep": peer})
    ccopy = remote(x, xc, xsend.at[1], xrecv.at[1], {"ep": sib})
    ycopy = [remote(x.at[pl.ds(k * half, half)], y.at[pl.ds(k * half, half)], xsend.at[2 + k], xrecv.at[2 + k], {"tp": 1 - tp})
             for k in range(2)]
    relay = remote(xx, xxc, xsend.at[4], xrecv.at[4], {"ep": sib})
    for c in (*tcopy, xcopy, *ycopy, ccopy):
        c.start()
    for i in range(nf):
        for c in up(i):
            c.start()
    for i in range(nn):
        down(i).start()

    def table(k):
        t = mine[...] if k == 0 else tabs[k - 1]
        c = _codes(t, me, el)
        cx[k] = jnp.concatenate([c, t[4:8, :]], axis=0)
        wide = jnp.concatenate([c, jnp.zeros((124, tok), jnp.float32)], axis=0)
        for b in range(0, tok, 128):
            tabt[k * tok + b:k * tok + b + 128, :] = jnp.transpose(wide[:, b:b + 128])

    def shared(src, lo, n, out, add, first):
        scopy = lambda i: pltpu.make_async_copy(
            sst.at[lax.rem(i, 2), pl.ds(0, n)], out.at[pl.ds(lo, n), pl.ds(pl.multiple_of(i * tn, tn), tn)], ssem.at[lax.rem(i, 2)])

        def gate(i, _):
            if first:
                for c in up(i):
                    c.wait()
            r = src[lo:lo + n, :]
            a = _dot(r, v1[i])
            b = _dot(r, v3[i])
            hs[lo:lo + n, pl.ds(pl.multiple_of(i * tf, tf), tf)] = (jax.nn.silu(a) * b).astype(jnp.bfloat16)
            return 0

        def tile(i, _):
            if first:
                down(i).wait()

            @pl.when(i >= 2)
            def _():
                scopy(i - 2).wait()

            r = _dot(hs[lo:lo + n, :], v2[i])
            if add:
                r = r + src[lo:lo + n, pl.ds(pl.multiple_of(i * tn, tn), tn)].astype(jnp.float32)
            sst[lax.rem(i, 2), 0:n, :] = r
            scopy(i).start()
            return 0

        lax.fori_loop(0, nf, gate, 0)
        lax.fori_loop(0, nn, tile, 0)
        for i in (nn - 2, nn - 1):
            scopy(jnp.int32(i)).wait()

    blk = gst.shape[1]
    gcopy = lambda i: pltpu.make_async_copy(gst.at[lax.rem(i, 2)], gm.at[pl.ds(pl.multiple_of(i * blk, blk), blk)], gsem.at[lax.rem(i, 2)])

    def picks(i, _):
        @pl.when(i >= 2)
        def _():
            gcopy(i - 2).wait()

        t = tabt[pl.ds(pl.multiple_of(i * blk, blk), blk), :]
        lane = lax.broadcasted_iota(jnp.int32, (blk, kt), 1).astype(jnp.float32)
        hit = t[:, 0:1] == lane
        for j in range(1, 4):
            hit = hit | (t[:, j:j + 1] == lane)
        gst[lax.rem(i, 2)] = jnp.where(hit, 1.0, 0.0).astype(jnp.bfloat16)
        gcopy(i).start()
        return 0

    ng = tok // blk
    table(0)
    lax.fori_loop(0, ng, picks, 0)
    for k in range(1, 4):
        tcopy[k - 1].wait()
        table(k)
    lax.fori_loop(ng, 4 * ng, picks, 0)
    for i in (4 * ng - 2, 4 * ng - 1):
        gcopy(jnp.int32(i)).wait()
    shared(x, 0, tok, base, True, True)
    ycopy[0].wait()
    shared(y, 0, half, sy, False, False)
    xcopy.wait()
    relay.start()
    ycopy[1].wait()
    shared(y, half, half, sy, False, False)
    ccopy.wait()
    relay.wait()


def _front(x, mine, w1, w3, w2, el, kt):
    tok, d = x.shape
    f = w1.shape[1]
    tf, tn = 256, 512
    nf, nn = f // tf, d // tn
    bf16, f32 = jnp.bfloat16, jnp.float32
    vmem = pl.BlockSpec(memory_space=pltpu.VMEM)
    dma = pltpu.SemaphoreType.DMA
    return pl.pallas_call(
        functools.partial(_front_kernel, el, kt),
        out_shape=[jax.ShapeDtypeStruct(sh, dt) for sh, dt in (
            ((4, 8, tok), f32), ((4 * tok, kt), bf16), ((tok, d), f32), ((tok, d), f32),
            ((tok, d), bf16), ((tok, d), bf16), ((tok, d), bf16))],
        in_specs=[vmem, vmem] + [ANY] * 3,
        out_specs=[vmem] + [ANY] * 6,
        scratch_shapes=[
            pltpu.VMEM((tok, d), bf16),
            pltpu.VMEM((3, 8, tok), f32),
            pltpu.VMEM((4 * tok, 128), f32),
            pltpu.VMEM((nf, d, tf), bf16),
            pltpu.VMEM((nf, d, tf), bf16),
            pltpu.VMEM((nn, f, tn), bf16),
            pltpu.VMEM((tok, f), bf16),
            pltpu.VMEM((2, tok, tn), f32),
            pltpu.VMEM((2, 128, kt), bf16),
            dma((2 * nf + nn,)), dma((5,)), dma((5,)), dma((3,)), dma((3,)), dma((2,)), dma((2,)),
        ],
        compiler_params=pltpu.CompilerParams(vmem_limit_bytes=62 * MIB, collective_id=1, has_side_effects=True),
        cost_estimate=pl.CostEstimate(flops=12 * tok * d * f, bytes_accessed=6 * d * f, transcendentals=0),
        name="front",
    )(x, mine, w1, w3, w2)


def _up_kernel(el, x0, x1, x2, x3, cx, w1, w3, h, gs, xs, tg, xb, wv, xsem, wsem):
    e = pl.program_id(0)
    tok, d = x0.shape
    ring = wv.shape[0]
    srcs = (x0, x1, x2, x3)
    some = 5

    def wcopy(w, i, k):
        slot = lax.rem(2 * i + k, ring)
        return pltpu.make_async_copy(w.at[i], wv.at[slot], wsem.at[slot])

    xcopy = lambda s, k: pltpu.make_async_copy(srcs[s], xb.at[k], xsem.at[k])

    @pl.when(e == 0)
    def _():
        xcopy(0, 0).start()
        xcopy(1, 1).start()
        for i in range(ring):
            wcopy(w3 if i % 2 else w1, jnp.int32(i // 2), i % 2).start()

        def select(s, _):
            k = lax.rem(s, 2)
            xcopy(0, k).wait()
            c = cx[s]
            for b in range(0, el, some):
                p, g = _hot(c, some * MAIN, b * MAIN, tok)
                for i in range(some):
                    gs[b + i, pl.ds(pl.multiple_of(s * MAIN, MAIN), MAIN), :] = g[i * MAIN:(i + 1) * MAIN]
                for n in range(0, d, 512):
                    r = _dot(p, xb[k, :, n:n + 512]).astype(jnp.bfloat16)
                    for i in range(some):
                        xs[b + i, pl.ds(pl.multiple_of(s * MAIN, MAIN), MAIN), n:n + 512] = r[i * MAIN:(i + 1) * MAIN]
            p, g = _hot(c, el * TAIL, el * MAIN, tok)
            for i in range(el):
                gs[i, pl.ds(pl.multiple_of(4 * MAIN + s * TAIL, TAIL), TAIL), :] = g[i * TAIL:(i + 1) * TAIL]
            for n in range(0, d, 512):
                tg[s, :, n:n + 512] = _dot(p, xb[k, :, n:n + 512])
            for j in range(2):
                @pl.when(s == j)
                def _(j=j):
                    xcopy(2 + j, j).start()
            return 0

        lax.fori_loop(0, 4, select, 0)

    tail = pl.ds(pl.multiple_of(e * TAIL, TAIL), TAIL)
    xs[e, 4 * MAIN:4 * CAP, :] = jnp.concatenate([tg[s, tail, :] for s in range(4)], axis=0).astype(jnp.bfloat16)
    f = h.shape[-1]
    full = f // 256 * 256
    wcopy(w1, e, 0).wait()
    wcopy(w3, e, 1).wait()
    x = xs[e]
    v1, v3 = wv.at[lax.rem(2 * e, ring)], wv.at[lax.rem(2 * e + 1, ring)]
    for n in range(0, full, 256):
        a = _dot(x, v1[:, n:n + 256])
        b = _dot(x, v3[:, n:n + 256])
        h[0, :, n:n + 256] = (jax.nn.silu(a) * b).astype(jnp.bfloat16)
    if full < f:
        r = f - full
        ab = _dot(x, jnp.concatenate([v1[:, full:], v3[:, full:]], axis=1))
        h[0, :, full:] = (jax.nn.silu(ab[:, :r]) * ab[:, r:]).astype(jnp.bfloat16)

    @pl.when(e + 2 < el)
    def _():
        wcopy(w3, e + 2, 1).start()

    @pl.when(e + 3 < el)
    def _():
        wcopy(w1, e + 3, 0).start()


def _up(xs, cx, w1, w3):
    el, d, f = w1.shape
    tok = xs[0].shape[0]
    ring = 5
    return pl.pallas_call(
        functools.partial(_up_kernel, el),
        grid=(el,),
        out_shape=[jax.ShapeDtypeStruct((el, 4 * CAP, f), jnp.bfloat16), jax.ShapeDtypeStruct((el, 4 * CAP, 128), jnp.float32)],
        in_specs=[ANY] * 4 + [pl.BlockSpec(cx.shape, lambda e: (0, 0, 0))] + [ANY] * 2,
        out_specs=[pl.BlockSpec((1, 4 * CAP, f), lambda e: (e, 0, 0)), pl.BlockSpec((el, 4 * CAP, 128), lambda e: (0, 0, 0))],
        scratch_shapes=[
            pltpu.VMEM((el, 4 * CAP, d), jnp.bfloat16),
            pltpu.VMEM((4, el * TAIL, d), jnp.float32),
            pltpu.VMEM((2, tok, d), jnp.bfloat16),
            pltpu.VMEM((ring, d, f), jnp.bfloat16),
            pltpu.SemaphoreType.DMA((2,)),
            pltpu.SemaphoreType.DMA((ring,)),
        ],
        compiler_params=_params(63),
        cost_estimate=pl.CostEstimate(flops=2 * 2 * el * 4 * CAP * d * f, bytes_accessed=4 * el * d * f, transcendentals=0),
        name="up",
    )(*xs, cx, w1, w3)


def _route_kernel(el, tok, cols, g, gs, h, w2, base, sy, out, gv, gsv, hv, wv, r3, rt, send, recv, far, own, back, yb, bv, ost,
                  gsem, hsem, wsem, ssem, rsem, xssem, xrsem, osem, yssem, yrsem, bsem):
    me = lax.axis_index("ep")
    tp = lax.axis_index("tp")
    sib = me + 1 - 2 * lax.rem(me, 2)
    peer = lax.rem(me + 2, 4)
    ring = wv.shape[0]
    chunks = back.shape[0]
    kt = gv.shape[1]
    nm = el * MAIN
    total = chunks * el

    gcopy = lambda s: pltpu.make_async_copy(g.at[pl.ds(s * tok, tok)], gv.at[pl.ds(s * tok, tok)], gsem.at[s])
    hcopy = lambda e: pltpu.make_async_copy(h.at[e], hv.at[e], hsem.at[e])
    gscopy = pltpu.make_async_copy(gs, gsv, gsem.at[4])

    def split(v):
        hi = v.astype(jnp.bfloat16)
        v = v - hi.astype(jnp.float32)
        mid = v.astype(jnp.bfloat16)
        return hi, mid, (v - mid.astype(jnp.float32)).astype(jnp.bfloat16)

    def wcopy(t):
        slot = lax.rem(t, ring)
        col = pl.multiple_of(t // el * cols, cols)
        return pltpu.make_async_copy(w2.at[lax.rem(t, el), :, pl.ds(col, cols)], wv.at[slot], wsem.at[slot])

    def pair(c, k):
        return pltpu.make_async_remote_copy(send.at[lax.rem(c, 2), k], recv.at[c, k], ssem.at[c, k], rsem.at[c, k],
                                            device_id={"ep": sib}, device_id_type=pl.DeviceIdType.MESH)

    def across(c):
        return pltpu.make_async_remote_copy(recv.at[c, 1], back.at[c], xssem.at[c], xrsem.at[c],
                                            device_id={"ep": peer}, device_id_type=pl.DeviceIdType.MESH)

    part = lambda ref, c: ref.at[:, pl.ds(pl.multiple_of(c * cols, cols), cols)]

    def ycopy(c):
        return pltpu.make_async_remote_copy(part(sy, c), yb.at[c], yssem.at[c], yrsem.at[c],
                                            device_id={"tp": 1 - tp}, device_id_type=pl.DeviceIdType.MESH)

    bcopy = lambda c: pltpu.make_async_copy(part(base, c), bv.at[lax.rem(c, 2)], bsem.at[lax.rem(c, 2)])
    ocopy = lambda c: pltpu.make_async_copy(ost.at[lax.rem(c, 2)], part(out, c), osem.at[lax.rem(c, 2)])

    first = (el + 1) // 2
    gscopy.start()
    for e in range(first):
        hcopy(e).start()
        wcopy(jnp.int32(e)).start()
    barrier = pltpu.get_barrier_semaphore()
    for dev in (sib, peer):
        pl.semaphore_signal(barrier, inc=1, device_id={"ep": dev}, device_id_type=pl.DeviceIdType.MESH)
    pl.semaphore_signal(barrier, inc=1, device_id={"tp": 1 - tp}, device_id_type=pl.DeviceIdType.MESH)
    pl.semaphore_wait(barrier, 3)
    for c in range(chunks):
        ycopy(jnp.int32(c)).start()

    def group(c, lo, hi):
        for e in range(lo, hi):
            wcopy(c * el + e).wait()

        @pl.when(c == 0)
        def _():
            if lo == 0:
                gscopy.wait()
            for e in range(lo, hi):
                hcopy(e).wait()
            if lo == 0:
                for e in range(hi, el):
                    hcopy(e).start()
                    wcopy(jnp.int32(e)).start()
            else:
                for s in (3, 1, 2, 0):
                    gcopy(s).start()
                for b in range(2):
                    bcopy(jnp.int32(b)).start()

        for e in range(lo, hi):
            r = _dot(hv[e], wv[lax.rem(c * el + e, ring)]).astype(jnp.bfloat16).astype(jnp.float32)
            r = r * jnp.concatenate([gsv[e]] * (cols // 128), axis=1)
            for s in range(4):
                for i, v in enumerate(split(r[s * MAIN:(s + 1) * MAIN])):
                    r3[s, e * MAIN + i * kt:(e + 1) * MAIN + i * kt, :] = v
                rt[s, e * TAIL:(e + 1) * TAIL, :] = r[4 * MAIN + s * TAIL:4 * MAIN + (s + 1) * TAIL]
        for e in range(lo, hi):
            t = c * el + e

            @pl.when(t + ring < total)
            def _(t=t):
                wcopy(t + ring).start()

    def combine(s):
        tail = jnp.concatenate([rt[s], jnp.zeros((kt - el * CAP, cols), jnp.float32)], axis=0)
        for i, v in enumerate(split(tail)):
            r3[s, i * kt + nm:(i + 1) * kt, :] = v
        p = gv[s * tok:(s + 1) * tok, :]
        return sum(_dot(p, r3[s, i * kt:(i + 1) * kt, :]) for i in range(1, 3)) + _dot(p, r3[s, 0:kt, :])

    def merge(c):
        pair(c, 1).wait_recv()
        recv[c, 1] = recv[c, 1] + far[...]
        pair(c, 0).wait_recv()
        recv[c, 0] = recv[c, 0] + own[...]
        across(c).start()

    def chunk(c, _):
        group(c, 0, first)

        @pl.when(c > 1)
        def _():
            merge(c - 1)

        group(c, first, el)

        @pl.when(c == 0)
        def _():
            for s in range(4):
                gcopy(s).wait()

        @pl.when(c >= 2)
        def _():
            pair(c - 2, 0).wait_send()
            pair(c - 2, 1).wait_send()

        slot = lax.rem(c, 2)
        send[slot, 1] = combine(3)
        send[slot, 0] = combine(1)
        pair(c, 1).start()
        pair(c, 0).start()
        far[...] = combine(2)
        own[...] = combine(0)

        @pl.when(c == 0)
        def _():
            merge(c)

        return 0

    lax.fori_loop(0, chunks, chunk, 0)
    merge(jnp.int32(chunks - 1))

    def finish(c, _):
        k = lax.rem(c, 2)
        bcopy(c).wait()
        ycopy(c).wait_recv()

        @pl.when(c >= 2)
        def _():
            ocopy(c - 2).wait()

        across(c).wait_recv()
        ost[k] = (bv[k] + yb[c] + (recv[c, 0] + back[c])).astype(jnp.bfloat16)
        ocopy(c).start()

        @pl.when(c + 2 < chunks)
        def _():
            bcopy(c + 2).start()

        return 0

    lax.fori_loop(0, chunks, finish, 0)
    for c in range(chunks - 2, chunks):
        pair(jnp.int32(c), 0).wait_send()
        pair(jnp.int32(c), 1).wait_send()
        ocopy(jnp.int32(c)).wait()
    for c in range(chunks):
        across(jnp.int32(c)).wait_send()
        ycopy(jnp.int32(c)).wait_send()


def _route(g, gs, h, w2, base, sy):
    el, f, d = w2.shape
    tok = base.shape[0]
    cols = 256
    chunks = d // cols
    ring = el
    kt = g.shape[1]
    f32 = jnp.float32
    return pl.pallas_call(
        functools.partial(_route_kernel, el, tok, cols),
        out_shape=jax.ShapeDtypeStruct((tok, d), jnp.bfloat16),
        in_specs=[ANY] * 6,
        out_specs=ANY,
        scratch_shapes=[
            pltpu.VMEM((4 * tok, kt), jnp.bfloat16),
            pltpu.VMEM(gs.shape, f32),
            pltpu.VMEM((el, 4 * CAP, f), jnp.bfloat16),
            pltpu.VMEM((ring, f, cols), jnp.bfloat16),
            pltpu.VMEM((4, 3 * kt, cols), jnp.bfloat16),
            pltpu.VMEM((4, el * TAIL, cols), f32),
            pltpu.VMEM((2, 2, tok, cols), f32),
            pltpu.VMEM((chunks, 2, tok, cols), f32),
            pltpu.VMEM((tok, cols), f32),
            pltpu.VMEM((tok, cols), f32),
            pltpu.VMEM((chunks, tok, cols), f32),
            pltpu.VMEM((chunks, tok, cols), f32),
            pltpu.VMEM((2, tok, cols), f32),
            pltpu.VMEM((2, tok, cols), jnp.bfloat16),
            pltpu.SemaphoreType.DMA((5,)),
            pltpu.SemaphoreType.DMA((el,)),
            pltpu.SemaphoreType.DMA((ring,)),
            pltpu.SemaphoreType.DMA((chunks, 2)),
            pltpu.SemaphoreType.DMA((chunks, 2)),
            pltpu.SemaphoreType.DMA((chunks,)),
            pltpu.SemaphoreType.DMA((chunks,)),
            pltpu.SemaphoreType.DMA((2,)),
            pltpu.SemaphoreType.DMA((chunks,)),
            pltpu.SemaphoreType.DMA((chunks,)),
            pltpu.SemaphoreType.DMA((2,)),
        ],
        compiler_params=pltpu.CompilerParams(vmem_limit_bytes=63 * MIB, collective_id=0, has_side_effects=True),
        cost_estimate=pl.CostEstimate(flops=2 * el * 4 * CAP * f * d + 24 * tok * kt * d,
                                      bytes_accessed=2 * el * f * d + 2 * el * 4 * CAP * f, transcendentals=0),
        name="route",
    )(g, gs, h, w2, base, sy)


def solution(mesh):
    rows = P(("ep", "tp"), None)
    def body(x, idx, g, slot, ws1, ws3, ws2, w1, w3, w2):
        tok, d = x.shape
        el = w1.shape[0]
        kt = -(-el * CAP // 16) * 16
        code = jnp.where(slot >= 0, idx * 128 + slot, -1).astype(jnp.float32)
        mine = jnp.concatenate([code, g], axis=1).T
        cx, gm, base, sy, xc, xx, xxc = _front(x, mine, ws1, ws3, ws2, el, kt)
        h, gs = _up((x, xc, xx, xxc), cx, w1, w3)
        return _route(gm, gs, h, w2, base, sy)

    return jax.shard_map(
        body, mesh=mesh,
        in_specs=(rows, rows, rows, rows, P(None, "tp"), P(None, "tp"), P("tp", None),
                  P("ep", None, None), P("ep", None, None), P("ep", None, None)),
        out_specs=rows, check_vma=False)
```

```python
import functools

import jax
import jax.numpy as jnp
from jax import lax
from jax.experimental import pallas as pl
from jax.experimental.pallas import tpu as pltpu
from jax.sharding import PartitionSpec as P

CAP = 72
MAIN = 64
TAIL = CAP - MAIN
MIB = 1024 * 1024
ANY = pl.BlockSpec(memory_space=pl.ANY)


def _params(mib):
    return pltpu.CompilerParams(vmem_limit_bytes=mib * MIB)


def _dot(a, b):
    return jnp.dot(a, b, preferred_element_type=jnp.float32)


def _hot(c, n, base, tok):
    r = (lax.broadcasted_iota(jnp.int32, (n, tok), 0) + base).astype(jnp.float32)
    g = jnp.zeros((n, tok), jnp.float32)
    for j in range(4):
        g = jnp.where(r == c[j:j + 1, :], c[4 + j:5 + j, :], g)
    pick = jnp.where(g > 0, 1.0, 0.0).astype(jnp.bfloat16)
    return pick, jnp.broadcast_to(jnp.sum(g, axis=1, keepdims=True), (n, 128))


def _codes(t, me, el):
    code = t[0:4, :].astype(jnp.int32)
    e, k = code >> 7, code & 127
    le = e - me * el
    ok = (code >= 0) & (le >= 0) & (le < el)
    c = jnp.where(ok, jnp.where(k < MAIN, le * MAIN + k, el * MAIN + le * TAIL + k - MAIN), -1).astype(jnp.float32)
    return c


def _front_kernel(el, kt, x, mine, w1, w3, w2, cx, gm, base, sy, xc, xx, xxc,
                  y, tabs, tabt, v1, v3, v2, hs, sst, gst, wsem, xsend, xrecv, tsend, trecv, ssem, gsem):
    me = lax.axis_index("ep")
    tp = lax.axis_index("tp")
    sib = me + 1 - 2 * lax.rem(me, 2)
    peer = lax.rem(me + 2, 4)
    diag = lax.rem(sib + 2, 4)
    tok, d = x.shape
    parts = ((0, tok * 5 // 8), (tok * 5 // 8, tok * 3 // 8))
    nf, nn = v1.shape[0], v2.shape[0]
    tf, tn = v1.shape[2], v2.shape[2]
    mesh_id = pl.DeviceIdType.MESH

    def remote(src, dst, ss, rs, dev):
        return pltpu.make_async_remote_copy(src, dst, ss, rs, device_id=dev, device_id_type=mesh_id)

    def up(i):
        col = pl.ds(pl.multiple_of(i * tf, tf), tf)
        return (pltpu.make_async_copy(w1.at[:, col], v1.at[i], wsem.at[i]),
                pltpu.make_async_copy(w3.at[:, col], v3.at[i], wsem.at[nf + i]))

    def down(i):
        return pltpu.make_async_copy(w2.at[:, pl.ds(pl.multiple_of(i * tn, tn), tn)], v2.at[i], wsem.at[2 * nf + i])

    barrier = pltpu.get_barrier_semaphore()
    for dev in (sib, peer, diag):
        pl.semaphore_signal(barrier, inc=1, device_id={"ep": dev}, device_id_type=mesh_id)
    pl.semaphore_signal(barrier, inc=1, device_id={"tp": 1 - tp}, device_id_type=mesh_id)
    pl.semaphore_wait(barrier, 4)
    tcopy = [remote(mine, tabs.at[k], tsend.at[k], trecv.at[k], {"ep": dev}) for k, dev in enumerate((sib, peer, diag))]
    xcopy = remote(x, xx, xsend.at[0], xrecv.at[0], {"ep": peer})
    ccopy = remote(x, xc, xsend.at[1], xrecv.at[1], {"ep": sib})
    ycopy = [remote(x.at[pl.ds(*r)], y.at[pl.ds(*r)], xsend.at[2 + k], xrecv.at[2 + k], {"tp": 1 - tp})
             for k, r in enumerate(parts)]
    relay = remote(xx, xxc, xsend.at[4], xrecv.at[4], {"ep": sib})
    for c in (*tcopy, xcopy, *ycopy, ccopy):
        c.start()
    for i in range(nf):
        for c in up(i):
            c.start()
    for i in range(nn):
        down(i).start()

    def table(k):
        t = mine[...] if k == 0 else tabs[k - 1]
        c = _codes(t, me, el)
        cx[k] = jnp.concatenate([c, t[4:8, :]], axis=0)
        wide = jnp.concatenate([c, jnp.zeros((124, tok), jnp.float32)], axis=0)
        for b in range(0, tok, 128):
            tabt[k * tok + b:k * tok + b + 128, :] = jnp.transpose(wide[:, b:b + 128])

    def shared(src, lo, n, out, add, first):
        scopy = lambda i: pltpu.make_async_copy(
            sst.at[lax.rem(i, 2), pl.ds(0, n)], out.at[pl.ds(lo, n), pl.ds(pl.multiple_of(i * tn, tn), tn)], ssem.at[lax.rem(i, 2)])

        def gate(i, _):
            if first:
                for c in up(i):
                    c.wait()
            r = src[lo:lo + n, :]
            a = _dot(r, v1[i])
            b = _dot(r, v3[i])
            hs[lo:lo + n, pl.ds(pl.multiple_of(i * tf, tf), tf)] = (jax.nn.silu(a) * b).astype(jnp.bfloat16)
            return 0

        def tile(i, _):
            if first:
                down(i).wait()

            @pl.when(i >= 2)
            def _():
                scopy(i - 2).wait()

            r = _dot(hs[lo:lo + n, :], v2[i])
            if add:
                r = r + src[lo:lo + n, pl.ds(pl.multiple_of(i * tn, tn), tn)].astype(jnp.float32)
            sst[lax.rem(i, 2), 0:n, :] = r
            scopy(i).start()
            return 0

        lax.fori_loop(0, nf, gate, 0)
        lax.fori_loop(0, nn, tile, 0)
        for i in (nn - 2, nn - 1):
            scopy(jnp.int32(i)).wait()

    blk = gst.shape[1]
    gcopy = lambda i: pltpu.make_async_copy(gst.at[lax.rem(i, 2)], gm.at[pl.ds(pl.multiple_of(i * blk, blk), blk)], gsem.at[lax.rem(i, 2)])

    def picks(i, _):
        @pl.when(i >= 2)
        def _():
            gcopy(i - 2).wait()

        t = tabt[pl.ds(pl.multiple_of(i * blk, blk), blk), :]
        lane = lax.broadcasted_iota(jnp.int32, (blk, kt), 1).astype(jnp.float32)
        hit = t[:, 0:1] == lane
        for j in range(1, 4):
            hit = hit | (t[:, j:j + 1] == lane)
        gst[lax.rem(i, 2)] = jnp.where(hit, 1.0, 0.0).astype(jnp.bfloat16)
        gcopy(i).start()
        return 0

    ng = tok // blk
    table(0)
    lax.fori_loop(0, ng, picks, 0)
    for k in range(1, 4):
        tcopy[k - 1].wait()
        table(k)
    lax.fori_loop(ng, 4 * ng, picks, 0)
    for i in (4 * ng - 2, 4 * ng - 1):
        gcopy(jnp.int32(i)).wait()
    shared(x, 0, tok, base, True, True)
    ycopy[0].wait()
    shared(y, *parts[0], sy, False, False)
    xcopy.wait()
    relay.start()
    ycopy[1].wait()
    shared(y, *parts[1], sy, False, False)
    ccopy.wait()
    relay.wait()


def _front(x, mine, w1, w3, w2, el, kt):
    tok, d = x.shape
    f = w1.shape[1]
    tf, tn = 256, 512
    nf, nn = f // tf, d // tn
    bf16, f32 = jnp.bfloat16, jnp.float32
    vmem = pl.BlockSpec(memory_space=pltpu.VMEM)
    dma = pltpu.SemaphoreType.DMA
    return pl.pallas_call(
        functools.partial(_front_kernel, el, kt),
        out_shape=[jax.ShapeDtypeStruct(sh, dt) for sh, dt in (
            ((4, 8, tok), f32), ((4 * tok, kt), bf16), ((tok, d), f32), ((tok, d), f32),
            ((tok, d), bf16), ((tok, d), bf16), ((tok, d), bf16))],
        in_specs=[vmem, vmem] + [ANY] * 3,
        out_specs=[vmem] + [ANY] * 6,
        scratch_shapes=[
            pltpu.VMEM((tok, d), bf16),
            pltpu.VMEM((3, 8, tok), f32),
            pltpu.VMEM((4 * tok, 128), f32),
            pltpu.VMEM((nf, d, tf), bf16),
            pltpu.VMEM((nf, d, tf), bf16),
            pltpu.VMEM((nn, f, tn), bf16),
            pltpu.VMEM((tok, f), bf16),
            pltpu.VMEM((2, tok, tn), f32),
            pltpu.VMEM((2, 128, kt), bf16),
            dma((2 * nf + nn,)), dma((5,)), dma((5,)), dma((3,)), dma((3,)), dma((2,)), dma((2,)),
        ],
        compiler_params=pltpu.CompilerParams(vmem_limit_bytes=62 * MIB, collective_id=1, has_side_effects=True),
        cost_estimate=pl.CostEstimate(flops=12 * tok * d * f, bytes_accessed=6 * d * f, transcendentals=0),
        name="front",
    )(x, mine, w1, w3, w2)


def _up_kernel(el, x0, x1, x2, x3, cx, w1, w3, h, gs, xs, tg, xb, wv, xsem, wsem):
    e = pl.program_id(0)
    tok, d = x0.shape
    ring = wv.shape[0]
    srcs = (x0, x1, x2, x3)
    some = 5

    def wcopy(w, i, k):
        slot = lax.rem(2 * i + k, ring)
        return pltpu.make_async_copy(w.at[i], wv.at[slot], wsem.at[slot])

    xcopy = lambda s, k: pltpu.make_async_copy(srcs[s], xb.at[k], xsem.at[k])

    @pl.when(e == 0)
    def _():
        xcopy(0, 0).start()
        xcopy(1, 1).start()
        for i in range(ring):
            wcopy(w3 if i % 2 else w1, jnp.int32(i // 2), i % 2).start()

        def select(s, _):
            k = lax.rem(s, 2)
            xcopy(0, k).wait()
            c = cx[s]
            for b in range(0, el, some):
                p, g = _hot(c, some * MAIN, b * MAIN, tok)
                for i in range(some):
                    gs[b + i, pl.ds(pl.multiple_of(s * MAIN, MAIN), MAIN), :] = g[i * MAIN:(i + 1) * MAIN]
                for n in range(0, d, 512):
                    r = _dot(p, xb[k, :, n:n + 512]).astype(jnp.bfloat16)
                    for i in range(some):
                        xs[b + i, pl.ds(pl.multiple_of(s * MAIN, MAIN), MAIN), n:n + 512] = r[i * MAIN:(i + 1) * MAIN]
            p, g = _hot(c, el * TAIL, el * MAIN, tok)
            for i in range(el):
                gs[i, pl.ds(pl.multiple_of(4 * MAIN + s * TAIL, TAIL), TAIL), :] = g[i * TAIL:(i + 1) * TAIL]
            for n in range(0, d, 512):
                tg[s, :, n:n + 512] = _dot(p, xb[k, :, n:n + 512])
            for j in range(2):
                @pl.when(s == j)
                def _(j=j):
                    xcopy(2 + j, j).start()
            return 0

        lax.fori_loop(0, 4, select, 0)

    tail = pl.ds(pl.multiple_of(e * TAIL, TAIL), TAIL)
    xs[e, 4 * MAIN:4 * CAP, :] = jnp.concatenate([tg[s, tail, :] for s in range(4)], axis=0).astype(jnp.bfloat16)
    f = h.shape[-1]
    full = f // 256 * 256
    wcopy(w1, e, 0).wait()
    wcopy(w3, e, 1).wait()
    x = xs[e]
    v1, v3 = wv.at[lax.rem(2 * e, ring)], wv.at[lax.rem(2 * e + 1, ring)]
    for n in range(0, full, 256):
        a = _dot(x, v1[:, n:n + 256])
        b = _dot(x, v3[:, n:n + 256])
        h[0, :, n:n + 256] = (jax.nn.silu(a) * b).astype(jnp.bfloat16)
    if full < f:
        r = f - full
        ab = _dot(x, jnp.concatenate([v1[:, full:], v3[:, full:]], axis=1))
        h[0, :, full:] = (jax.nn.silu(ab[:, :r]) * ab[:, r:]).astype(jnp.bfloat16)

    @pl.when(e + 2 < el)
    def _():
        wcopy(w3, e + 2, 1).start()

    @pl.when(e + 3 < el)
    def _():
        wcopy(w1, e + 3, 0).start()


def _up(xs, cx, w1, w3):
    el, d, f = w1.shape
    tok = xs[0].shape[0]
    ring = 5
    return pl.pallas_call(
        functools.partial(_up_kernel, el),
        grid=(el,),
        out_shape=[jax.ShapeDtypeStruct((el, 4 * CAP, f), jnp.bfloat16), jax.ShapeDtypeStruct((el, 4 * CAP, 128), jnp.float32)],
        in_specs=[ANY] * 4 + [pl.BlockSpec(cx.shape, lambda e: (0, 0, 0))] + [ANY] * 2,
        out_specs=[pl.BlockSpec((1, 4 * CAP, f), lambda e: (e, 0, 0)), pl.BlockSpec((el, 4 * CAP, 128), lambda e: (0, 0, 0))],
        scratch_shapes=[
            pltpu.VMEM((el, 4 * CAP, d), jnp.bfloat16),
            pltpu.VMEM((4, el * TAIL, d), jnp.float32),
            pltpu.VMEM((2, tok, d), jnp.bfloat16),
            pltpu.VMEM((ring, d, f), jnp.bfloat16),
            pltpu.SemaphoreType.DMA((2,)),
            pltpu.SemaphoreType.DMA((ring,)),
        ],
        compiler_params=_params(63),
        cost_estimate=pl.CostEstimate(flops=2 * 2 * el * 4 * CAP * d * f, bytes_accessed=4 * el * d * f, transcendentals=0),
        name="up",
    )(*xs, cx, w1, w3)


def _route_kernel(el, tok, cols, g, gs, h, w2, base, sy, out, gv, gsv, hv, wv, r3, rt, send, recv, far, own, back, yb, bv, ost,
                  gsem, hsem, wsem, ssem, rsem, xssem, xrsem, osem, yssem, yrsem, bsem):
    me = lax.axis_index("ep")
    tp = lax.axis_index("tp")
    sib = me + 1 - 2 * lax.rem(me, 2)
    peer = lax.rem(me + 2, 4)
    ring = wv.shape[0]
    chunks = back.shape[0]
    kt = gv.shape[1]
    nm = el * MAIN
    total = chunks * el

    gcopy = lambda s: pltpu.make_async_copy(g.at[pl.ds(s * tok, tok)], gv.at[pl.ds(s * tok, tok)], gsem.at[s])
    hcopy = lambda e: pltpu.make_async_copy(h.at[e], hv.at[e], hsem.at[e])
    gscopy = pltpu.make_async_copy(gs, gsv, gsem.at[4])

    def split(v):
        hi = v.astype(jnp.bfloat16)
        v = v - hi.astype(jnp.float32)
        mid = v.astype(jnp.bfloat16)
        return hi, mid, (v - mid.astype(jnp.float32)).astype(jnp.bfloat16)

    def wcopy(t):
        slot = lax.rem(t, ring)
        col = pl.multiple_of(t // el * cols, cols)
        return pltpu.make_async_copy(w2.at[lax.rem(t, el), :, pl.ds(col, cols)], wv.at[slot], wsem.at[slot])

    def pair(c, k):
        return pltpu.make_async_remote_copy(send.at[lax.rem(c, 2), k], recv.at[c, k], ssem.at[c, k], rsem.at[c, k],
                                            device_id={"ep": sib}, device_id_type=pl.DeviceIdType.MESH)

    def across(c):
        return pltpu.make_async_remote_copy(recv.at[c, 1], back.at[c], xssem.at[c], xrsem.at[c],
                                            device_id={"ep": peer}, device_id_type=pl.DeviceIdType.MESH)

    part = lambda ref, c: ref.at[:, pl.ds(pl.multiple_of(c * cols, cols), cols)]

    def ycopy(c):
        return pltpu.make_async_remote_copy(part(sy, c), yb.at[c], yssem.at[c], yrsem.at[c],
                                            device_id={"tp": 1 - tp}, device_id_type=pl.DeviceIdType.MESH)

    bcopy = lambda c: pltpu.make_async_copy(part(base, c), bv.at[lax.rem(c, 2)], bsem.at[lax.rem(c, 2)])
    ocopy = lambda c: pltpu.make_async_copy(ost.at[lax.rem(c, 2)], part(out, c), osem.at[lax.rem(c, 2)])

    first = (el + 1) // 2
    gscopy.start()
    for e in range(first):
        hcopy(e).start()
        wcopy(jnp.int32(e)).start()
    barrier = pltpu.get_barrier_semaphore()
    for dev in (sib, peer):
        pl.semaphore_signal(barrier, inc=1, device_id={"ep": dev}, device_id_type=pl.DeviceIdType.MESH)
    pl.semaphore_signal(barrier, inc=1, device_id={"tp": 1 - tp}, device_id_type=pl.DeviceIdType.MESH)
    pl.semaphore_wait(barrier, 3)

    def group(c, lo, hi):
        for e in range(lo, hi):
            wcopy(c * el + e).wait()

        @pl.when(c == 0)
        def _():
            if lo == 0:
                gscopy.wait()
            for e in range(lo, hi):
                hcopy(e).wait()
            if lo == 0:
                for e in range(hi, el):
                    hcopy(e).start()
                    wcopy(jnp.int32(e)).start()
            else:
                for s in (3, 1, 2, 0):
                    gcopy(s).start()
                for b in range(2):
                    bcopy(jnp.int32(b)).start()

        for e in range(lo, hi):
            r = _dot(hv[e], wv[lax.rem(c * el + e, ring)]).astype(jnp.bfloat16).astype(jnp.float32)
            r = r * jnp.concatenate([gsv[e]] * (cols // 128), axis=1)
            for s in range(4):
                for i, v in enumerate(split(r[s * MAIN:(s + 1) * MAIN])):
                    r3[s, e * MAIN + i * kt:(e + 1) * MAIN + i * kt, :] = v
                rt[s, e * TAIL:(e + 1) * TAIL, :] = r[4 * MAIN + s * TAIL:4 * MAIN + (s + 1) * TAIL]
        for e in range(lo, hi):
            t = c * el + e

            @pl.when(t + ring < total)
            def _(t=t):
                wcopy(t + ring).start()

    def combine(s):
        tail = jnp.concatenate([rt[s], jnp.zeros((kt - el * CAP, cols), jnp.float32)], axis=0)
        for i, v in enumerate(split(tail)):
            r3[s, i * kt + nm:(i + 1) * kt, :] = v
        p = gv[s * tok:(s + 1) * tok, :]
        return sum(_dot(p, r3[s, i * kt:(i + 1) * kt, :]) for i in range(1, 3)) + _dot(p, r3[s, 0:kt, :])

    def merge(c):
        pair(c, 1).wait_recv()
        recv[c, 1] = recv[c, 1] + far[...]
        pair(c, 0).wait_recv()
        recv[c, 0] = recv[c, 0] + own[...]
        across(c).start()

    def chunk(c, _):
        group(c, 0, first)
        ycopy(c).start()

        @pl.when(c > 1)
        def _():
            merge(c - 1)

        group(c, first, el)

        @pl.when(c == 0)
        def _():
            for s in range(4):
                gcopy(s).wait()

        @pl.when(c >= 2)
        def _():
            pair(c - 2, 0).wait_send()
            pair(c - 2, 1).wait_send()

        slot = lax.rem(c, 2)
        send[slot, 1] = combine(3)
        send[slot, 0] = combine(1)
        pair(c, 1).start()
        pair(c, 0).start()
        far[...] = combine(2)
        own[...] = combine(0)

        @pl.when(c == 0)
        def _():
            merge(c)

        return 0

    lax.fori_loop(0, chunks, chunk, 0)
    merge(jnp.int32(chunks - 1))

    def finish(c, _):
        k = lax.rem(c, 2)
        bcopy(c).wait()
        ycopy(c).wait_recv()

        @pl.when(c >= 2)
        def _():
            ocopy(c - 2).wait()

        across(c).wait_recv()
        ost[k] = (bv[k] + yb[c] + (recv[c, 0] + back[c])).astype(jnp.bfloat16)
        ocopy(c).start()

        @pl.when(c + 2 < chunks)
        def _():
            bcopy(c + 2).start()

        return 0

    lax.fori_loop(0, chunks, finish, 0)
    for c in range(chunks - 2, chunks):
        pair(jnp.int32(c), 0).wait_send()
        pair(jnp.int32(c), 1).wait_send()
        ocopy(jnp.int32(c)).wait()
    for c in range(chunks):
        across(jnp.int32(c)).wait_send()
        ycopy(jnp.int32(c)).wait_send()


def _route(g, gs, h, w2, base, sy):
    el, f, d = w2.shape
    tok = base.shape[0]
    cols = 256
    chunks = d // cols
    ring = el
    kt = g.shape[1]
    f32 = jnp.float32
    return pl.pallas_call(
        functools.partial(_route_kernel, el, tok, cols),
        out_shape=jax.ShapeDtypeStruct((tok, d), jnp.bfloat16),
        in_specs=[ANY] * 6,
        out_specs=ANY,
        scratch_shapes=[
            pltpu.VMEM((4 * tok, kt), jnp.bfloat16),
            pltpu.VMEM(gs.shape, f32),
            pltpu.VMEM((el, 4 * CAP, f), jnp.bfloat16),
            pltpu.VMEM((ring, f, cols), jnp.bfloat16),
            pltpu.VMEM((4, 3 * kt, cols), jnp.bfloat16),
            pltpu.VMEM((4, el * TAIL, cols), f32),
            pltpu.VMEM((2, 2, tok, cols), f32),
            pltpu.VMEM((chunks, 2, tok, cols), f32),
            pltpu.VMEM((tok, cols), f32),
            pltpu.VMEM((tok, cols), f32),
            pltpu.VMEM((chunks, tok, cols), f32),
            pltpu.VMEM((chunks, tok, cols), f32),
            pltpu.VMEM((2, tok, cols), f32),
            pltpu.VMEM((2, tok, cols), jnp.bfloat16),
            pltpu.SemaphoreType.DMA((5,)),
            pltpu.SemaphoreType.DMA((el,)),
            pltpu.SemaphoreType.DMA((ring,)),
            pltpu.SemaphoreType.DMA((chunks, 2)),
            pltpu.SemaphoreType.DMA((chunks, 2)),
            pltpu.SemaphoreType.DMA((chunks,)),
            pltpu.SemaphoreType.DMA((chunks,)),
            pltpu.SemaphoreType.DMA((2,)),
            pltpu.SemaphoreType.DMA((chunks,)),
            pltpu.SemaphoreType.DMA((chunks,)),
            pltpu.SemaphoreType.DMA((2,)),
        ],
        compiler_params=pltpu.CompilerParams(vmem_limit_bytes=63 * MIB, collective_id=0, has_side_effects=True),
        cost_estimate=pl.CostEstimate(flops=2 * el * 4 * CAP * f * d + 24 * tok * kt * d,
                                      bytes_accessed=2 * el * f * d + 2 * el * 4 * CAP * f, transcendentals=0),
        name="route",
    )(g, gs, h, w2, base, sy)


def solution(mesh):
    rows = P(("ep", "tp"), None)
    def body(x, idx, g, slot, ws1, ws3, ws2, w1, w3, w2):
        tok, d = x.shape
        el = w1.shape[0]
        kt = -(-el * CAP // 16) * 16
        code = jnp.where(slot >= 0, idx * 128 + slot, -1).astype(jnp.float32)
        mine = jnp.concatenate([code, g], axis=1).T
        cx, gm, base, sy, xc, xx, xxc = _front(x, mine, ws1, ws3, ws2, el, kt)
        h, gs = _up((x, xc, xx, xxc), cx, w1, w3)
        return _route(gm, gs, h, w2, base, sy)

    return jax.shard_map(
        body, mesh=mesh,
        in_specs=(rows, rows, rows, rows, P(None, "tp"), P(None, "tp"), P("tp", None),
                  P("ep", None, None), P("ep", None, None), P("ep", None, None)),
        out_specs=rows, check_vma=False)
```

```python
import functools

import jax
import jax.numpy as jnp
from jax import lax
from jax.experimental import pallas as pl
from jax.experimental.pallas import tpu as pltpu
from jax.sharding import PartitionSpec as P

CAP = 72
MAIN = 64
TAIL = CAP - MAIN
MIB = 1024 * 1024
ANY = pl.BlockSpec(memory_space=pl.ANY)


def _params(mib):
    return pltpu.CompilerParams(vmem_limit_bytes=mib * MIB)


def _dot(a, b):
    return jnp.dot(a, b, preferred_element_type=jnp.float32)


def _hot(c, n, base, tok):
    r = (lax.broadcasted_iota(jnp.int32, (n, tok), 0) + base).astype(jnp.float32)
    g = jnp.zeros((n, tok), jnp.float32)
    for j in range(4):
        g = jnp.where(r == c[j:j + 1, :], c[4 + j:5 + j, :], g)
    pick = jnp.where(g > 0, 1.0, 0.0).astype(jnp.bfloat16)
    return pick, jnp.broadcast_to(jnp.sum(g, axis=1, keepdims=True), (n, 128))


def _codes(t, me, el):
    code = t[0:4, :].astype(jnp.int32)
    e, k = code >> 7, code & 127
    le = e - me * el
    ok = (code >= 0) & (le >= 0) & (le < el)
    c = jnp.where(ok, jnp.where(k < MAIN, le * MAIN + k, el * MAIN + le * TAIL + k - MAIN), -1).astype(jnp.float32)
    return c


def _front_kernel(el, kt, x, mine, w1, w3, w2, cx, gm, base, sy, xc, xx, xxc,
                  y, tabs, tabt, v1, v3, v2, hs, sst, gst, wsem, xsend, xrecv, tsend, trecv, ssem, gsem):
    me = lax.axis_index("ep")
    tp = lax.axis_index("tp")
    sib = me + 1 - 2 * lax.rem(me, 2)
    peer = lax.rem(me + 2, 4)
    diag = lax.rem(sib + 2, 4)
    tok, d = x.shape
    parts = ((0, tok * 5 // 8), (tok * 5 // 8, tok * 3 // 8))
    nf, nn = v1.shape[0], v2.shape[0]
    tf, tn = v1.shape[2], v2.shape[2]
    mesh_id = pl.DeviceIdType.MESH

    def remote(src, dst, ss, rs, dev):
        return pltpu.make_async_remote_copy(src, dst, ss, rs, device_id=dev, device_id_type=mesh_id)

    def up(i):
        col = pl.ds(pl.multiple_of(i * tf, tf), tf)
        return (pltpu.make_async_copy(w1.at[:, col], v1.at[i], wsem.at[i]),
                pltpu.make_async_copy(w3.at[:, col], v3.at[i], wsem.at[nf + i]))

    def down(i):
        return pltpu.make_async_copy(w2.at[:, pl.ds(pl.multiple_of(i * tn, tn), tn)], v2.at[i], wsem.at[2 * nf + i])

    barrier = pltpu.get_barrier_semaphore()
    for dev in (sib, peer, diag):
        pl.semaphore_signal(barrier, inc=1, device_id={"ep": dev}, device_id_type=mesh_id)
    pl.semaphore_signal(barrier, inc=1, device_id={"tp": 1 - tp}, device_id_type=mesh_id)
    pl.semaphore_wait(barrier, 4)
    tcopy = [remote(mine, tabs.at[k], tsend.at[k], trecv.at[k], {"ep": dev}) for k, dev in enumerate((sib, peer, diag))]
    xcopy = remote(x, xx, xsend.at[0], xrecv.at[0], {"ep": peer})
    ccopy = remote(x, xc, xsend.at[1], xrecv.at[1], {"ep": sib})
    ycopy = [remote(x.at[pl.ds(*r)], y.at[pl.ds(*r)], xsend.at[2 + k], xrecv.at[2 + k], {"tp": 1 - tp})
             for k, r in enumerate(parts)]
    relay = remote(xx, xxc, xsend.at[4], xrecv.at[4], {"ep": sib})
    for c in (*tcopy, xcopy, *ycopy, ccopy):
        c.start()
    for i in range(nf):
        for c in up(i):
            c.start()
    for i in range(nn):
        down(i).start()

    def table(k):
        t = mine[...] if k == 0 else tabs[k - 1]
        c = _codes(t, me, el)
        cx[k] = jnp.concatenate([c, t[4:8, :]], axis=0)
        wide = jnp.concatenate([c, jnp.zeros((124, tok), jnp.float32)], axis=0)
        for b in range(0, tok, 128):
            tabt[k * tok + b:k * tok + b + 128, :] = jnp.transpose(wide[:, b:b + 128])

    def shared(src, lo, n, out, add, first):
        scopy = lambda i: pltpu.make_async_copy(
            sst.at[lax.rem(i, 2), pl.ds(0, n)], out.at[pl.ds(lo, n), pl.ds(pl.multiple_of(i * tn, tn), tn)], ssem.at[lax.rem(i, 2)])

        def gate(i, _):
            if first:
                for c in up(i):
                    c.wait()
            r = src[lo:lo + n, :]
            a = _dot(r, v1[i])
            b = _dot(r, v3[i])
            hs[lo:lo + n, pl.ds(pl.multiple_of(i * tf, tf), tf)] = (jax.nn.silu(a) * b).astype(jnp.bfloat16)
            return 0

        def tile(i, _):
            if first:
                down(i).wait()

            @pl.when(i >= 2)
            def _():
                scopy(i - 2).wait()

            r = _dot(hs[lo:lo + n, :], v2[i])
            if add:
                r = r + src[lo:lo + n, pl.ds(pl.multiple_of(i * tn, tn), tn)].astype(jnp.float32)
            sst[lax.rem(i, 2), 0:n, :] = r
            scopy(i).start()
            return 0

        lax.fori_loop(0, nf, gate, 0)
        lax.fori_loop(0, nn, tile, 0)
        for i in (nn - 2, nn - 1):
            scopy(jnp.int32(i)).wait()

    blk = gst.shape[1]
    gcopy = lambda i: pltpu.make_async_copy(gst.at[lax.rem(i, 2)], gm.at[pl.ds(pl.multiple_of(i * blk, blk), blk)], gsem.at[lax.rem(i, 2)])

    def picks(i, _):
        @pl.when(i >= 2)
        def _():
            gcopy(i - 2).wait()

        t = tabt[pl.ds(pl.multiple_of(i * blk, blk), blk), :]
        lane = lax.broadcasted_iota(jnp.int32, (blk, kt), 1).astype(jnp.float32)
        hit = t[:, 0:1] == lane
        for j in range(1, 4):
            hit = hit | (t[:, j:j + 1] == lane)
        gst[lax.rem(i, 2)] = jnp.where(hit, 1.0, 0.0).astype(jnp.bfloat16)
        gcopy(i).start()
        return 0

    ng = tok // blk
    table(0)
    lax.fori_loop(0, ng, picks, 0)
    for k in range(1, 4):
        tcopy[k - 1].wait()
        table(k)
    lax.fori_loop(ng, 4 * ng, picks, 0)
    for i in (4 * ng - 2, 4 * ng - 1):
        gcopy(jnp.int32(i)).wait()
    shared(x, 0, tok, base, True, True)
    ycopy[0].wait()
    shared(y, *parts[0], sy, False, False)
    xcopy.wait()
    relay.start()
    ycopy[1].wait()
    shared(y, *parts[1], sy, False, False)
    ccopy.wait()
    relay.wait()


def _front(x, mine, w1, w3, w2, el, kt):
    tok, d = x.shape
    f = w1.shape[1]
    tf, tn = 256, 512
    nf, nn = f // tf, d // tn
    bf16, f32 = jnp.bfloat16, jnp.float32
    vmem = pl.BlockSpec(memory_space=pltpu.VMEM)
    dma = pltpu.SemaphoreType.DMA
    return pl.pallas_call(
        functools.partial(_front_kernel, el, kt),
        out_shape=[jax.ShapeDtypeStruct(sh, dt) for sh, dt in (
            ((4, 8, tok), f32), ((4 * tok, kt), bf16), ((tok, d), f32), ((tok, d), f32),
            ((tok, d), bf16), ((tok, d), bf16), ((tok, d), bf16))],
        in_specs=[vmem, vmem] + [ANY] * 3,
        out_specs=[vmem] + [ANY] * 6,
        scratch_shapes=[
            pltpu.VMEM((tok, d), bf16),
            pltpu.VMEM((3, 8, tok), f32),
            pltpu.VMEM((4 * tok, 128), f32),
            pltpu.VMEM((nf, d, tf), bf16),
            pltpu.VMEM((nf, d, tf), bf16),
            pltpu.VMEM((nn, f, tn), bf16),
            pltpu.VMEM((tok, f), bf16),
            pltpu.VMEM((2, tok, tn), f32),
            pltpu.VMEM((2, 128, kt), bf16),
            dma((2 * nf + nn,)), dma((5,)), dma((5,)), dma((3,)), dma((3,)), dma((2,)), dma((2,)),
        ],
        compiler_params=pltpu.CompilerParams(vmem_limit_bytes=62 * MIB, collective_id=1, has_side_effects=True),
        cost_estimate=pl.CostEstimate(flops=12 * tok * d * f, bytes_accessed=6 * d * f, transcendentals=0),
        name="front",
    )(x, mine, w1, w3, w2)


def _up_kernel(el, x0, x1, x2, x3, cx, w1, w3, h, gs, xs, tg, xb, wv, xsem, wsem):
    e = pl.program_id(0)
    tok, d = x0.shape
    ring = wv.shape[0]
    srcs = (x0, x1, x2, x3)
    some = 5

    def wcopy(w, i, k):
        slot = lax.rem(2 * i + k, ring)
        return pltpu.make_async_copy(w.at[i], wv.at[slot], wsem.at[slot])

    xcopy = lambda s, k: pltpu.make_async_copy(srcs[s], xb.at[k], xsem.at[k])

    @pl.when(e == 0)
    def _():
        xcopy(0, 0).start()
        xcopy(1, 1).start()
        for i in range(ring):
            wcopy(w3 if i % 2 else w1, jnp.int32(i // 2), i % 2).start()

        def select(s, _):
            k = lax.rem(s, 2)
            xcopy(0, k).wait()
            c = cx[s]
            for b in range(0, el, some):
                p, g = _hot(c, some * MAIN, b * MAIN, tok)
                for i in range(some):
                    gs[b + i, pl.ds(pl.multiple_of(s * MAIN, MAIN), MAIN), :] = g[i * MAIN:(i + 1) * MAIN]
                for n in range(0, d, 512):
                    r = _dot(p, xb[k, :, n:n + 512]).astype(jnp.bfloat16)
                    for i in range(some):
                        xs[b + i, pl.ds(pl.multiple_of(s * MAIN, MAIN), MAIN), n:n + 512] = r[i * MAIN:(i + 1) * MAIN]
            p, g = _hot(c, el * TAIL, el * MAIN, tok)
            for i in range(el):
                gs[i, pl.ds(pl.multiple_of(4 * MAIN + s * TAIL, TAIL), TAIL), :] = g[i * TAIL:(i + 1) * TAIL]
            for n in range(0, d, 512):
                tg[s, :, n:n + 512] = _dot(p, xb[k, :, n:n + 512])
            for j in range(2):
                @pl.when(s == j)
                def _(j=j):
                    xcopy(2 + j, j).start()
            return 0

        lax.fori_loop(0, 4, select, 0)

    tail = pl.ds(pl.multiple_of(e * TAIL, TAIL), TAIL)
    xs[e, 4 * MAIN:4 * CAP, :] = jnp.concatenate([tg[s, tail, :] for s in range(4)], axis=0).astype(jnp.bfloat16)
    f = h.shape[-1]
    full = f // 256 * 256
    wcopy(w1, e, 0).wait()
    wcopy(w3, e, 1).wait()
    x = xs[e]
    v1, v3 = wv.at[lax.rem(2 * e, ring)], wv.at[lax.rem(2 * e + 1, ring)]
    for n in range(0, full, 256):
        a = _dot(x, v1[:, n:n + 256])
        b = _dot(x, v3[:, n:n + 256])
        h[0, :, n:n + 256] = (jax.nn.silu(a) * b).astype(jnp.bfloat16)
    if full < f:
        r = f - full
        ab = _dot(x, jnp.concatenate([v1[:, full:], v3[:, full:]], axis=1))
        h[0, :, full:] = (jax.nn.silu(ab[:, :r]) * ab[:, r:]).astype(jnp.bfloat16)

    @pl.when(e + 2 < el)
    def _():
        wcopy(w3, e + 2, 1).start()

    @pl.when(e + 3 < el)
    def _():
        wcopy(w1, e + 3, 0).start()


def _up(xs, cx, w1, w3):
    el, d, f = w1.shape
    tok = xs[0].shape[0]
    ring = 5
    return pl.pallas_call(
        functools.partial(_up_kernel, el),
        grid=(el,),
        out_shape=[jax.ShapeDtypeStruct((el, 4 * CAP, f), jnp.bfloat16), jax.ShapeDtypeStruct((el, 4 * CAP, 128), jnp.float32)],
        in_specs=[ANY] * 4 + [pl.BlockSpec(cx.shape, lambda e: (0, 0, 0))] + [ANY] * 2,
        out_specs=[pl.BlockSpec((1, 4 * CAP, f), lambda e: (e, 0, 0)), pl.BlockSpec((el, 4 * CAP, 128), lambda e: (0, 0, 0))],
        scratch_shapes=[
            pltpu.VMEM((el, 4 * CAP, d), jnp.bfloat16),
            pltpu.VMEM((4, el * TAIL, d), jnp.float32),
            pltpu.VMEM((2, tok, d), jnp.bfloat16),
            pltpu.VMEM((ring, d, f), jnp.bfloat16),
            pltpu.SemaphoreType.DMA((2,)),
            pltpu.SemaphoreType.DMA((ring,)),
        ],
        compiler_params=_params(63),
        cost_estimate=pl.CostEstimate(flops=2 * 2 * el * 4 * CAP * d * f, bytes_accessed=4 * el * d * f, transcendentals=0),
        name="up",
    )(*xs, cx, w1, w3)


def _route_kernel(el, tok, cols, g, gs, h, w2, base, sy, out, gv, gsv, hv, wv, r3, rt, send, recv, far, own, back, yb, bv, ost,
                  gsem, hsem, wsem, ssem, rsem, xssem, xrsem, osem, yssem, yrsem, bsem):
    me = lax.axis_index("ep")
    tp = lax.axis_index("tp")
    sib = me + 1 - 2 * lax.rem(me, 2)
    peer = lax.rem(me + 2, 4)
    ring = wv.shape[0]
    chunks = back.shape[0]
    kt = gv.shape[1]
    nm = el * MAIN
    total = chunks * el

    gcopy = lambda s: pltpu.make_async_copy(g.at[pl.ds(s * tok, tok)], gv.at[pl.ds(s * tok, tok)], gsem.at[s])
    hcopy = lambda e: pltpu.make_async_copy(h.at[e], hv.at[e], hsem.at[e])
    gscopy = pltpu.make_async_copy(gs, gsv, gsem.at[4])

    def split(v):
        hi = v.astype(jnp.bfloat16)
        v = v - hi.astype(jnp.float32)
        mid = v.astype(jnp.bfloat16)
        return hi, mid, (v - mid.astype(jnp.float32)).astype(jnp.bfloat16)

    def wcopy(t):
        slot = lax.rem(t, ring)
        col = pl.multiple_of(t // el * cols, cols)
        return pltpu.make_async_copy(w2.at[lax.rem(t, el), :, pl.ds(col, cols)], wv.at[slot], wsem.at[slot])

    def pair(c, k):
        return pltpu.make_async_remote_copy(send.at[lax.rem(c, 2), k], recv.at[c, k], ssem.at[c, k], rsem.at[c, k],
                                            device_id={"ep": sib}, device_id_type=pl.DeviceIdType.MESH)

    def across(c):
        return pltpu.make_async_remote_copy(recv.at[c, 1], back.at[c], xssem.at[c], xrsem.at[c],
                                            device_id={"ep": peer}, device_id_type=pl.DeviceIdType.MESH)

    part = lambda ref, c: ref.at[:, pl.ds(pl.multiple_of(c * cols, cols), cols)]

    def ycopy(c):
        return pltpu.make_async_remote_copy(part(sy, c), yb.at[c], yssem.at[c], yrsem.at[c],
                                            device_id={"tp": 1 - tp}, device_id_type=pl.DeviceIdType.MESH)

    bcopy = lambda c: pltpu.make_async_copy(part(base, c), bv.at[lax.rem(c, 2)], bsem.at[lax.rem(c, 2)])
    ocopy = lambda c: pltpu.make_async_copy(ost.at[lax.rem(c, 2)], part(out, c), osem.at[lax.rem(c, 2)])

    size = 4
    blocks = [(lo, min(lo + size, el)) for lo in range(0, el, size)]

    def load(k):
        for e in range(*blocks[k]):
            hcopy(e).start()
            wcopy(jnp.int32(e)).start()

    load(0)
    gscopy.start()
    load(1)
    barrier = pltpu.get_barrier_semaphore()
    for dev in (sib, peer):
        pl.semaphore_signal(barrier, inc=1, device_id={"ep": dev}, device_id_type=pl.DeviceIdType.MESH)
    pl.semaphore_signal(barrier, inc=1, device_id={"tp": 1 - tp}, device_id_type=pl.DeviceIdType.MESH)
    pl.semaphore_wait(barrier, 3)

    def group(c, lo, hi):
        for e in range(lo, hi):
            wcopy(c * el + e).wait()

        @pl.when(c == 0)
        def _():
            if lo == 0:
                gscopy.wait()
            for e in range(lo, hi):
                hcopy(e).wait()
            if lo + 2 * size < el:
                load(lo // size + 2)
            elif hi < el:
                for s in (3, 1, 2, 0):
                    gcopy(s).start()
                for b in range(2):
                    bcopy(jnp.int32(b)).start()

        for e in range(lo, hi):
            r = _dot(hv[e], wv[lax.rem(c * el + e, ring)]).astype(jnp.bfloat16).astype(jnp.float32)
            r = r * jnp.concatenate([gsv[e]] * (cols // 128), axis=1)
            for s in range(4):
                for i, v in enumerate(split(r[s * MAIN:(s + 1) * MAIN])):
                    r3[s, e * MAIN + i * kt:(e + 1) * MAIN + i * kt, :] = v
                rt[s, e * TAIL:(e + 1) * TAIL, :] = r[4 * MAIN + s * TAIL:4 * MAIN + (s + 1) * TAIL]
        for e in range(lo, hi):
            t = c * el + e

            @pl.when(t + ring < total)
            def _(t=t):
                wcopy(t + ring).start()

    def combine(s):
        tail = jnp.concatenate([rt[s], jnp.zeros((kt - el * CAP, cols), jnp.float32)], axis=0)
        for i, v in enumerate(split(tail)):
            r3[s, i * kt + nm:(i + 1) * kt, :] = v
        p = gv[s * tok:(s + 1) * tok, :]
        return sum(_dot(p, r3[s, i * kt:(i + 1) * kt, :]) for i in range(1, 3)) + _dot(p, r3[s, 0:kt, :])

    def merge(c):
        pair(c, 1).wait_recv()
        recv[c, 1] = recv[c, 1] + far[...]
        pair(c, 0).wait_recv()
        recv[c, 0] = recv[c, 0] + own[...]
        across(c).start()

    def chunk(c, _):
        group(c, *blocks[0])
        ycopy(c).start()

        @pl.when(c > 1)
        def _():
            merge(c - 1)

        for b in blocks[1:]:
            group(c, *b)

        @pl.when(c == 0)
        def _():
            for s in range(4):
                gcopy(s).wait()

        @pl.when(c >= 2)
        def _():
            pair(c - 2, 0).wait_send()
            pair(c - 2, 1).wait_send()

        slot = lax.rem(c, 2)
        send[slot, 1] = combine(3)
        send[slot, 0] = combine(1)
        pair(c, 1).start()
        pair(c, 0).start()
        far[...] = combine(2)
        own[...] = combine(0)

        @pl.when(c == 0)
        def _():
            merge(c)

        return 0

    lax.fori_loop(0, chunks, chunk, 0)
    merge(jnp.int32(chunks - 1))

    def finish(c, _):
        k = lax.rem(c, 2)
        bcopy(c).wait()
        ycopy(c).wait_recv()

        @pl.when(c >= 2)
        def _():
            ocopy(c - 2).wait()

        across(c).wait_recv()
        ost[k] = (bv[k] + yb[c] + (recv[c, 0] + back[c])).astype(jnp.bfloat16)
        ocopy(c).start()

        @pl.when(c + 2 < chunks)
        def _():
            bcopy(c + 2).start()

        return 0

    lax.fori_loop(0, chunks, finish, 0)
    for c in range(chunks - 2, chunks):
        pair(jnp.int32(c), 0).wait_send()
        pair(jnp.int32(c), 1).wait_send()
        ocopy(jnp.int32(c)).wait()
    for c in range(chunks):
        across(jnp.int32(c)).wait_send()
        ycopy(jnp.int32(c)).wait_send()


def _route(g, gs, h, w2, base, sy):
    el, f, d = w2.shape
    tok = base.shape[0]
    cols = 256
    chunks = d // cols
    ring = el
    kt = g.shape[1]
    f32 = jnp.float32
    return pl.pallas_call(
        functools.partial(_route_kernel, el, tok, cols),
        out_shape=jax.ShapeDtypeStruct((tok, d), jnp.bfloat16),
        in_specs=[ANY] * 6,
        out_specs=ANY,
        scratch_shapes=[
            pltpu.VMEM((4 * tok, kt), jnp.bfloat16),
            pltpu.VMEM(gs.shape, f32),
            pltpu.VMEM((el, 4 * CAP, f), jnp.bfloat16),
            pltpu.VMEM((ring, f, cols), jnp.bfloat16),
            pltpu.VMEM((4, 3 * kt, cols), jnp.bfloat16),
            pltpu.VMEM((4, el * TAIL, cols), f32),
            pltpu.VMEM((2, 2, tok, cols), f32),
            pltpu.VMEM((chunks, 2, tok, cols), f32),
            pltpu.VMEM((tok, cols), f32),
            pltpu.VMEM((tok, cols), f32),
            pltpu.VMEM((chunks, tok, cols), f32),
            pltpu.VMEM((chunks, tok, cols), f32),
            pltpu.VMEM((2, tok, cols), f32),
            pltpu.VMEM((2, tok, cols), jnp.bfloat16),
            pltpu.SemaphoreType.DMA((5,)),
            pltpu.SemaphoreType.DMA((el,)),
            pltpu.SemaphoreType.DMA((ring,)),
            pltpu.SemaphoreType.DMA((chunks, 2)),
            pltpu.SemaphoreType.DMA((chunks, 2)),
            pltpu.SemaphoreType.DMA((chunks,)),
            pltpu.SemaphoreType.DMA((chunks,)),
            pltpu.SemaphoreType.DMA((2,)),
            pltpu.SemaphoreType.DMA((chunks,)),
            pltpu.SemaphoreType.DMA((chunks,)),
            pltpu.SemaphoreType.DMA((2,)),
        ],
        compiler_params=pltpu.CompilerParams(vmem_limit_bytes=63 * MIB, collective_id=0, has_side_effects=True),
        cost_estimate=pl.CostEstimate(flops=2 * el * 4 * CAP * f * d + 24 * tok * kt * d,
                                      bytes_accessed=2 * el * f * d + 2 * el * 4 * CAP * f, transcendentals=0),
        name="route",
    )(g, gs, h, w2, base, sy)


def solution(mesh):
    rows = P(("ep", "tp"), None)
    def body(x, idx, g, slot, ws1, ws3, ws2, w1, w3, w2):
        tok, d = x.shape
        el = w1.shape[0]
        kt = -(-el * CAP // 16) * 16
        code = jnp.where(slot >= 0, idx * 128 + slot, -1).astype(jnp.float32)
        mine = jnp.concatenate([code, g], axis=1).T
        cx, gm, base, sy, xc, xx, xxc = _front(x, mine, ws1, ws3, ws2, el, kt)
        h, gs = _up((x, xc, xx, xxc), cx, w1, w3)
        return _route(gm, gs, h, w2, base, sy)

    return jax.shard_map(
        body, mesh=mesh,
        in_specs=(rows, rows, rows, rows, P(None, "tp"), P(None, "tp"), P("tp", None),
                  P("ep", None, None), P("ep", None, None), P("ep", None, None)),
        out_specs=rows, check_vma=False)
```

```python
import functools

import jax
import jax.numpy as jnp
from jax import lax
from jax.experimental import pallas as pl
from jax.experimental.pallas import tpu as pltpu
from jax.sharding import PartitionSpec as P

CAP = 72
MAIN = 64
TAIL = CAP - MAIN
MIB = 1024 * 1024
ANY = pl.BlockSpec(memory_space=pl.ANY)


def _params(mib):
    return pltpu.CompilerParams(vmem_limit_bytes=mib * MIB)


def _dot(a, b):
    return jnp.dot(a, b, preferred_element_type=jnp.float32)


def _hot(c, n, base, tok):
    r = (lax.broadcasted_iota(jnp.int32, (n, tok), 0) + base).astype(jnp.float32)
    g = jnp.zeros((n, tok), jnp.float32)
    for j in range(4):
        g = jnp.where(r == c[j:j + 1, :], c[4 + j:5 + j, :], g)
    pick = jnp.where(g > 0, 1.0, 0.0).astype(jnp.bfloat16)
    return pick, jnp.broadcast_to(jnp.sum(g, axis=1, keepdims=True), (n, 128))


def _codes(t, me, el):
    code = t[0:4, :].astype(jnp.int32)
    e, k = code >> 7, code & 127
    le = e - me * el
    ok = (code >= 0) & (le >= 0) & (le < el)
    c = jnp.where(ok, jnp.where(k < MAIN, le * MAIN + k, el * MAIN + le * TAIL + k - MAIN), -1).astype(jnp.float32)
    return c


def _front_kernel(el, kt, x, mine, w1, w3, w2, cx, gm, base, sy, xc, xx, xxc,
                  y, tabs, tabt, v1, v3, v2, hs, sst, gst, wsem, xsend, xrecv, tsend, trecv, ssem, gsem):
    me = lax.axis_index("ep")
    tp = lax.axis_index("tp")
    sib = me + 1 - 2 * lax.rem(me, 2)
    peer = lax.rem(me + 2, 4)
    diag = lax.rem(sib + 2, 4)
    tok, d = x.shape
    parts = ((0, tok * 5 // 8), (tok * 5 // 8, tok * 3 // 8))
    nf, nn = v1.shape[0], v2.shape[0]
    tf, tn = v1.shape[2], v2.shape[2]
    mesh_id = pl.DeviceIdType.MESH

    def remote(src, dst, ss, rs, dev):
        return pltpu.make_async_remote_copy(src, dst, ss, rs, device_id=dev, device_id_type=mesh_id)

    def up(i):
        col = pl.ds(pl.multiple_of(i * tf, tf), tf)
        return (pltpu.make_async_copy(w1.at[:, col], v1.at[i], wsem.at[i]),
                pltpu.make_async_copy(w3.at[:, col], v3.at[i], wsem.at[nf + i]))

    def down(i):
        return pltpu.make_async_copy(w2.at[:, pl.ds(pl.multiple_of(i * tn, tn), tn)], v2.at[i], wsem.at[2 * nf + i])

    barrier = pltpu.get_barrier_semaphore()
    for dev in (sib, peer, diag):
        pl.semaphore_signal(barrier, inc=1, device_id={"ep": dev}, device_id_type=mesh_id)
    pl.semaphore_signal(barrier, inc=1, device_id={"tp": 1 - tp}, device_id_type=mesh_id)
    pl.semaphore_wait(barrier, 4)
    tcopy = [remote(mine, tabs.at[k], tsend.at[k], trecv.at[k], {"ep": dev}) for k, dev in enumerate((sib, peer, diag))]
    xcopy = remote(x, xx, xsend.at[0], xrecv.at[0], {"ep": peer})
    ccopy = remote(x, xc, xsend.at[1], xrecv.at[1], {"ep": sib})
    ycopy = [remote(x.at[pl.ds(*r)], y.at[pl.ds(*r)], xsend.at[2 + k], xrecv.at[2 + k], {"tp": 1 - tp})
             for k, r in enumerate(parts)]
    relay = remote(xx, xxc, xsend.at[4], xrecv.at[4], {"ep": sib})
    for c in (*tcopy, xcopy, *ycopy, ccopy):
        c.start()
    for i in range(nf):
        for c in up(i):
            c.start()
    for i in range(nn):
        down(i).start()

    def table(k):
        t = mine[...] if k == 0 else tabs[k - 1]
        c = _codes(t, me, el)
        cx[k] = jnp.concatenate([c, t[4:8, :]], axis=0)
        wide = jnp.concatenate([c, jnp.zeros((124, tok), jnp.float32)], axis=0)
        for b in range(0, tok, 128):
            tabt[k * tok + b:k * tok + b + 128, :] = jnp.transpose(wide[:, b:b + 128])

    def shared(src, lo, n, out, add, first):
        scopy = lambda i: pltpu.make_async_copy(
            sst.at[lax.rem(i, 2), pl.ds(0, n)], out.at[pl.ds(lo, n), pl.ds(pl.multiple_of(i * tn, tn), tn)], ssem.at[lax.rem(i, 2)])

        def gate(i, _):
            if first:
                for c in up(i):
                    c.wait()
            r = src[lo:lo + n, :]
            a = _dot(r, v1[i])
            b = _dot(r, v3[i])
            hs[lo:lo + n, pl.ds(pl.multiple_of(i * tf, tf), tf)] = (jax.nn.silu(a) * b).astype(jnp.bfloat16)
            return 0

        def tile(i, _):
            if first:
                down(i).wait()

            @pl.when(i >= 2)
            def _():
                scopy(i - 2).wait()

            r = _dot(hs[lo:lo + n, :], v2[i])
            if add:
                r = r + src[lo:lo + n, pl.ds(pl.multiple_of(i * tn, tn), tn)].astype(jnp.float32)
            sst[lax.rem(i, 2), 0:n, :] = r
            scopy(i).start()
            return 0

        lax.fori_loop(0, nf, gate, 0)
        lax.fori_loop(0, nn, tile, 0)
        for i in (nn - 2, nn - 1):
            scopy(jnp.int32(i)).wait()

    blk = gst.shape[1]
    gcopy = lambda i: pltpu.make_async_copy(gst.at[lax.rem(i, 2)], gm.at[pl.ds(pl.multiple_of(i * blk, blk), blk)], gsem.at[lax.rem(i, 2)])

    def picks(i, _):
        @pl.when(i >= 2)
        def _():
            gcopy(i - 2).wait()

        t = tabt[pl.ds(pl.multiple_of(i * blk, blk), blk), :]
        lane = lax.broadcasted_iota(jnp.int32, (blk, kt), 1).astype(jnp.float32)
        hit = t[:, 0:1] == lane
        for j in range(1, 4):
            hit = hit | (t[:, j:j + 1] == lane)
        gst[lax.rem(i, 2)] = jnp.where(hit, 1.0, 0.0).astype(jnp.bfloat16)
        gcopy(i).start()
        return 0

    ng = tok // blk
    table(0)
    lax.fori_loop(0, ng, picks, 0)
    for k in range(1, 4):
        tcopy[k - 1].wait()
        table(k)
    lax.fori_loop(ng, 4 * ng, picks, 0)
    for i in (4 * ng - 2, 4 * ng - 1):
        gcopy(jnp.int32(i)).wait()
    shared(x, 0, tok, base, True, True)
    ycopy[0].wait()
    shared(y, *parts[0], sy, False, False)
    xcopy.wait()
    relay.start()
    ycopy[1].wait()
    shared(y, *parts[1], sy, False, False)
    ccopy.wait()
    relay.wait()


def _front(x, mine, w1, w3, w2, el, kt):
    tok, d = x.shape
    f = w1.shape[1]
    tf, tn = 256, 512
    nf, nn = f // tf, d // tn
    bf16, f32 = jnp.bfloat16, jnp.float32
    vmem = pl.BlockSpec(memory_space=pltpu.VMEM)
    dma = pltpu.SemaphoreType.DMA
    return pl.pallas_call(
        functools.partial(_front_kernel, el, kt),
        out_shape=[jax.ShapeDtypeStruct(sh, dt) for sh, dt in (
            ((4, 8, tok), f32), ((4 * tok, kt), bf16), ((tok, d), f32), ((tok, d), f32),
            ((tok, d), bf16), ((tok, d), bf16), ((tok, d), bf16))],
        in_specs=[vmem, vmem] + [ANY] * 3,
        out_specs=[vmem] + [ANY] * 6,
        scratch_shapes=[
            pltpu.VMEM((tok, d), bf16),
            pltpu.VMEM((3, 8, tok), f32),
            pltpu.VMEM((4 * tok, 128), f32),
            pltpu.VMEM((nf, d, tf), bf16),
            pltpu.VMEM((nf, d, tf), bf16),
            pltpu.VMEM((nn, f, tn), bf16),
            pltpu.VMEM((tok, f), bf16),
            pltpu.VMEM((2, tok, tn), f32),
            pltpu.VMEM((2, 128, kt), bf16),
            dma((2 * nf + nn,)), dma((5,)), dma((5,)), dma((3,)), dma((3,)), dma((2,)), dma((2,)),
        ],
        compiler_params=pltpu.CompilerParams(vmem_limit_bytes=62 * MIB, collective_id=1, has_side_effects=True),
        cost_estimate=pl.CostEstimate(flops=12 * tok * d * f, bytes_accessed=6 * d * f, transcendentals=0),
        name="front",
    )(x, mine, w1, w3, w2)


def _up_kernel(el, x0, x1, x2, x3, cx, w1, w3, h, gs, xs, tg, xb, wv, xsem, wsem):
    e = pl.program_id(0)
    tok, d = x0.shape
    ring = wv.shape[0]
    srcs = (x0, x1, x2, x3)
    some = 5

    def wcopy(w, i, k):
        slot = lax.rem(2 * i + k, ring)
        return pltpu.make_async_copy(w.at[i], wv.at[slot], wsem.at[slot])

    xcopy = lambda s, k: pltpu.make_async_copy(srcs[s], xb.at[k], xsem.at[k])

    @pl.when(e == 0)
    def _():
        xcopy(0, 0).start()
        xcopy(1, 1).start()
        for i in range(ring):
            wcopy(w3 if i % 2 else w1, jnp.int32(i // 2), i % 2).start()

        def select(s, _):
            k = lax.rem(s, 2)
            xcopy(0, k).wait()
            c = cx[s]
            for b in range(0, el, some):
                p, g = _hot(c, some * MAIN, b * MAIN, tok)
                for i in range(some):
                    gs[b + i, pl.ds(pl.multiple_of(s * MAIN, MAIN), MAIN), :] = g[i * MAIN:(i + 1) * MAIN]
                for n in range(0, d, 512):
                    r = _dot(p, xb[k, :, n:n + 512]).astype(jnp.bfloat16)
                    for i in range(some):
                        xs[b + i, pl.ds(pl.multiple_of(s * MAIN, MAIN), MAIN), n:n + 512] = r[i * MAIN:(i + 1) * MAIN]
            p, g = _hot(c, el * TAIL, el * MAIN, tok)
            for i in range(el):
                gs[i, pl.ds(pl.multiple_of(4 * MAIN + s * TAIL, TAIL), TAIL), :] = g[i * TAIL:(i + 1) * TAIL]
            for n in range(0, d, 512):
                tg[s, :, n:n + 512] = _dot(p, xb[k, :, n:n + 512])
            for j in range(2):
                @pl.when(s == j)
                def _(j=j):
                    xcopy(2 + j, j).start()
            return 0

        lax.fori_loop(0, 4, select, 0)

    tail = pl.ds(pl.multiple_of(e * TAIL, TAIL), TAIL)
    xs[e, 4 * MAIN:4 * CAP, :] = jnp.concatenate([tg[s, tail, :] for s in range(4)], axis=0).astype(jnp.bfloat16)
    f = h.shape[-1]
    full = f // 256 * 256
    wcopy(w1, e, 0).wait()
    wcopy(w3, e, 1).wait()
    x = xs[e]
    v1, v3 = wv.at[lax.rem(2 * e, ring)], wv.at[lax.rem(2 * e + 1, ring)]
    for n in range(0, full, 256):
        a = _dot(x, v1[:, n:n + 256])
        b = _dot(x, v3[:, n:n + 256])
        h[0, :, n:n + 256] = (jax.nn.silu(a) * b).astype(jnp.bfloat16)
    if full < f:
        r = f - full
        ab = _dot(x, jnp.concatenate([v1[:, full:], v3[:, full:]], axis=1))
        h[0, :, full:] = (jax.nn.silu(ab[:, :r]) * ab[:, r:]).astype(jnp.bfloat16)

    @pl.when(e + 2 < el)
    def _():
        wcopy(w3, e + 2, 1).start()

    @pl.when(e + 3 < el)
    def _():
        wcopy(w1, e + 3, 0).start()


def _up(xs, cx, w1, w3):
    el, d, f = w1.shape
    tok = xs[0].shape[0]
    ring = 5
    return pl.pallas_call(
        functools.partial(_up_kernel, el),
        grid=(el,),
        out_shape=[jax.ShapeDtypeStruct((el, 4 * CAP, f), jnp.bfloat16), jax.ShapeDtypeStruct((el, 4 * CAP, 128), jnp.float32)],
        in_specs=[ANY] * 4 + [pl.BlockSpec(cx.shape, lambda e: (0, 0, 0))] + [ANY] * 2,
        out_specs=[pl.BlockSpec((1, 4 * CAP, f), lambda e: (e, 0, 0)), pl.BlockSpec((el, 4 * CAP, 128), lambda e: (0, 0, 0))],
        scratch_shapes=[
            pltpu.VMEM((el, 4 * CAP, d), jnp.bfloat16),
            pltpu.VMEM((4, el * TAIL, d), jnp.float32),
            pltpu.VMEM((2, tok, d), jnp.bfloat16),
            pltpu.VMEM((ring, d, f), jnp.bfloat16),
            pltpu.SemaphoreType.DMA((2,)),
            pltpu.SemaphoreType.DMA((ring,)),
        ],
        compiler_params=_params(63),
        cost_estimate=pl.CostEstimate(flops=2 * 2 * el * 4 * CAP * d * f, bytes_accessed=4 * el * d * f, transcendentals=0),
        name="up",
    )(*xs, cx, w1, w3)


def _route_kernel(el, tok, cols, g, gs, h, w2, base, sy, out, gv, gsv, hv, wv, r3, rt, send, recv, far, own, back, yb, bv, ost,
                  gsem, hsem, wsem, ssem, rsem, xssem, xrsem, osem, yssem, yrsem, bsem):
    me = lax.axis_index("ep")
    tp = lax.axis_index("tp")
    sib = me + 1 - 2 * lax.rem(me, 2)
    peer = lax.rem(me + 2, 4)
    ring = wv.shape[0]
    chunks = back.shape[0]
    kt = gv.shape[1]
    nm = el * MAIN
    total = chunks * el

    gcopy = lambda s: pltpu.make_async_copy(g.at[pl.ds(s * tok, tok)], gv.at[pl.ds(s * tok, tok)], gsem.at[s])
    hcopy = lambda e: pltpu.make_async_copy(h.at[e], hv.at[e], hsem.at[e])
    gscopy = pltpu.make_async_copy(gs, gsv, gsem.at[4])

    def split(v):
        hi = v.astype(jnp.bfloat16)
        v = v - hi.astype(jnp.float32)
        mid = v.astype(jnp.bfloat16)
        return hi, mid, (v - mid.astype(jnp.float32)).astype(jnp.bfloat16)

    def wcopy(t):
        slot = lax.rem(t, ring)
        col = pl.multiple_of(t // el * cols, cols)
        return pltpu.make_async_copy(w2.at[lax.rem(t, el), :, pl.ds(col, cols)], wv.at[slot], wsem.at[slot])

    def pair(c, k):
        return pltpu.make_async_remote_copy(send.at[lax.rem(c, 2), k], recv.at[c, k], ssem.at[c, k], rsem.at[c, k],
                                            device_id={"ep": sib}, device_id_type=pl.DeviceIdType.MESH)

    def across(c):
        return pltpu.make_async_remote_copy(recv.at[c, 1], back.at[c], xssem.at[c], xrsem.at[c],
                                            device_id={"ep": peer}, device_id_type=pl.DeviceIdType.MESH)

    part = lambda ref, c: ref.at[:, pl.ds(pl.multiple_of(c * cols, cols), cols)]

    def ycopy(c):
        return pltpu.make_async_remote_copy(part(sy, c), yb.at[c], yssem.at[c], yrsem.at[c],
                                            device_id={"tp": 1 - tp}, device_id_type=pl.DeviceIdType.MESH)

    bcopy = lambda c: pltpu.make_async_copy(part(base, c), bv.at[lax.rem(c, 2)], bsem.at[lax.rem(c, 2)])
    ocopy = lambda c: pltpu.make_async_copy(ost.at[lax.rem(c, 2)], part(out, c), osem.at[lax.rem(c, 2)])

    size = 4
    blocks = [(lo, min(lo + size, el)) for lo in range(0, el, size)]

    def load(k):
        for e in range(*blocks[k]):
            hcopy(e).start()
            wcopy(jnp.int32(e)).start()

    load(0)
    gscopy.start()
    load(1)
    barrier = pltpu.get_barrier_semaphore()
    for dev in (sib, peer):
        pl.semaphore_signal(barrier, inc=1, device_id={"ep": dev}, device_id_type=pl.DeviceIdType.MESH)
    pl.semaphore_signal(barrier, inc=1, device_id={"tp": 1 - tp}, device_id_type=pl.DeviceIdType.MESH)
    pl.semaphore_wait(barrier, 3)

    def group(c, lo, hi):
        for e in range(lo, hi):
            wcopy(c * el + e).wait()

        @pl.when(c == 0)
        def _():
            if lo == 0:
                gscopy.wait()
            for e in range(lo, hi):
                hcopy(e).wait()
            if lo + 2 * size < el:
                load(lo // size + 2)
            elif hi < el:
                for s in (3, 1, 2, 0):
                    gcopy(s).start()
                for b in range(2):
                    bcopy(jnp.int32(b)).start()

        for e in range(lo, hi):
            r = _dot(hv[e], wv[lax.rem(c * el + e, ring)]).astype(jnp.bfloat16).astype(jnp.float32)
            r = r * jnp.concatenate([gsv[e]] * (cols // 128), axis=1)
            for s in range(4):
                for i, v in enumerate(split(r[s * MAIN:(s + 1) * MAIN])):
                    r3[s, e * MAIN + i * kt:(e + 1) * MAIN + i * kt, :] = v
                rt[s, e * TAIL:(e + 1) * TAIL, :] = r[4 * MAIN + s * TAIL:4 * MAIN + (s + 1) * TAIL]
        for e in range(lo, hi):
            t = c * el + e

            @pl.when(t + ring < total)
            def _(t=t):
                wcopy(t + ring).start()

    def combine(s):
        tail = jnp.concatenate([rt[s], jnp.zeros((kt - el * CAP, cols), jnp.float32)], axis=0)
        for i, v in enumerate(split(tail)):
            r3[s, i * kt + nm:(i + 1) * kt, :] = v
        p = gv[s * tok:(s + 1) * tok, :]
        return sum(_dot(p, r3[s, i * kt:(i + 1) * kt, :]) for i in range(1, 3)) + _dot(p, r3[s, 0:kt, :])

    def merge(c):
        pair(c, 1).wait_recv()
        recv[c, 1] = recv[c, 1] + far[...]
        pair(c, 0).wait_recv()
        recv[c, 0] = recv[c, 0] + own[...]
        across(c).start()

    def chunk(c, _):
        group(c, *blocks[0])
        ycopy(c).start()

        @pl.when(c > 1)
        def _():
            merge(c - 1)

        for b in blocks[1:]:
            group(c, *b)

        @pl.when(c == 0)
        def _():
            for s in range(4):
                gcopy(s).wait()

        @pl.when(c >= 2)
        def _():
            pair(c - 2, 0).wait_send()
            pair(c - 2, 1).wait_send()

        slot = lax.rem(c, 2)
        send[slot, 1] = combine(3)
        send[slot, 0] = combine(1)
        pair(c, 1).start()
        pair(c, 0).start()
        far[...] = combine(2)
        own[...] = combine(0)

        @pl.when(c == 0)
        def _():
            merge(c)

        return 0

    lax.fori_loop(0, chunks, chunk, 0)
    merge(jnp.int32(chunks - 1))

    def finish(c, _):
        k = lax.rem(c, 2)
        bcopy(c).wait()
        ycopy(c).wait_recv()

        @pl.when(c >= 2)
        def _():
            ocopy(c - 2).wait()

        across(c).wait_recv()
        ost[k] = (bv[k] + yb[c] + (recv[c, 0] + back[c])).astype(jnp.bfloat16)
        ocopy(c).start()

        @pl.when(c + 2 < chunks)
        def _():
            bcopy(c + 2).start()

        return 0

    lax.fori_loop(0, chunks, finish, 0)
    for c in range(chunks - 2, chunks):
        pair(jnp.int32(c), 0).wait_send()
        pair(jnp.int32(c), 1).wait_send()
        ocopy(jnp.int32(c)).wait()
    for c in range(chunks):
        across(jnp.int32(c)).wait_send()
        ycopy(jnp.int32(c)).wait_send()


def _route(g, gs, h, w2, base, sy):
    el, f, d = w2.shape
    tok = base.shape[0]
    cols = 256
    chunks = d // cols
    ring = el
    kt = g.shape[1]
    f32 = jnp.float32
    return pl.pallas_call(
        functools.partial(_route_kernel, el, tok, cols),
        out_shape=jax.ShapeDtypeStruct((tok, d), jnp.bfloat16),
        in_specs=[ANY] * 6,
        out_specs=ANY,
        scratch_shapes=[
            pltpu.VMEM((4 * tok, kt), jnp.bfloat16),
            pltpu.VMEM(gs.shape, f32),
            pltpu.VMEM((el, 4 * CAP, f), jnp.bfloat16),
            pltpu.VMEM((ring, f, cols), jnp.bfloat16),
            pltpu.VMEM((4, 3 * kt, cols), jnp.bfloat16),
            pltpu.VMEM((4, el * TAIL, cols), f32),
            pltpu.VMEM((2, 2, tok, cols), f32),
            pltpu.VMEM((chunks, 2, tok, cols), f32),
            pltpu.VMEM((tok, cols), f32),
            pltpu.VMEM((tok, cols), f32),
            pltpu.VMEM((chunks, tok, cols), f32),
            pltpu.VMEM((chunks, tok, cols), f32),
            pltpu.VMEM((2, tok, cols), f32),
            pltpu.VMEM((2, tok, cols), jnp.bfloat16),
            pltpu.SemaphoreType.DMA((5,)),
            pltpu.SemaphoreType.DMA((el,)),
            pltpu.SemaphoreType.DMA((ring,)),
            pltpu.SemaphoreType.DMA((chunks, 2)),
            pltpu.SemaphoreType.DMA((chunks, 2)),
            pltpu.SemaphoreType.DMA((chunks,)),
            pltpu.SemaphoreType.DMA((chunks,)),
            pltpu.SemaphoreType.DMA((2,)),
            pltpu.SemaphoreType.DMA((chunks,)),
            pltpu.SemaphoreType.DMA((chunks,)),
            pltpu.SemaphoreType.DMA((2,)),
        ],
        compiler_params=pltpu.CompilerParams(vmem_limit_bytes=63 * MIB, collective_id=0, has_side_effects=True),
        cost_estimate=pl.CostEstimate(flops=2 * el * 4 * CAP * f * d + 24 * tok * kt * d,
                                      bytes_accessed=2 * el * f * d + 2 * el * 4 * CAP * f, transcendentals=0),
        name="route",
    )(g, gs, h, w2, base, sy)


def solution(mesh):
    rows = P(("ep", "tp"), None)
    def body(x, idx, g, slot, ws1, ws3, ws2, w1, w3, w2):
        tok, d = x.shape
        el = w1.shape[0]
        kt = -(-el * CAP // 16) * 16
        wide = lambda a, lo: jnp.pad(a, ((0, 0), (lo, 4 - lo)))
        kept = wide(slot, 0) >= 0
        head = jnp.where(kept, wide(idx, 0) * 128 + wide(slot, 0), -1).astype(jnp.float32)
        lane = lax.broadcasted_iota(jnp.int32, head.shape, 1)
        mine = jnp.where(lane < 4, head, wide(g, 4)).T
        cx, gm, base, sy, xc, xx, xxc = _front(x, mine, ws1, ws3, ws2, el, kt)
        h, gs = _up((x, xc, xx, xxc), cx, w1, w3)
        return _route(gm, gs, h, w2, base, sy)

    return jax.shard_map(
        body, mesh=mesh,
        in_specs=(rows, rows, rows, rows, P(None, "tp"), P(None, "tp"), P("tp", None),
                  P("ep", None, None), P("ep", None, None), P("ep", None, None)),
        out_specs=rows, check_vma=False)
```
